32 devices in a mesh: curve: 8 (over z, y), sub: 4 (over x, core).
Axes of the slice: x: 2, y: 2, z: 4, core: 2. Of those that a mesh axis runs over, the one named last changes fastest.
Arguments:
- state: float32 [4, 25, 8192], P(None, None, ('curve', 'sub')), may hold values from -6 to 6
- register: float32 [4, 25, 8192], P(None, None, ('curve', 'sub')), may hold values from -6 to 6
- neighbor: int32 [4, 2048], P(None, ('curve', 'sub')), may hold values from 0 to 2047, as said below
- neighbor_face: int32 [4, 2048], P(None, ('curve', 'sub')), may hold values from 0 to 3, as said below
- seam: int32 [4, 2048], P(None, ('curve', 'sub')), may hold values from 0 to 7, as said below
Outputs:
- next_state: float32 [4, 25, 8192], P(None, None, ('curve', 'sub'))
- next_register: float32 [4, 25, 8192], P(None, None, ('curve', 'sub'))
The draws below stay inside these ranges and needn't reach their ends.
Inputs may be any that keep to these rules, and one draw needn't show every extreme that they name: neighbor[k, e] is the element across local face k of element e, and the relation is mutual through neighbor_face. Elements d * 64 to (d + 1) * 64 - 1 lie on device d, whose curve index is d // 4 and sub index d % 4. A neighbour lies on the same device; or on one of the two devices with the same curve index and sub index one higher or one lower (wrapping), exactly 8 faces toward each; or on a device with the same sub index whose curve index is 1 to 3 higher or lower (wrapping), 8 such faces in each direction, at most 3 toward any one device. Every device has such faces at distance 3 in both directions, and every device reaches 3 toward some device. neighbor_face[k, e] is the face of neighbor[k, e] whose neighbour is e. seam = rot + 4 * flip; the two faces of a pair carry rot and (4 - rot) % 4 and the same flip; inside a device rot and flip are 0.
All inputs are finite; a program needn't handle non-finite values.
Results may differ from the reference program's by a relative error of at most 0.0003.
Values sent between devices are 32-bit elements; how exact they have to be, the bound alone decides.
A program may use at most 64 MiB of HBM per device.

```python
import math
import jax
import jax.numpy as jnp
import numpy as np
from jax import lax

TW = 8
LEVELS = 4
NODES = 25
FIELDS = 4
GROUPS = 8
STRIPS = 4
DMAX = 3
E_DEV = 64
ELEMS = 2048


def facing_negative(face, frame):
    return jnp.where(face % 2 == 0, (frame == 1) | (frame == 2), frame >= 2)


def build_mesh(key):
    base_key = jax.random.fold_in(key, 7)
    key_frame, key_order, key_rows, key_shift = jax.random.split(base_key, 4)
    devices = GROUPS * STRIPS
    frames = jax.random.randint(key_frame, (devices,), 0, 4).astype(jnp.int32)
    local_of_pos = jax.vmap(lambda sub_key: jax.random.permutation(sub_key, E_DEV))(jax.random.split(key_order, devices)).astype(jnp.int32)
    pos_of_local = jnp.argsort(local_of_pos, axis=1).astype(jnp.int32)
    row_order = jax.vmap(lambda sub_key: jax.random.permutation(sub_key, TW))(jax.random.split(key_rows, STRIPS)).astype(jnp.int32)
    row_shift = jax.random.randint(key_shift, (STRIPS, 1), 0, DMAX).astype(jnp.int32)
    distance = 1 + (row_order + row_shift) % DMAX
    device_ids = jnp.arange(devices, dtype=jnp.int32)[:, None]
    group_ids = device_ids // STRIPS
    strip_ids = device_ids % STRIPS
    position = pos_of_local
    column_ids = position // TW
    row_ids = position % TW
    row_reach = jnp.take_along_axis(distance[strip_ids[:, 0]], row_ids, axis=1)
    inside = column_ids < TW - 1
    dest_east = jnp.where(inside, device_ids, (group_ids + row_reach) % GROUPS * STRIPS + strip_ids)
    pos_east = jnp.where(inside, position + TW, row_ids)
    inside = row_ids < TW - 1
    dest_north = jnp.where(inside, device_ids, group_ids * STRIPS + (strip_ids + 1) % STRIPS)
    pos_north = jnp.where(inside, position + 1, column_ids * TW)
    inside = column_ids > 0
    dest_west = jnp.where(inside, device_ids, (group_ids - row_reach) % GROUPS * STRIPS + strip_ids)
    pos_west = jnp.where(inside, position - TW, (TW - 1) * TW + row_ids)
    inside = row_ids > 0
    dest_south = jnp.where(inside, device_ids, group_ids * STRIPS + (strip_ids - 1) % STRIPS)
    pos_south = jnp.where(inside, position - 1, column_ids * TW + TW - 1)
    dest = jnp.stack([dest_east, dest_north, dest_west, dest_south]).astype(jnp.int32)
    dest_pos = jnp.stack([pos_east, pos_north, pos_west, pos_south]).astype(jnp.int32)
    global_nb = dest * E_DEV + local_of_pos[dest, dest_pos]
    frame_nb = frames[dest]
    frame_self = jnp.broadcast_to(frames[None, :, None], (4, devices, E_DEV))
    face_ids = jnp.broadcast_to(jnp.arange(4, dtype=jnp.int32)[:, None, None], (4, devices, E_DEV))
    side = (face_ids + frame_self) % 4
    nb_local = jnp.take_along_axis(global_nb, side, axis=0)
    frame_across = jnp.take_along_axis(frame_nb, side, axis=0)
    face_back = ((side + 2) % 4 - frame_across) % 4
    turn = (frame_across - frame_self) % 4
    flipped = (facing_negative(face_ids, frame_self) != facing_negative(face_back, frame_across)).astype(jnp.int32)
    codes = turn + 4 * flipped
    total = devices * E_DEV
    return (nb_local.reshape(4, total).astype(jnp.int32), face_back.reshape(4, total).astype(jnp.int32), codes.reshape(4, total).astype(jnp.int32))


def draw_neighbor(key, part):
    return build_mesh(key)[0]


def draw_neighbor_face(key, part):
    return build_mesh(key)[1]


def draw_seam(key, part):
    return build_mesh(key)[2]


def steps_of(rng, extent, cuts, least, largest):
    factor_of, own = 1.0, jax.random.fold_in(rng, 6)
    for dim, blocks in cuts:
        steps = jnp.exp(jax.random.uniform(jax.random.fold_in(own, dim), (blocks,), jnp.float32, least / len(cuts), largest / len(cuts)))
        factor_of = factor_of * jnp.repeat(steps, extent[dim] // blocks).reshape([-1 if axis == dim else 1 for axis in range(len(extent))])
    return factor_of


def noise(stream_key, dims, scale, limit, shards=(), held_as=jnp.bfloat16):
    drawn = jax.random.normal(stream_key, dims, jnp.float32) * scale
    if len(shards) > 0:
        drawn = steps_of(stream_key, dims, shards, -0.22, 0.18) * drawn
    return jnp.clip(drawn, min=-limit, max=limit).astype(held_as)


def setup_inputs(seed: int = 0) -> dict:
    keys = jax.random.split(jax.random.key(seed), 6)
    state = noise(keys[0], (FIELDS, NODES, ELEMS * LEVELS), 1.0, 6.0, ((2, 32),), jnp.float32)
    register = noise(keys[1], (FIELDS, NODES, ELEMS * LEVELS), 1.0, 6.0, ((2, 32),), jnp.float32)
    neighbor = draw_neighbor(jax.random.fold_in(keys[5], 71), 0)
    neighbor_face = draw_neighbor_face(jax.random.fold_in(keys[5], 71), 0)
    seam = draw_seam(jax.random.fold_in(keys[5], 71), 0)
    return {"state": state, "register": register, "neighbor": neighbor, "neighbor_face": neighbor_face, "seam": seam}


def build_derivative():
    points = np.array([-1.0, -math.sqrt(3.0 / 7.0), 0.0, math.sqrt(3.0 / 7.0), 1.0])
    weights = np.array([1.0 / np.prod([points[row] - points[col] for col in range(5) if col != row]) for row in range(5)])
    table = np.zeros((5, 5))
    for row in range(5):
        for col in range(5):
            if row != col:
                table[row, col] = weights[col] / weights[row] / (points[row] - points[col])
        table[row, row] = -np.sum(table[row])
    return table
lift_gain = 10.0
step_size = 0.02
viscosity = 0.05
penalty = 2.0
section_a = -567301805773.0 / 1357537059087.0
section_b = 2404267990393.0 / 2016746695238.0
normal_table_x = np.array([1.0, 0.0, -1.0, 0.0]).reshape(1, 4, 1)
normal_table_y = np.array([0.0, 1.0, 0.0, -1.0]).reshape(1, 4, 1)
value_pairs = [(1, 2)]
grad_pairs = [(2, 4), (3, 5), (0, 1), (2, 3), (4, 5), (6, 7)]

def along_x(values):
    table = jnp.asarray(build_derivative(), jnp.float32)
    return jnp.einsum('ij,cjbm->cibm', table, values, precision=lax.Precision.HIGHEST)

def along_y(values):
    table = jnp.asarray(build_derivative(), jnp.float32)
    return jnp.einsum('ij,cajm->caim', table, values, precision=lax.Precision.HIGHEST)

def face_traces(values):
    return jnp.stack([values[:, 4, :], values[:, :, 4], values[:, 0, :], values[:, :, 0]], axis=2)

def add_faces(total, terms):
    total = total.at[:, 4, :].add(terms[:, :, 0])
    total = total.at[:, :, 4].add(terms[:, :, 1])
    total = total.at[:, 0, :].add(terms[:, :, 2])
    return total.at[:, :, 0].add(terms[:, :, 3])

def align_faces(outer_faces, seam_codes, levels, pairs):
    turn = jnp.repeat(seam_codes % 4, levels, axis=1)[None]
    flipped = jnp.repeat(seam_codes // 4, levels, axis=1)[None, None]
    outer_faces = jnp.where(flipped == 1, outer_faces[:, ::-1], outer_faces)
    cosine = (turn == 0).astype(jnp.float32) - (turn == 2).astype(jnp.float32)
    sine_part = (turn == 1).astype(jnp.float32) - (turn == 3).astype(jnp.float32)
    parts = list(outer_faces)
    for first, second in pairs:
        left, right = (parts[first], parts[second])
        parts[first] = cosine * left - sine_part * right
        parts[second] = sine_part * left + cosine * right
    return jnp.stack(parts)

def gradients(values, inner_faces, outer_faces):
    normal_x = jnp.asarray(normal_table_x, jnp.float32)
    normal_y = jnp.asarray(normal_table_y, jnp.float32)
    half_jump = 0.5 * (outer_faces - inner_faces)
    grad_x = add_faces(along_x(values), lift_gain * half_jump * normal_x)
    grad_y = add_faces(along_y(values), lift_gain * half_jump * normal_y)
    columns = values.shape[3]
    return jnp.stack([grad_x, grad_y], axis=1).reshape(8, 5, 5, columns)

def normal_flux(faces, normal_x, normal_y):
    normal_speed = faces[1] * normal_x + faces[2] * normal_y
    return (jnp.stack([normal_speed, faces[0] * normal_x, faces[0] * normal_y, faces[3] * normal_speed]), normal_speed)

def advance(values, carry_in, gradient, inner_faces, outer_faces, grad_inner, grad_outer):
    normal_x = jnp.asarray(normal_table_x, jnp.float32)
    normal_y = jnp.asarray(normal_table_y, jnp.float32)
    columns = values.shape[3]
    pressure, velocity_u, velocity_v, potential = (values[0], values[1], values[2], values[3])
    split_grad = gradient.reshape(4, 2, 5, 5, columns)
    zeros_field = jnp.zeros_like(pressure)
    flux_x = jnp.stack([velocity_u, pressure, zeros_field, potential * velocity_u]) - viscosity * split_grad[:, 0]
    flux_y = jnp.stack([velocity_v, zeros_field, pressure, potential * velocity_v]) - viscosity * split_grad[:, 1]
    volume = -(along_x(flux_x) + along_y(flux_y))
    flux_in, speed_in = normal_flux(inner_faces, normal_x, normal_y)
    flux_out, speed_out = normal_flux(outer_faces, normal_x, normal_y)
    wave_speed = 1.0 + jnp.maximum(jnp.abs(speed_in), jnp.abs(speed_out))
    split_in = grad_inner.reshape(4, 2, 5, 4, columns)
    split_out = grad_outer.reshape(4, 2, 5, 4, columns)
    slope_in = split_in[:, 0] * normal_x + split_in[:, 1] * normal_y
    slope_out = split_out[:, 0] * normal_x + split_out[:, 1] * normal_y
    visc_star = 0.5 * (slope_in + slope_out) - penalty * (inner_faces - outer_faces)
    flux_star = 0.5 * (flux_in + flux_out) - 0.5 * wave_speed * (outer_faces - inner_faces) - viscosity * visc_star
    flux_own = flux_in - viscosity * slope_in
    tendency = add_faces(volume, lift_gain * (flux_own - flux_star))
    next_carry = section_a * carry_in + step_size * tendency
    return (values + section_b * next_carry, next_carry)

def reference(state, register, neighbor, neighbor_face, seam):
    elems = neighbor.shape[1]
    levels = state.shape[2] // elems
    values_all = state.reshape(4, 5, 5, elems * levels)
    carry_all = register.reshape(4, 5, 5, elems * levels)
    traces = face_traces(values_all).reshape(4, 5, 4 * elems, levels)
    group = E_DEV * STRIPS
    count = elems // group
    columns = group * levels
    source_all = (neighbor_face * elems + neighbor).astype(jnp.int32)

    def block_columns(array, block_id):
        return lax.dynamic_slice_in_dim(array, block_id * columns, columns, axis=3)

    def block_faces(table, block_id):
        return lax.dynamic_slice_in_dim(table, block_id * group, group, axis=1)

    def first_round(block_id):
        values = block_columns(values_all, block_id)
        source = block_faces(source_all, block_id).reshape(-1)
        codes = block_faces(seam, block_id)
        inner_faces = face_traces(values)
        outer_faces = align_faces(traces[:, :, source, :].reshape(4, 5, 4, columns), codes, levels, value_pairs)
        return (values, source, codes, inner_faces, outer_faces)

    def gradient_block(block_id):
        values, source, codes, inner_faces, outer_faces = first_round(block_id)
        return face_traces(gradients(values, inner_faces, outer_faces))
    grad_traces = lax.map(gradient_block, jnp.arange(count, dtype=jnp.int32))
    grad_traces = grad_traces.reshape(count, 8, 5, 4, group, levels).transpose(1, 2, 3, 0, 4, 5).reshape(8, 5, 4 * elems, levels)

    def final_block(block_id):
        values, source, codes, inner_faces, outer_faces = first_round(block_id)
        gradient = gradients(values, inner_faces, outer_faces)
        grad_inner = face_traces(gradient)
        grad_outer = align_faces(grad_traces[:, :, source, :].reshape(8, 5, 4, columns), codes, levels, grad_pairs)
        return advance(values, block_columns(carry_all, block_id), gradient, inner_faces, outer_faces, grad_inner, grad_outer)
    new_values, new_carry = lax.map(final_block, jnp.arange(count, dtype=jnp.int32))
    next_state = new_values.transpose(1, 2, 3, 0, 4).reshape(4, 25, elems * levels)
    next_register = new_carry.transpose(1, 2, 3, 0, 4).reshape(4, 25, elems * levels)
    return (next_state, next_register)
```

```python
import functools
import math

import jax
import jax.numpy as jnp
import ml_dtypes
import numpy as np
from jax import lax
from jax.experimental import pallas as pl
from jax.experimental.pallas import tpu as pltpu
from jax.sharding import PartitionSpec as P

TW = 8
LANES = 128

lift_gain = 10.0
step_size = 0.02
viscosity = 0.05
penalty = 2.0
section_a = -567301805773.0 / 1357537059087.0
section_b = 2404267990393.0 / 2016746695238.0

f32 = jnp.float32
bf16 = jnp.bfloat16


def build_derivative():
    points = np.array([-1.0, -math.sqrt(3.0 / 7.0), 0.0, math.sqrt(3.0 / 7.0), 1.0])
    weights = np.array(
        [
            1.0 / np.prod([points[row] - points[col] for col in range(5) if col != row])
            for row in range(5)
        ]
    )
    table = np.zeros((5, 5))
    for row in range(5):
        for col in range(5):
            if row != col:
                table[row, col] = weights[col] / weights[row] / (points[row] - points[col])
        table[row, row] = -np.sum(table[row])
    return table


def face_node(face, node):
    return [(4, node), (node, 4), (0, node), (node, 0)][face]


def split_const(table):
    high = table.astype(ml_dtypes.bfloat16)
    low = (table - high.astype(np.float64)).astype(ml_dtypes.bfloat16)
    return np.concatenate([high, low, high], axis=1)


def build_tables():
    d = build_derivative()
    eye = np.eye(5)
    dx = np.zeros((32, 32))
    dy = np.zeros((32, 32))
    dx[:25, :25] = np.kron(d, eye)
    dy[:25, :25] = np.kron(eye, d)
    pick = np.zeros((32, 32))
    for face in range(4):
        for node in range(5):
            a, b = face_node(face, node)
            pick[face * 8 + node, a * 5 + b] = 1.0
    normal_x = np.repeat([1.0, 0.0, -1.0, 0.0], 8)
    normal_y = np.repeat([0.0, 1.0, 0.0, -1.0], 8)
    lift_x = pick.T * normal_x[None] * (0.5 * lift_gain)
    lift_y = pick.T * normal_y[None] * (0.5 * lift_gain)
    grad_x = np.concatenate([dx, lift_x], axis=1)
    grad_y = np.concatenate([dy, lift_y], axis=1)
    grad = np.concatenate([grad_x, grad_y, pick @ grad_x, pick @ grad_y], axis=0)
    volume = np.concatenate([-dx, -dy, lift_gain * pick.T], axis=1)
    late = lift_gain * 0.5 * viscosity * pick.T
    out = np.zeros((224, 384), ml_dtypes.bfloat16)
    out[:128, :192] = split_const(grad)
    out[:128, 192:288] = split_const(grad[:, 32:])
    out[128:160, :288] = split_const(volume)
    out[160:192, :96] = split_const(late)
    out[192:224, :32] = pick.astype(ml_dtypes.bfloat16)
    out[192:224, 32:64] = pick.astype(ml_dtypes.bfloat16)
    return out


def halves(x):
    high = x.astype(bf16)
    low = (x - high.astype(f32)).astype(bf16)
    return high, low


def dot(a, b):
    return lax.dot_general(a, b, (((1,), (0,)), ((), ())), preferred_element_type=f32)


def dot_t(a, b):
    return lax.dot_general(a, b, (((1,), (1,)), ((), ())), preferred_element_type=f32)


def dot3(table, x):
    high, low = halves(x)
    return dot(table, jnp.concatenate([high, high, low], axis=0))


def onehot(mask):
    return jnp.where(mask, 1.0, 0.0).astype(bf16)


def permute(x, perm):
    rows = x.shape[0]
    high, low = halves(x)
    both = dot(jnp.concatenate([high, low], axis=0), perm)
    return both[:rows] + both[rows:]


def iota(shape, dim):
    return lax.broadcasted_iota(jnp.int32, shape, dim)


def kernel(
    plan,
    state_hbm,
    neighbor_hbm,
    neighbor_face_hbm,
    seam_hbm,
    tables_hbm,
    change,
    state,
    neighbor,
    neighbor_face,
    seam,
    tables,
    padded,
    sent,
    arrived,
    own_faces,
    early_grads,
    early_change,
    load_sem,
    send_sem,
    recv_sem,
):
    elems, levels, curve_count, strip_count, links, rows_of, offsets = plan
    columns = elems * levels
    inner = LANES // elems
    outer_levels = levels // inner
    groups = 4 * outer_levels
    span = 4 * LANES
    total_rows = offsets[-1] + rows_of[-1]
    link_count = len(links)
    link_rows = -(-link_count // 8) * 8

    curve_pos = lax.axis_index("curve")
    strip_pos = lax.axis_index("sub")
    device_pos = curve_pos * strip_count + strip_pos
    places = []
    for axis, step in links:
        if axis == "curve":
            places.append((lax.rem(curve_pos + step + curve_count, curve_count), strip_pos))
        else:
            places.append((curve_pos, lax.rem(strip_pos + step + strip_count, strip_count)))

    barrier = pltpu.get_barrier_semaphore()
    for place in places:
        pl.semaphore_signal(
            barrier, inc=1, device_id=place, device_id_type=pl.DeviceIdType.MESH
        )
    loads = [
        pltpu.make_async_copy(source_ref, target_ref, load_sem.at[index])
        for index, (source_ref, target_ref) in enumerate(
            [
                (neighbor_hbm, neighbor),
                (neighbor_face_hbm, neighbor_face),
                (seam_hbm, seam),
                (state_hbm, state),
                (tables_hbm, tables),
            ]
        )
    ]
    for load in loads:
        load.start()
    for load in loads[:3]:
        load.wait()

    def widen(ref):
        block = ref[...]
        return jnp.concatenate([block] * inner, axis=1)

    across = widen(neighbor)
    face_back = widen(neighbor_face)
    codes = widen(seam)
    owner = across // elems
    place_in = across % elems
    turn = codes % 4
    flipped = codes // 4
    sub_level = iota((4, LANES), 1) // elems
    position = face_back * LANES + sub_level * elems + place_in
    source = jnp.where(owner == device_pos, position, -1)
    heading = (face_back + turn) % 4
    cosine = jnp.where(turn == 0, 1.0, 0.0) - jnp.where(turn == 2, 1.0, 0.0)
    sine = jnp.where(turn == 3, 1.0, 0.0) - jnp.where(turn == 1, 1.0, 0.0)
    head_x = jnp.where(heading == 0, 1.0, 0.0) - jnp.where(heading == 2, 1.0, 0.0)
    head_y = jnp.where(heading == 1, 1.0, 0.0) - jnp.where(heading == 3, 1.0, 0.0)

    link_iota = iota((link_rows, LANES), 0)
    target = jnp.full((link_rows, LANES), -1, jnp.int32)
    base = jnp.zeros((link_rows, LANES), f32)
    for index, place in enumerate(places):
        target = jnp.where(link_iota == index, place[0] * strip_count + place[1], target)
        base = jnp.where(link_iota == index, float(offsets[index] + 1), base)
    base = base + (iota((link_rows, LANES), 1) // elems).astype(f32)
    member = [
        jnp.where(owner[face : face + 1] == target, 1.0, 0.0) for face in range(4)
    ]
    from_lane = iota((LANES, 2 * LANES), 0)
    to_lane = iota((LANES, 2 * LANES), 1)
    same = from_lane // elems == (to_lane % LANES) // elems
    earlier = same & ((from_lane < to_lane) | (to_lane >= LANES))
    counts = dot(jnp.concatenate(member, axis=0).astype(bf16), onehot(earlier))
    before = jnp.zeros((link_rows, LANES), f32)
    slot_rows = []
    for face in range(4):
        part = counts[face * link_rows : (face + 1) * link_rows]
        rank = part[:, :LANES] + before
        before = before + part[:, LANES:]
        slot_rows.append(
            jnp.sum(member[face] * (base + inner * rank), axis=0, keepdims=True)
        )
    slot_row = jnp.concatenate(slot_rows, axis=1)
    pack = onehot(
        (iota((total_rows, span), 0) + 1).astype(f32)
        == jnp.broadcast_to(slot_row, (total_rows, span))
    )
    pack2 = jnp.concatenate([pack, pack], axis=1)

    def local_table():
        span_iota = iota((span, LANES), 0)
        return jnp.concatenate(
            [onehot(span_iota == source[face : face + 1]) for face in range(4)], axis=1
        )

    meta_iota = iota((8, LANES), 0)
    meta_blocks = []
    for face in range(4):
        block = jnp.zeros((8, LANES), f32)
        for row, values in enumerate(
            [flipped.astype(f32), cosine, sine, (position + 1).astype(f32)]
        ):
            block = jnp.where(meta_iota == row, values[face : face + 1], block)
        meta_blocks.append(block)
    meta = jnp.concatenate(meta_blocks, axis=1)
    heads_x = jnp.concatenate(
        [jnp.broadcast_to(head_x[face : face + 1], (8, LANES)) for face in range(4)], axis=0
    )
    heads_y = jnp.concatenate(
        [jnp.broadcast_to(head_y[face : face + 1], (8, LANES)) for face in range(4)], axis=0
    )

    def to_exchange(faces):
        return jnp.concatenate(
            [
                jnp.concatenate(
                    [
                        faces[face * 8 : face * 8 + 8, group * LANES : (group + 1) * LANES]
                        for face in range(4)
                    ],
                    axis=1,
                )
                for group in range(groups)
            ],
            axis=0,
        )

    def from_exchange(block):
        return jnp.concatenate(
            [
                jnp.concatenate(
                    [
                        block[group * 8 : group * 8 + 8, face * LANES : (face + 1) * LANES]
                        for group in range(groups)
                    ],
                    axis=1,
                )
                for face in range(4)
            ],
            axis=0,
        )

    data_lanes = groups * 8
    field_lanes = outer_levels * 8
    lane = iota((total_rows, LANES), 1)
    node_lane = lane % 8
    in_data = lane < data_lanes

    def copy_of(turn_index, index):
        rows = pl.ds(offsets[index], rows_of[index])
        return pltpu.make_async_remote_copy(
            src_ref=sent.at[turn_index, rows],
            dst_ref=arrived.at[turn_index, rows],
            send_sem=send_sem.at[turn_index, index],
            recv_sem=recv_sem.at[turn_index, index],
            device_id=places[index],
            device_id_type=pl.DeviceIdType.MESH,
        )

    def post(turn_index, block, flags):
        if flags is None:
            pieces = [block, meta]
            if data_lanes + 8 < LANES:
                pieces.append(jnp.zeros((LANES - data_lanes - 8, span), f32))
            block = jnp.concatenate(pieces, axis=0)
        high, low = halves(block)
        message = dot_t(pack2, jnp.concatenate([high, low], axis=1))
        if flags is None:
            flags = [
                jnp.broadcast_to(
                    message[:, data_lanes + index : data_lanes + index + 1], message.shape
                )
                for index in range(3)
            ]
        else:
            rest = jnp.zeros((total_rows, LANES - data_lanes), f32)
            message = jnp.concatenate([message, rest], axis=1)
        flip, cos, sin = flags
        mirrored = message
        for node, shift in ((0, LANES - 4), (1, LANES - 2), (3, 2), (4, 4)):
            mirrored = jnp.where(
                node_lane == node, pltpu.roll(message, shift, axis=1), mirrored
            )
        aligned = jnp.where(in_data & (flip > 0.5), mirrored, message)
        field = lane // field_lanes
        turned_u = cos * aligned - sin * pltpu.roll(aligned, LANES - field_lanes, axis=1)
        turned_v = cos * aligned + sin * pltpu.roll(aligned, field_lanes, axis=1)
        aligned = jnp.where(field == 1, turned_u, jnp.where(field == 2, turned_v, aligned))
        sent[turn_index] = aligned
        if turn_index == 0:
            pl.semaphore_wait(barrier, link_count)
        for index in range(link_count):
            copy_of(turn_index, index).start()
        return flags

    def gather_local(block):
        rows = block.shape[0]
        high, low = halves(block)
        both = dot(jnp.concatenate([high, low], axis=0), local_table())
        return both[:rows] + both[rows:]

    def await_all(turn_index):
        for index in range(link_count):
            copy_of(turn_index, index).wait_recv()

    def spread_table():
        message = arrived[0]
        spot = jnp.broadcast_to(
            message[:, data_lanes + 3 : data_lanes + 4], (total_rows, span)
        )
        return onehot((iota((total_rows, span), 1) + 1).astype(f32) == spot)

    def collect(turn_index, spread):
        message = arrived[turn_index]
        high, low = halves(jnp.transpose(message)[:data_lanes])
        both = dot(jnp.concatenate([high, low], axis=0), spread)
        return both[:data_lanes] + both[data_lanes:]

    row = iota((columns, columns), 0)
    col = iota((columns, columns), 1)
    to_level = onehot(row == (col % elems) * levels + col // elems)
    to_elem = onehot(row == (col % levels) * elems + col // levels)

    padded[...] = jnp.zeros_like(padded)
    for load in loads[3:]:
        load.wait()
    for field in range(4):
        padded[field, :25] = state[:, field, :]
    nodal = permute(padded[...].reshape(128, columns), to_level)
    values = jnp.concatenate(
        [nodal[field * 32 : field * 32 + 32] for field in range(4)], axis=1
    )
    high, low = halves(values)
    faces_in = dot(tables[192:224, :64], jnp.concatenate([high, low], axis=0))

    def fields_of(wide):
        return [wide[:, field * columns : (field + 1) * columns] for field in range(4)]

    def elementwise_lanes(wide):
        return permute(jnp.concatenate(fields_of(wide), axis=0), to_elem)

    def early_part(values, faces_in, faces_out, grad_x, grad_y, face_gx, face_gy, own_slope):
        face_of_row = iota((32, columns), 0) // 8
        normal_x = jnp.where(face_of_row == 0, 1.0, 0.0) - jnp.where(face_of_row == 2, 1.0, 0.0)
        normal_y = jnp.where(face_of_row == 1, 1.0, 0.0) - jnp.where(face_of_row == 3, 1.0, 0.0)

        def flux_of(faces):
            speed = faces[1] * normal_x + faces[2] * normal_y
            return [speed, faces[0] * normal_x, faces[0] * normal_y, faces[3] * speed], speed

        inside, outside = fields_of(faces_in), fields_of(faces_out)
        gx_in, gy_in = fields_of(face_gx), fields_of(face_gy)
        slope_own = fields_of(own_slope)
        flux_in, speed_in = flux_of(inside)
        flux_out, speed_out = flux_of(outside)
        wave = 1.0 + jnp.maximum(jnp.abs(speed_in), jnp.abs(speed_out))
        terms = []
        for field in range(4):
            slope_in = gx_in[field] * normal_x + gy_in[field] * normal_y
            jump = outside[field] - inside[field]
            terms.append(
                0.5 * (flux_in[field] - flux_out[field])
                - 0.5 * viscosity * (slope_in - slope_own[field])
                + (0.5 * wave + viscosity * penalty) * jump
            )
        face_term = jnp.concatenate(terms, axis=1)
        pressure, vel_u, vel_v, theta = fields_of(values)
        nothing = jnp.zeros_like(pressure)
        flux_x = jnp.concatenate([vel_u, pressure, nothing, theta * vel_u], axis=1)
        flux_y = jnp.concatenate([vel_v, nothing, pressure, theta * vel_v], axis=1)
        tendency = dot3(
            tables[128:160, :288],
            jnp.concatenate(
                [flux_x - viscosity * grad_x, flux_y - viscosity * grad_y, face_term], axis=0
            ),
        )

        return elementwise_lanes(tendency)

    block_in = to_exchange(faces_in)
    flags = post(0, block_in, None)
    always = device_pos >= 0

    @pl.when(always)
    def _():
        own = from_exchange(gather_local(block_in))
        own_faces[...] = own
        early_grads[...] = dot3(
            tables[:128, :192], jnp.concatenate([values, own - faces_in], axis=0)
        )

    await_all(0)
    spread = spread_table()
    far_faces = from_exchange(collect(0, spread))
    face_grads = early_grads[64:128] + dot3(tables[64:128, 192:288], far_faces)
    face_gx, face_gy = face_grads[:32], face_grads[32:]
    wide_x = jnp.concatenate([heads_x] * groups, axis=1)
    wide_y = jnp.concatenate([heads_y] * groups, axis=1)
    block_grad = to_exchange(face_gx * wide_x + face_gy * wide_y)
    post(1, block_grad, flags)

    @pl.when(always)
    def _():
        own_slope = from_exchange(gather_local(block_grad))
        grads = early_grads[:64] + dot3(tables[:64, 192:288], far_faces)
        faces_out = own_faces[...] + far_faces
        grad_x, grad_y = grads[:32], grads[32:]
        early_change[...] = early_part(
            values, faces_in, faces_out, grad_x, grad_y, face_gx, face_gy, own_slope
        )

    await_all(1)
    far_slope = from_exchange(collect(1, spread))
    late = elementwise_lanes(dot3(tables[160:192, :96], far_slope))
    total = early_change[...] + late
    for field in range(4):
        change[:, field, :] = step_size * total[field * 32 : field * 32 + 25]

    for turn_index in range(2):
        for index in range(link_count):
            copy_of(turn_index, index).wait_send()


def body(curve_count, strip_count, state, register, neighbor, neighbor_face, seam):
    elems = neighbor.shape[1]
    levels = state.shape[2] // elems
    inner = LANES // elems
    reach = min(7, (curve_count - 1) // 2)
    slots = (TW + reach - 1) // reach
    links, rows_of = [], []
    for distance in range(reach, 0, -1):
        for direction in (1, -1):
            links.append(("curve", direction * distance))
            rows_of.append(-(-slots * inner // 8) * 8)
    for direction in (1, -1):
        links.append(("sub", direction))
        rows_of.append(-(-TW * inner // 8) * 8)
    offsets = [sum(rows_of[:index]) for index in range(len(links))]
    total_rows = sum(rows_of)
    plan = (elems, levels, curve_count, strip_count, links, rows_of, offsets)
    vmem = pl.BlockSpec(memory_space=pltpu.VMEM)
    nodes_first = jnp.transpose(state, (1, 0, 2))
    operands = (nodes_first, neighbor, neighbor_face, seam, jnp.asarray(build_tables()))
    change = pl.pallas_call(
        functools.partial(kernel, plan),
        out_shape=pltpu.VMEM(nodes_first.shape, f32),
        in_specs=[pl.BlockSpec(memory_space=pl.ANY)] * 5,
        out_specs=vmem,
        scratch_shapes=[
            pltpu.VMEM(nodes_first.shape, f32),
            pltpu.VMEM(neighbor.shape, jnp.int32),
            pltpu.VMEM(neighbor.shape, jnp.int32),
            pltpu.VMEM(neighbor.shape, jnp.int32),
            pltpu.VMEM((224, 384), bf16),
            pltpu.VMEM((4, 32, state.shape[2]), f32),
            pltpu.VMEM((2, total_rows, LANES), f32),
            pltpu.VMEM((2, total_rows, LANES), f32),
            pltpu.VMEM((32, 4 * state.shape[2]), f32),
            pltpu.VMEM((128, 4 * state.shape[2]), f32),
            pltpu.VMEM((128, state.shape[2]), f32),
            pltpu.SemaphoreType.DMA((5,)),
            pltpu.SemaphoreType.DMA((2, len(links))),
            pltpu.SemaphoreType.DMA((2, len(links))),
        ],
        compiler_params=pltpu.CompilerParams(collective_id=0, has_side_effects=True),
    )(*[pltpu.with_memory_space_constraint(operand, pltpu.HBM) for operand in operands])
    next_register = section_a * register + jnp.transpose(change, (1, 0, 2))
    return state + section_b * next_register, next_register


def solution(mesh):
    wide = P(None, None, ("curve", "sub"))
    flat = P(None, ("curve", "sub"))
    return jax.shard_map(
        functools.partial(body, mesh.shape["curve"], mesh.shape["sub"]),
        mesh=mesh,
        in_specs=(wide, wide, flat, flat, flat),
        out_specs=(wide, wide),
        check_vma=False,
    )
```

```python
import functools
import math

import jax
import jax.numpy as jnp
import ml_dtypes
import numpy as np
from jax import lax
from jax.experimental import pallas as pl
from jax.experimental.pallas import tpu as pltpu
from jax.sharding import PartitionSpec as P

TW = 8
LANES = 128
DIRECT_LIMIT = 64

lift_gain = 10.0
step_size = 0.02
viscosity = 0.05
penalty = 2.0
section_a = -567301805773.0 / 1357537059087.0
section_b = 2404267990393.0 / 2016746695238.0

f32 = jnp.float32
bf16 = jnp.bfloat16


def build_derivative():
    points = np.array([-1.0, -math.sqrt(3.0 / 7.0), 0.0, math.sqrt(3.0 / 7.0), 1.0])
    weights = np.array(
        [
            1.0 / np.prod([points[row] - points[col] for col in range(5) if col != row])
            for row in range(5)
        ]
    )
    table = np.zeros((5, 5))
    for row in range(5):
        for col in range(5):
            if row != col:
                table[row, col] = weights[col] / weights[row] / (points[row] - points[col])
        table[row, row] = -np.sum(table[row])
    return table


def face_node(face, node):
    return [(4, node), (node, 4), (0, node), (node, 0)][face]


def split_const(table):
    high = table.astype(ml_dtypes.bfloat16)
    low = (table - high.astype(np.float64)).astype(ml_dtypes.bfloat16)
    return np.concatenate([high, low, high], axis=1)


def element_tables():
    d = build_derivative()
    eye = np.eye(5)
    dx = np.zeros((32, 32))
    dy = np.zeros((32, 32))
    dx[:25, :25] = np.kron(d, eye)
    dy[:25, :25] = np.kron(eye, d)
    pick = np.zeros((32, 32))
    for face in range(4):
        for node in range(5):
            a, b = face_node(face, node)
            pick[face * 8 + node, a * 5 + b] = 1.0
    normal_x = np.repeat([1.0, 0.0, -1.0, 0.0], 8)
    normal_y = np.repeat([0.0, 1.0, 0.0, -1.0], 8)
    lift_x = pick.T * normal_x[None] * (0.5 * lift_gain)
    lift_y = pick.T * normal_y[None] * (0.5 * lift_gain)
    return dx, dy, pick, normal_x, normal_y, lift_x, lift_y


def build_tables():
    dx, dy, pick, _, _, lift_x, lift_y = element_tables()
    grad_x = np.concatenate([dx, lift_x], axis=1)
    grad_y = np.concatenate([dy, lift_y], axis=1)
    grad = np.concatenate([grad_x, grad_y, pick @ grad_x, pick @ grad_y], axis=0)
    volume = np.concatenate([-dx, -dy, lift_gain * pick.T], axis=1)
    late = lift_gain * 0.5 * viscosity * pick.T
    out = np.zeros((224, 384), ml_dtypes.bfloat16)
    out[:128, :192] = split_const(grad)
    out[:128, 192:288] = split_const(grad[:, 32:])
    out[128:160, :288] = split_const(volume)
    out[160:192, :96] = split_const(late)
    out[192:224, :32] = pick.astype(ml_dtypes.bfloat16)
    out[192:224, 32:64] = pick.astype(ml_dtypes.bfloat16)
    return out


def build_direct_tables():
    dx, dy, pick, normal_x, normal_y, lift_x, lift_y = element_tables()
    slope = normal_x[:, None] * (pick @ dx) + normal_y[:, None] * (pick @ dy)
    base = np.concatenate([-dx, -dy, viscosity * (dx @ dx + dy @ dy)], axis=1)
    jump = viscosity * (dx @ lift_x + dy @ lift_y)
    late = np.concatenate([lift_gain * pick.T, jump], axis=1)
    out = np.zeros((128, 384), ml_dtypes.bfloat16)
    out[:64, :96] = split_const(np.concatenate([pick, slope], axis=0))
    out[64:96, :288] = split_const(base)
    out[96:128, :192] = split_const(late)
    return out


def halves(x):
    high = x.astype(bf16)
    low = (x - high.astype(f32)).astype(bf16)
    return high, low


def dot(a, b):
    return lax.dot_general(a, b, (((1,), (0,)), ((), ())), preferred_element_type=f32)


def dot_t(a, b):
    return lax.dot_general(a, b, (((1,), (1,)), ((), ())), preferred_element_type=f32)


def dot3(table, x):
    high, low = halves(x)
    return dot(table, jnp.concatenate([high, high, low], axis=0))


def onehot(mask):
    return jnp.where(mask, 1.0, 0.0).astype(bf16)


def permute(x, perm):
    rows = x.shape[0]
    high, low = halves(x)
    both = dot(jnp.concatenate([high, low], axis=0), perm)
    return both[:rows] + both[rows:]


def iota(shape, dim):
    return lax.broadcasted_iota(jnp.int32, shape, dim)


def two_round_kernel(
    plan,
    state_hbm,
    neighbor_hbm,
    neighbor_face_hbm,
    seam_hbm,
    tables_hbm,
    change,
    state,
    neighbor,
    neighbor_face,
    seam,
    tables,
    padded,
    sent,
    arrived,
    own_faces,
    early_grads,
    early_change,
    load_sem,
    send_sem,
    recv_sem,
):
    elems, levels, curve_count, strip_count, links, rows_of, offsets = plan
    columns = elems * levels
    inner = LANES // elems
    outer_levels = levels // inner
    groups = 4 * outer_levels
    span = 4 * LANES
    total_rows = offsets[-1] + rows_of[-1]
    link_count = len(links)
    link_rows = -(-link_count // 8) * 8

    curve_pos = lax.axis_index("curve")
    strip_pos = lax.axis_index("sub")
    device_pos = curve_pos * strip_count + strip_pos
    places = []
    for axis, step in links:
        if axis == "curve":
            places.append((lax.rem(curve_pos + step + curve_count, curve_count), strip_pos))
        else:
            places.append((curve_pos, lax.rem(strip_pos + step + strip_count, strip_count)))

    barrier = pltpu.get_barrier_semaphore()
    for place in places:
        pl.semaphore_signal(
            barrier, inc=1, device_id=place, device_id_type=pl.DeviceIdType.MESH
        )
    loads = [
        pltpu.make_async_copy(source_ref, target_ref, load_sem.at[index])
        for index, (source_ref, target_ref) in enumerate(
            [
                (neighbor_hbm, neighbor),
                (neighbor_face_hbm, neighbor_face),
                (seam_hbm, seam),
                (state_hbm, state),
                (tables_hbm, tables),
            ]
        )
    ]
    for load in loads:
        load.start()
    for load in loads[:3]:
        load.wait()

    def widen(ref):
        block = ref[...]
        return jnp.concatenate([block] * inner, axis=1)

    across = widen(neighbor)
    face_back = widen(neighbor_face)
    codes = widen(seam)
    owner = across // elems
    place_in = across % elems
    turn = codes % 4
    flipped = codes // 4
    sub_level = iota((4, LANES), 1) // elems
    position = face_back * LANES + sub_level * elems + place_in
    source = jnp.where(owner == device_pos, position, -1)
    heading = (face_back + turn) % 4
    cosine = jnp.where(turn == 0, 1.0, 0.0) - jnp.where(turn == 2, 1.0, 0.0)
    sine = jnp.where(turn == 3, 1.0, 0.0) - jnp.where(turn == 1, 1.0, 0.0)
    head_x = jnp.where(heading == 0, 1.0, 0.0) - jnp.where(heading == 2, 1.0, 0.0)
    head_y = jnp.where(heading == 1, 1.0, 0.0) - jnp.where(heading == 3, 1.0, 0.0)

    link_iota = iota((link_rows, LANES), 0)
    target = jnp.full((link_rows, LANES), -1, jnp.int32)
    base = jnp.zeros((link_rows, LANES), f32)
    for index, place in enumerate(places):
        target = jnp.where(link_iota == index, place[0] * strip_count + place[1], target)
        base = jnp.where(link_iota == index, float(offsets[index] + 1), base)
    base = base + (iota((link_rows, LANES), 1) // elems).astype(f32)
    member = [
        jnp.where(owner[face : face + 1] == target, 1.0, 0.0) for face in range(4)
    ]
    from_lane = iota((LANES, 2 * LANES), 0)
    to_lane = iota((LANES, 2 * LANES), 1)
    same = from_lane // elems == (to_lane % LANES) // elems
    earlier = same & ((from_lane < to_lane) | (to_lane >= LANES))
    counts = dot(jnp.concatenate(member, axis=0).astype(bf16), onehot(earlier))
    before = jnp.zeros((link_rows, LANES), f32)
    slot_rows = []
    for face in range(4):
        part = counts[face * link_rows : (face + 1) * link_rows]
        rank = part[:, :LANES] + before
        before = before + part[:, LANES:]
        slot_rows.append(
            jnp.sum(member[face] * (base + inner * rank), axis=0, keepdims=True)
        )
    slot_row = jnp.concatenate(slot_rows, axis=1)
    pack = onehot(
        (iota((total_rows, span), 0) + 1).astype(f32)
        == jnp.broadcast_to(slot_row, (total_rows, span))
    )
    pack2 = jnp.concatenate([pack, pack], axis=1)

    def local_table():
        span_iota = iota((span, LANES), 0)
        return jnp.concatenate(
            [onehot(span_iota == source[face : face + 1]) for face in range(4)], axis=1
        )

    meta_iota = iota((8, LANES), 0)
    meta_blocks = []
    for face in range(4):
        block = jnp.zeros((8, LANES), f32)
        for row, values in enumerate(
            [flipped.astype(f32), cosine, sine, (position + 1).astype(f32)]
        ):
            block = jnp.where(meta_iota == row, values[face : face + 1], block)
        meta_blocks.append(block)
    meta = jnp.concatenate(meta_blocks, axis=1)
    heads_x = jnp.concatenate(
        [jnp.broadcast_to(head_x[face : face + 1], (8, LANES)) for face in range(4)], axis=0
    )
    heads_y = jnp.concatenate(
        [jnp.broadcast_to(head_y[face : face + 1], (8, LANES)) for face in range(4)], axis=0
    )

    def to_exchange(faces):
        return jnp.concatenate(
            [
                jnp.concatenate(
                    [
                        faces[face * 8 : face * 8 + 8, group * LANES : (group + 1) * LANES]
                        for face in range(4)
                    ],
                    axis=1,
                )
                for group in range(groups)
            ],
            axis=0,
        )

    def from_exchange(block):
        return jnp.concatenate(
            [
                jnp.concatenate(
                    [
                        block[group * 8 : group * 8 + 8, face * LANES : (face + 1) * LANES]
                        for group in range(groups)
                    ],
                    axis=1,
                )
                for face in range(4)
            ],
            axis=0,
        )

    data_lanes = groups * 8
    field_lanes = outer_levels * 8
    lane = iota((total_rows, LANES), 1)
    node_lane = lane % 8
    in_data = lane < data_lanes

    def copy_of(turn_index, index):
        rows = pl.ds(offsets[index], rows_of[index])
        return pltpu.make_async_remote_copy(
            src_ref=sent.at[turn_index, rows],
            dst_ref=arrived.at[turn_index, rows],
            send_sem=send_sem.at[turn_index, index],
            recv_sem=recv_sem.at[turn_index, index],
            device_id=places[index],
            device_id_type=pl.DeviceIdType.MESH,
        )

    def post(turn_index, block, flags):
        if flags is None:
            pieces = [block, meta]
            if data_lanes + 8 < LANES:
                pieces.append(jnp.zeros((LANES - data_lanes - 8, span), f32))
            block = jnp.concatenate(pieces, axis=0)
        high, low = halves(block)
        message = dot_t(pack2, jnp.concatenate([high, low], axis=1))
        if flags is None:
            flags = [
                jnp.broadcast_to(
                    message[:, data_lanes + index : data_lanes + index + 1], message.shape
                )
                for index in range(3)
            ]
        else:
            rest = jnp.zeros((total_rows, LANES - data_lanes), f32)
            message = jnp.concatenate([message, rest], axis=1)
        flip, cos, sin = flags
        mirrored = message
        for node, shift in ((0, LANES - 4), (1, LANES - 2), (3, 2), (4, 4)):
            mirrored = jnp.where(
                node_lane == node, pltpu.roll(message, shift, axis=1), mirrored
            )
        aligned = jnp.where(in_data & (flip > 0.5), mirrored, message)
        field = lane // field_lanes
        turned_u = cos * aligned - sin * pltpu.roll(aligned, LANES - field_lanes, axis=1)
        turned_v = cos * aligned + sin * pltpu.roll(aligned, field_lanes, axis=1)
        aligned = jnp.where(field == 1, turned_u, jnp.where(field == 2, turned_v, aligned))
        sent[turn_index] = aligned
        if turn_index == 0:
            pl.semaphore_wait(barrier, link_count)
        for index in range(link_count):
            copy_of(turn_index, index).start()
        return flags

    def gather_local(block):
        rows = block.shape[0]
        high, low = halves(block)
        both = dot(jnp.concatenate([high, low], axis=0), local_table())
        return both[:rows] + both[rows:]

    def await_all(turn_index):
        for index in range(link_count):
            copy_of(turn_index, index).wait_recv()

    def spread_table():
        message = arrived[0]
        spot = jnp.broadcast_to(
            message[:, data_lanes + 3 : data_lanes + 4], (total_rows, span)
        )
        return onehot((iota((total_rows, span), 1) + 1).astype(f32) == spot)

    def collect(turn_index, spread):
        message = arrived[turn_index]
        high, low = halves(jnp.transpose(message)[:data_lanes])
        both = dot(jnp.concatenate([high, low], axis=0), spread)
        return both[:data_lanes] + both[data_lanes:]

    row = iota((columns, columns), 0)
    col = iota((columns, columns), 1)
    to_level = onehot(row == (col % elems) * levels + col // elems)
    to_elem = onehot(row == (col % levels) * elems + col // levels)

    padded[...] = jnp.zeros_like(padded)
    for load in loads[3:]:
        load.wait()
    for field in range(4):
        padded[field, :25] = state[:, field, :]
    nodal = permute(padded[...].reshape(128, columns), to_level)
    values = jnp.concatenate(
        [nodal[field * 32 : field * 32 + 32] for field in range(4)], axis=1
    )
    high, low = halves(values)
    faces_in = dot(tables[192:224, :64], jnp.concatenate([high, low], axis=0))

    def fields_of(wide):
        return [wide[:, field * columns : (field + 1) * columns] for field in range(4)]

    def elementwise_lanes(wide):
        return permute(jnp.concatenate(fields_of(wide), axis=0), to_elem)

    def early_part(values, faces_in, faces_out, grad_x, grad_y, face_gx, face_gy, own_slope):
        face_of_row = iota((32, columns), 0) // 8
        normal_x = jnp.where(face_of_row == 0, 1.0, 0.0) - jnp.where(face_of_row == 2, 1.0, 0.0)
        normal_y = jnp.where(face_of_row == 1, 1.0, 0.0) - jnp.where(face_of_row == 3, 1.0, 0.0)

        def flux_of(faces):
            speed = faces[1] * normal_x + faces[2] * normal_y
            return [speed, faces[0] * normal_x, faces[0] * normal_y, faces[3] * speed], speed

        inside, outside = fields_of(faces_in), fields_of(faces_out)
        gx_in, gy_in = fields_of(face_gx), fields_of(face_gy)
        slope_own = fields_of(own_slope)
        flux_in, speed_in = flux_of(inside)
        flux_out, speed_out = flux_of(outside)
        wave = 1.0 + jnp.maximum(jnp.abs(speed_in), jnp.abs(speed_out))
        terms = []
        for field in range(4):
            slope_in = gx_in[field] * normal_x + gy_in[field] * normal_y
            jump = outside[field] - inside[field]
            terms.append(
                0.5 * (flux_in[field] - flux_out[field])
                - 0.5 * viscosity * (slope_in - slope_own[field])
                + (0.5 * wave + viscosity * penalty) * jump
            )
        face_term = jnp.concatenate(terms, axis=1)
        pressure, vel_u, vel_v, theta = fields_of(values)
        nothing = jnp.zeros_like(pressure)
        flux_x = jnp.concatenate([vel_u, pressure, nothing, theta * vel_u], axis=1)
        flux_y = jnp.concatenate([vel_v, nothing, pressure, theta * vel_v], axis=1)
        tendency = dot3(
            tables[128:160, :288],
            jnp.concatenate(
                [flux_x - viscosity * grad_x, flux_y - viscosity * grad_y, face_term], axis=0
            ),
        )

        return elementwise_lanes(tendency)

    block_in = to_exchange(faces_in)
    flags = post(0, block_in, None)
    always = device_pos >= 0

    @pl.when(always)
    def _():
        own = from_exchange(gather_local(block_in))
        own_faces[...] = own
        early_grads[...] = dot3(
            tables[:128, :192], jnp.concatenate([values, own - faces_in], axis=0)
        )

    await_all(0)
    spread = spread_table()
    far_faces = from_exchange(collect(0, spread))
    face_grads = early_grads[64:128] + dot3(tables[64:128, 192:288], far_faces)
    face_gx, face_gy = face_grads[:32], face_grads[32:]
    wide_x = jnp.concatenate([heads_x] * groups, axis=1)
    wide_y = jnp.concatenate([heads_y] * groups, axis=1)
    block_grad = to_exchange(face_gx * wide_x + face_gy * wide_y)
    post(1, block_grad, flags)

    @pl.when(always)
    def _():
        own_slope = from_exchange(gather_local(block_grad))
        grads = early_grads[:64] + dot3(tables[:64, 192:288], far_faces)
        faces_out = own_faces[...] + far_faces
        grad_x, grad_y = grads[:32], grads[32:]
        early_change[...] = early_part(
            values, faces_in, faces_out, grad_x, grad_y, face_gx, face_gy, own_slope
        )

    await_all(1)
    far_slope = from_exchange(collect(1, spread))
    late = elementwise_lanes(dot3(tables[160:192, :96], far_slope))
    total = early_change[...] + late
    for field in range(4):
        change[:, field, :] = total[field * 32 : field * 32 + 25]

    for turn_index in range(2):
        for index in range(link_count):
            copy_of(turn_index, index).wait_send()


def direct_kernel(
    plan,
    state_hbm,
    neighbor_hbm,
    neighbor_face_hbm,
    seam_hbm,
    tables_hbm,
    change,
    sideways,
    state,
    neighbor,
    neighbor_face,
    seam,
    tables,
    padded,
    sent,
    arrived,
    notice,
    notices,
    spread,
    known,
    base_change,
    load_sem,
    send_sem,
    recv_sem,
    notice_send_sem,
    notice_recv_sem,
):
    elems, levels, curve_count, strip_count, links, rows_of, offsets = plan
    columns = elems * levels
    span = 4 * columns
    inner = LANES // elems
    outer_levels = levels // inner
    total_rows = offsets[-1] + rows_of[-1]
    link_count = len(links)
    link_rows = -(-link_count // 8) * 8
    half = LANES // outer_levels

    curve_pos = lax.axis_index("curve")
    strip_pos = lax.axis_index("sub")
    device_pos = curve_pos * strip_count + strip_pos

    def place_at(curve_step, strip_step):
        return (
            lax.rem(curve_pos + curve_step + curve_count, curve_count),
            lax.rem(strip_pos + strip_step + strip_count, strip_count),
        )

    places = [place_at(step, 0) if axis == "curve" else place_at(0, step) for axis, step in links]
    others = [
        place_at(curve_step, strip_step)
        for curve_step in range(curve_count)
        for strip_step in range(strip_count)
        if curve_step or strip_step
    ]

    barrier = pltpu.get_barrier_semaphore()
    for place in others:
        pl.semaphore_signal(
            barrier, inc=1, device_id=place, device_id_type=pl.DeviceIdType.MESH
        )
    loads = [
        pltpu.make_async_copy(source_ref, target_ref, load_sem.at[index])
        for index, (source_ref, target_ref) in enumerate(
            [
                (neighbor_hbm, neighbor),
                (neighbor_face_hbm, neighbor_face),
                (seam_hbm, seam),
                (state_hbm, state),
                (tables_hbm, tables),
            ]
        )
    ]
    for load in loads:
        load.start()
    padded[...] = jnp.zeros_like(padded)

    def copy_of(index):
        rows = pl.ds(offsets[index], rows_of[index])
        return pltpu.make_async_remote_copy(
            src_ref=sent.at[rows],
            dst_ref=arrived.at[rows],
            send_sem=send_sem.at[index],
            recv_sem=recv_sem.at[index],
            device_id=places[index],
            device_id_type=pl.DeviceIdType.MESH,
        )

    def notice_of(index):
        return pltpu.make_async_remote_copy(
            src_ref=notice.at[pl.ds(0, 1)],
            dst_ref=notices.at[pl.ds(index, 1)],
            send_sem=notice_send_sem.at[index],
            recv_sem=notice_recv_sem.at[index],
            device_id=others[index],
            device_id_type=pl.DeviceIdType.MESH,
        )

    for load in loads[:3]:
        load.wait()

    def widen(ref):
        block = ref[...]
        return jnp.concatenate([block] * inner, axis=1)

    across = widen(neighbor)
    face_back = widen(neighbor_face)
    codes = widen(seam)
    owner = across // elems
    place_in = across % elems
    turn = codes % 4
    flipped = codes // 4
    own_face = iota((4, LANES), 0)
    quarter = (face_back + turn - own_face + 4) % 4
    odd = jnp.where(quarter % 2 == 1, 1.0, 0.0)
    notice[...] = jnp.broadcast_to(jnp.sum(odd, axis=0, keepdims=True), (8, LANES))
    side = jnp.where(quarter == 0, 1.0, -1.0)
    cosine = jnp.where(turn == 0, 1.0, 0.0) - jnp.where(turn == 2, 1.0, 0.0)
    sine = jnp.where(turn == 3, 1.0, 0.0) - jnp.where(turn == 1, 1.0, 0.0)

    link_iota = iota((link_rows, LANES), 0)
    target = jnp.full((link_rows, LANES), -1, jnp.int32)
    base = jnp.zeros((link_rows, LANES), f32)
    base_back = jnp.zeros((link_rows, LANES), f32)
    for index, place in enumerate(places):
        here = link_iota == index
        target = jnp.where(here, place[0] * strip_count + place[1], target)
        base = jnp.where(here, float(offsets[index] + 1), base)
        base_back = jnp.where(here, float(offsets[index ^ 1] + 1), base_back)
    member = [
        jnp.where(owner[face : face + 1] == target, 1.0, 0.0) for face in range(4)
    ]
    from_lane = iota((LANES, 2 * LANES), 0)
    to_lane = iota((LANES, 2 * LANES), 1)
    same = from_lane // elems == (to_lane % LANES) // elems
    earlier = same & ((from_lane < to_lane) | (to_lane >= LANES))
    counts = dot(jnp.concatenate(member, axis=0).astype(bf16), onehot(earlier))
    before = jnp.zeros((link_rows, LANES), f32)
    slot_rows = []
    for face in range(4):
        part = counts[face * link_rows : (face + 1) * link_rows]
        rank = part[:, :LANES] + before
        before = before + part[:, LANES:]
        slot_rows.append(
            jnp.sum(member[face] * (base + inner * rank), axis=0, keepdims=True)
        )

    stretch = onehot(iota((LANES, columns), 0) == iota((LANES, columns), 1) // levels)

    def stretched(per_face):
        rows = []
        for values in per_face:
            rows.append(values)
            rows.append(jnp.zeros_like(values))
        wide = dot(jnp.concatenate(rows, axis=0).astype(bf16), stretch)
        return [wide[8 * index : 8 * index + 8] for index in range(len(per_face))]

    slot, flip_wide, cos_wide, sin_wide, side_wide = stretched(
        [jnp.concatenate(slot_rows, axis=0), flipped.astype(f32), cosine, sine, side]
    )
    level = iota((8, columns), 1) % levels

    def rows_for(slot, stride):
        spot = slot + (level % inner + level // inner * stride).astype(f32)
        return jnp.where(slot > 0.5, spot, 0.0)

    def hot_rows(count, spots):
        count_iota = (iota((count, columns), 0) + 1).astype(f32)
        return jnp.concatenate(
            [
                onehot(
                    count_iota == jnp.broadcast_to(spots[face : face + 1], (count, columns))
                )
                for face in range(4)
            ],
            axis=1,
        )

    pack = hot_rows(outer_levels * total_rows, rows_for(slot, total_rows))

    def over_faces(wide, rows):
        return jnp.concatenate(
            [jnp.broadcast_to(wide[face : face + 1], (rows, columns)) for face in range(4)],
            axis=1,
        )

    def to_fields(block):
        return jnp.concatenate(
            [
                jnp.concatenate(
                    [
                        block[face * 8 : face * 8 + 8, field * columns : (field + 1) * columns]
                        for face in range(4)
                    ],
                    axis=1,
                )
                for field in range(4)
            ],
            axis=0,
        )

    def to_faces(block):
        return jnp.concatenate(
            [
                jnp.concatenate(
                    [
                        block[field * 8 : field * 8 + 8, face * columns : (face + 1) * columns]
                        for field in range(4)
                    ],
                    axis=1,
                )
                for face in range(4)
            ],
            axis=0,
        )

    for load in loads[3:]:
        load.wait()
    for field in range(4):
        padded[field, :25] = state[:, field, :]
    values = jnp.concatenate([padded[field] for field in range(4)], axis=1)
    on_faces = dot3(tables[:64, :96], values)
    traces = to_fields(on_faces[:32])
    slopes = to_fields(on_faces[32:])
    row32 = iota((32, span), 0)
    marked = jnp.where(row32 == 5, over_faces(flip_wide, 32), traces)
    marked = jnp.where(row32 == 13, over_faces(cos_wide, 32), marked)
    marked = jnp.where(row32 == 21, over_faces(sin_wide, 32), marked)
    slopes_out = slopes * over_faces(side_wide, 32)
    high, low = halves(jnp.concatenate([marked, slopes_out], axis=0))
    stacked = dot_t(pack, jnp.concatenate([high, low], axis=0))
    lane = iota((total_rows, LANES), 1)
    message = jnp.zeros((total_rows, LANES), f32)
    for index in range(outer_levels):
        part = stacked[index * total_rows : (index + 1) * total_rows]
        part = part + pltpu.roll(part, half, axis=1)
        message = jnp.where(lane // half == index, part, message)
    flip, cos, sin = [
        jnp.broadcast_to(message[:, spot : spot + 1], message.shape) for spot in (5, 13, 21)
    ]
    node_lane = lane % 8
    field_lane = lane % 32 // 8
    mirrored = message
    for node, shift in ((0, LANES - 4), (1, LANES - 2), (3, 2), (4, 4)):
        mirrored = jnp.where(node_lane == node, pltpu.roll(message, shift, axis=1), mirrored)
    aligned = jnp.where(flip > 0.5, mirrored, message)
    turned_u = cos * aligned - sin * pltpu.roll(aligned, LANES - 8, axis=1)
    turned_v = cos * aligned + sin * pltpu.roll(aligned, 8, axis=1)
    sent[...] = jnp.where(
        field_lane == 1, turned_u, jnp.where(field_lane == 2, turned_v, aligned)
    )
    pl.semaphore_wait(barrier, len(others))
    for index in range(link_count):
        copy_of(index).start()
    for index in range(len(others)):
        notice_of(index).start()
    always = device_pos >= 0

    @pl.when(always)
    def _():
        first_of = owner * (4 * elems)
        key = (first_of + face_back * elems + place_in).astype(f32)
        first_of = first_of.astype(f32)
        key_down = jnp.transpose(jnp.concatenate([key, key], axis=0))
        back_rows = []
        for face in range(4):
            smaller = jnp.zeros((elems, LANES), f32)
            for other in range(4):
                rival = jnp.broadcast_to(key_down[:elems, other : other + 1], (elems, LANES))
                mine = (rival < key[face : face + 1]) & (rival >= first_of[face : face + 1])
                smaller = smaller + jnp.where(mine, 1.0, 0.0)
            rank = jnp.sum(smaller, axis=0, keepdims=True)
            back_rows.append(
                jnp.sum(member[face] * (base_back + inner * rank), axis=0, keepdims=True)
            )
        at_home = owner == device_pos
        homes = [
            jnp.where(at_home & (face_back == face), place_in + 1, 0).astype(f32)
            for face in range(4)
        ]
        back, *homes = stretched([jnp.concatenate(back_rows, axis=0)] + homes)
        spread[...] = hot_rows(outer_levels * LANES, rows_for(back, LANES))

        both_high, both_low = halves(jnp.concatenate([traces, slopes_out], axis=0))
        both = jnp.concatenate([both_high, both_low], axis=0)
        found = jnp.zeros((128, span), f32)
        for face in range(4):
            spots = jnp.where(
                homes[face] > 0.5, homes[face] * levels + (level - levels + 1).astype(f32), 0.0
            )
            found = found + dot(
                both[:, face * columns : (face + 1) * columns], hot_rows(columns, spots)
            )
        found = found[:64] + found[64:]
        known[:32] = traces
        known[32:64] = found[:32]
        known[64:96] = found[32:] - slopes
        known[96:128] = over_faces(
            0.5 + viscosity * penalty - 0.25 * lift_gain * viscosity * (1.0 + side_wide), 32
        )
        pressure, vel_u, vel_v, theta = [
            values[:, field * columns : (field + 1) * columns] for field in range(4)
        ]
        nothing = jnp.zeros_like(pressure)
        flux_x = jnp.concatenate([vel_u, pressure, nothing, theta * vel_u], axis=1)
        flux_y = jnp.concatenate([vel_v, nothing, pressure, theta * vel_v], axis=1)
        base_change[...] = dot3(
            tables[64:96, :288], jnp.concatenate([flux_x, flux_y, values], axis=0)
        )

    for index in range(link_count):
        copy_of(index).wait_recv()
    filler = jnp.zeros((LANES - total_rows, LANES), f32)
    turned = jnp.transpose(jnp.concatenate([arrived[...], filler], axis=0))
    turned = jnp.concatenate(
        [turned[half * index : half * (index + 1)] for index in range(outer_levels)], axis=1
    )
    high, low = halves(turned)
    far = dot(jnp.concatenate([high, low], axis=0), spread[...])
    far = far[:half] + far[half:]
    inside = known[:32]
    outside = known[32:64] + far[:32]
    jump = outside - inside
    slope_term = (0.5 * viscosity) * (known[64:96] + far[32:])
    weight = known[96:128]
    terms = []
    for face in range(4):
        sides = slice(face * columns, (face + 1) * columns)
        ins = [inside[field * 8 : field * 8 + 8, sides] for field in range(4)]
        outs = [outside[field * 8 : field * 8 + 8, sides] for field in range(4)]
        step = [jump[field * 8 : field * 8 + 8, sides] for field in range(4)]
        normal = 1 + face % 2
        sign = 1.0 if face < 2 else -1.0
        raw_in, raw_out = ins[normal], outs[normal]
        wave = weight[:8, sides] + 0.5 * jnp.maximum(jnp.abs(raw_in), jnp.abs(raw_out))
        drops = [
            (-0.5 * sign) * step[normal],
            None,
            None,
            (0.5 * sign) * (ins[3] * raw_in - outs[3] * raw_out),
        ]
        drops[normal] = (-0.5 * sign) * step[0]
        rows = []
        for field in range(4):
            term = wave * step[field] + slope_term[field * 8 : field * 8 + 8, sides]
            rows.append(term if drops[field] is None else term + drops[field])
        terms.append(jnp.concatenate(rows, axis=0))
    face_term = jnp.concatenate(terms, axis=1)
    total = base_change[...] + dot3(
        tables[96:128, :192], jnp.concatenate([to_faces(face_term), to_faces(jump)], axis=0)
    )
    for field in range(4):
        change[:, field, :] = total[:25, field * columns : (field + 1) * columns]

    for index in range(len(others)):
        notice_of(index).wait_recv()
    heard = jnp.max(notices[: len(others)]) + jnp.max(notice[...])
    sideways[0] = jnp.where(heard > 0.5, 1, 0)
    for index in range(link_count):
        copy_of(index).wait_send()
    for index in range(len(others)):
        notice_of(index).wait_send()


def body(curve_count, strip_count, state, register, neighbor, neighbor_face, seam):
    elems = neighbor.shape[1]
    columns = state.shape[2]
    levels = columns // elems
    inner = LANES // elems
    outer_levels = levels // inner
    reach = min(7, (curve_count - 1) // 2)
    slots = (TW + reach - 1) // reach
    links, rows_of = [], []
    for distance in range(reach, 0, -1):
        for direction in (1, -1):
            links.append(("curve", direction * distance))
            rows_of.append(-(-slots * inner // 8) * 8)
    for direction in (1, -1):
        links.append(("sub", direction))
        rows_of.append(-(-TW * inner // 8) * 8)
    offsets = [sum(rows_of[:index]) for index in range(len(links))]
    total_rows = sum(rows_of)
    plan = (elems, levels, curve_count, strip_count, links, rows_of, offsets)
    vmem = pl.BlockSpec(memory_space=pltpu.VMEM)
    nodes_first = jnp.transpose(state, (1, 0, 2))

    def call(kernel, tables, outputs, out_specs, scratch, collective_id):
        operands = (nodes_first, neighbor, neighbor_face, seam, jnp.asarray(tables))
        return pl.pallas_call(
            functools.partial(kernel, plan),
            out_shape=outputs,
            in_specs=[pl.BlockSpec(memory_space=pl.ANY)] * 5,
            out_specs=out_specs,
            scratch_shapes=[
                pltpu.VMEM(nodes_first.shape, f32),
                pltpu.VMEM(neighbor.shape, jnp.int32),
                pltpu.VMEM(neighbor.shape, jnp.int32),
                pltpu.VMEM(neighbor.shape, jnp.int32),
                pltpu.VMEM(tables.shape, bf16),
                pltpu.VMEM((4, 32, columns), f32),
            ]
            + scratch,
            compiler_params=pltpu.CompilerParams(
                collective_id=collective_id, has_side_effects=True
            ),
        )(*[pltpu.with_memory_space_constraint(operand, pltpu.HBM) for operand in operands])

    def two_rounds():
        return call(
            two_round_kernel,
            build_tables(),
            pltpu.VMEM(nodes_first.shape, f32),
            vmem,
            [
                pltpu.VMEM((2, total_rows, LANES), f32),
                pltpu.VMEM((2, total_rows, LANES), f32),
                pltpu.VMEM((32, 4 * columns), f32),
                pltpu.VMEM((128, 4 * columns), f32),
                pltpu.VMEM((128, columns), f32),
                pltpu.SemaphoreType.DMA((5,)),
                pltpu.SemaphoreType.DMA((2, len(links))),
                pltpu.SemaphoreType.DMA((2, len(links))),
            ],
            0,
        )

    others = curve_count * strip_count - 1
    if others < DIRECT_LIMIT and total_rows <= LANES and outer_levels * 64 == LANES:
        change, sideways = call(
            direct_kernel,
            build_direct_tables(),
            (pltpu.VMEM(nodes_first.shape, f32), jax.ShapeDtypeStruct((1,), jnp.int32)),
            (vmem, pl.BlockSpec(memory_space=pltpu.SMEM)),
            [
                pltpu.VMEM((total_rows, LANES), f32),
                pltpu.VMEM((total_rows, LANES), f32),
                pltpu.VMEM((8, LANES), f32),
                pltpu.VMEM((-(-others // 8) * 8, LANES), f32),
                pltpu.VMEM((outer_levels * LANES, 4 * columns), bf16),
                pltpu.VMEM((128, 4 * columns), f32),
                pltpu.VMEM((32, 4 * columns), f32),
                pltpu.SemaphoreType.DMA((5,)),
                pltpu.SemaphoreType.DMA((len(links),)),
                pltpu.SemaphoreType.DMA((len(links),)),
                pltpu.SemaphoreType.DMA((others,)),
                pltpu.SemaphoreType.DMA((others,)),
            ],
            1,
        )
        change = lax.cond(sideways[0] == 0, lambda kept: kept, lambda _: two_rounds(), change)
    else:
        change = two_rounds()
    next_register = section_a * register + step_size * jnp.transpose(change, (1, 0, 2))
    return state + section_b * next_register, next_register


def solution(mesh):
    wide = P(None, None, ("curve", "sub"))
    flat = P(None, ("curve", "sub"))
    return jax.shard_map(
        functools.partial(body, mesh.shape["curve"], mesh.shape["sub"]),
        mesh=mesh,
        in_specs=(wide, wide, flat, flat, flat),
        out_specs=(wide, wide),
        check_vma=False,
    )
```

```python
import functools
import math

import jax
import jax.numpy as jnp
import ml_dtypes
import numpy as np
from jax import lax
from jax.experimental import pallas as pl
from jax.experimental.pallas import tpu as pltpu
from jax.sharding import PartitionSpec as P

TW = 8
LANES = 128
DIRECT_LIMIT = 64

lift_gain = 10.0
step_size = 0.02
viscosity = 0.05
penalty = 2.0
section_a = -567301805773.0 / 1357537059087.0
section_b = 2404267990393.0 / 2016746695238.0

f32 = jnp.float32
bf16 = jnp.bfloat16


def build_derivative():
    points = np.array([-1.0, -math.sqrt(3.0 / 7.0), 0.0, math.sqrt(3.0 / 7.0), 1.0])
    weights = np.array(
        [
            1.0 / np.prod([points[row] - points[col] for col in range(5) if col != row])
            for row in range(5)
        ]
    )
    table = np.zeros((5, 5))
    for row in range(5):
        for col in range(5):
            if row != col:
                table[row, col] = weights[col] / weights[row] / (points[row] - points[col])
        table[row, row] = -np.sum(table[row])
    return table


def face_node(face, node):
    return [(4, node), (node, 4), (0, node), (node, 0)][face]


def split_const(table):
    high = table.astype(ml_dtypes.bfloat16)
    low = (table - high.astype(np.float64)).astype(ml_dtypes.bfloat16)
    return np.concatenate([high, low, high], axis=1)


def element_tables():
    d = build_derivative()
    eye = np.eye(5)
    dx = np.zeros((32, 32))
    dy = np.zeros((32, 32))
    dx[:25, :25] = np.kron(d, eye)
    dy[:25, :25] = np.kron(eye, d)
    pick = np.zeros((32, 32))
    for face in range(4):
        for node in range(5):
            a, b = face_node(face, node)
            pick[face * 8 + node, a * 5 + b] = 1.0
    normal_x = np.repeat([1.0, 0.0, -1.0, 0.0], 8)
    normal_y = np.repeat([0.0, 1.0, 0.0, -1.0], 8)
    lift_x = pick.T * normal_x[None] * (0.5 * lift_gain)
    lift_y = pick.T * normal_y[None] * (0.5 * lift_gain)
    return dx, dy, pick, normal_x, normal_y, lift_x, lift_y


def build_tables():
    dx, dy, pick, _, _, lift_x, lift_y = element_tables()
    grad_x = np.concatenate([dx, lift_x], axis=1)
    grad_y = np.concatenate([dy, lift_y], axis=1)
    grad = np.concatenate([grad_x, grad_y, pick @ grad_x, pick @ grad_y], axis=0)
    volume = np.concatenate([-dx, -dy, lift_gain * pick.T], axis=1)
    late = lift_gain * 0.5 * viscosity * pick.T
    out = np.zeros((224, 384), ml_dtypes.bfloat16)
    out[:128, :192] = split_const(grad)
    out[:128, 192:288] = split_const(grad[:, 32:])
    out[128:160, :288] = split_const(volume)
    out[160:192, :96] = split_const(late)
    out[192:224, :32] = pick.astype(ml_dtypes.bfloat16)
    out[192:224, 32:64] = pick.astype(ml_dtypes.bfloat16)
    return out


def build_direct_tables():
    dx, dy, pick, normal_x, normal_y, lift_x, lift_y = element_tables()
    slope = normal_x[:, None] * (pick @ dx) + normal_y[:, None] * (pick @ dy)
    base = np.concatenate([-dx, -dy, viscosity * (dx @ dx + dy @ dy)], axis=1)
    jump = viscosity * (dx @ lift_x + dy @ lift_y)
    late = np.concatenate([lift_gain * pick.T, jump], axis=1)
    out = np.zeros((128, 384), ml_dtypes.bfloat16)
    out[:64, :96] = split_const(np.concatenate([pick, slope], axis=0))
    out[64:96, :288] = split_const(base)
    out[96:128, :192] = split_const(late)
    return out


def halves(x):
    high = x.astype(bf16)
    low = (x - high.astype(f32)).astype(bf16)
    return high, low


def dot(a, b):
    return lax.dot_general(a, b, (((1,), (0,)), ((), ())), preferred_element_type=f32)


def dot_t(a, b):
    return lax.dot_general(a, b, (((1,), (1,)), ((), ())), preferred_element_type=f32)


def dot3(table, x):
    high, low = halves(x)
    return dot(table, jnp.concatenate([high, high, low], axis=0))


def onehot(mask):
    return jnp.where(mask, 1.0, 0.0).astype(bf16)


def permute(x, perm):
    rows = x.shape[0]
    high, low = halves(x)
    both = dot(jnp.concatenate([high, low], axis=0), perm)
    return both[:rows] + both[rows:]


def iota(shape, dim):
    return lax.broadcasted_iota(jnp.int32, shape, dim)


def two_round_kernel(
    plan,
    state_hbm,
    neighbor_hbm,
    neighbor_face_hbm,
    seam_hbm,
    tables_hbm,
    change,
    state,
    neighbor,
    neighbor_face,
    seam,
    tables,
    padded,
    sent,
    arrived,
    own_faces,
    early_grads,
    early_change,
    load_sem,
    send_sem,
    recv_sem,
):
    elems, levels, curve_count, strip_count, links, rows_of, offsets = plan
    columns = elems * levels
    inner = LANES // elems
    outer_levels = levels // inner
    groups = 4 * outer_levels
    span = 4 * LANES
    total_rows = offsets[-1] + rows_of[-1]
    link_count = len(links)
    link_rows = -(-link_count // 8) * 8

    curve_pos = lax.axis_index("curve")
    strip_pos = lax.axis_index("sub")
    device_pos = curve_pos * strip_count + strip_pos
    places = []
    for axis, step in links:
        if axis == "curve":
            places.append((lax.rem(curve_pos + step + curve_count, curve_count), strip_pos))
        else:
            places.append((curve_pos, lax.rem(strip_pos + step + strip_count, strip_count)))

    barrier = pltpu.get_barrier_semaphore()
    for place in places:
        pl.semaphore_signal(
            barrier, inc=1, device_id=place, device_id_type=pl.DeviceIdType.MESH
        )
    loads = [
        pltpu.make_async_copy(source_ref, target_ref, load_sem.at[index])
        for index, (source_ref, target_ref) in enumerate(
            [
                (neighbor_hbm, neighbor),
                (neighbor_face_hbm, neighbor_face),
                (seam_hbm, seam),
                (state_hbm, state),
                (tables_hbm, tables),
            ]
        )
    ]
    for load in loads:
        load.start()
    for load in loads[:3]:
        load.wait()

    def widen(ref):
        block = ref[...]
        return jnp.concatenate([block] * inner, axis=1)

    across = widen(neighbor)
    face_back = widen(neighbor_face)
    codes = widen(seam)
    owner = across // elems
    place_in = across % elems
    turn = codes % 4
    flipped = codes // 4
    sub_level = iota((4, LANES), 1) // elems
    position = face_back * LANES + sub_level * elems + place_in
    source = jnp.where(owner == device_pos, position, -1)
    heading = (face_back + turn) % 4
    cosine = jnp.where(turn == 0, 1.0, 0.0) - jnp.where(turn == 2, 1.0, 0.0)
    sine = jnp.where(turn == 3, 1.0, 0.0) - jnp.where(turn == 1, 1.0, 0.0)
    head_x = jnp.where(heading == 0, 1.0, 0.0) - jnp.where(heading == 2, 1.0, 0.0)
    head_y = jnp.where(heading == 1, 1.0, 0.0) - jnp.where(heading == 3, 1.0, 0.0)

    link_iota = iota((link_rows, LANES), 0)
    target = jnp.full((link_rows, LANES), -1, jnp.int32)
    base = jnp.zeros((link_rows, LANES), f32)
    for index, place in enumerate(places):
        target = jnp.where(link_iota == index, place[0] * strip_count + place[1], target)
        base = jnp.where(link_iota == index, float(offsets[index] + 1), base)
    base = base + (iota((link_rows, LANES), 1) // elems).astype(f32)
    member = [
        jnp.where(owner[face : face + 1] == target, 1.0, 0.0) for face in range(4)
    ]
    from_lane = iota((LANES, 2 * LANES), 0)
    to_lane = iota((LANES, 2 * LANES), 1)
    same = from_lane // elems == (to_lane % LANES) // elems
    earlier = same & ((from_lane < to_lane) | (to_lane >= LANES))
    counts = dot(jnp.concatenate(member, axis=0).astype(bf16), onehot(earlier))
    before = jnp.zeros((link_rows, LANES), f32)
    slot_rows = []
    for face in range(4):
        part = counts[face * link_rows : (face + 1) * link_rows]
        rank = part[:, :LANES] + before
        before = before + part[:, LANES:]
        slot_rows.append(
            jnp.sum(member[face] * (base + inner * rank), axis=0, keepdims=True)
        )
    slot_row = jnp.concatenate(slot_rows, axis=1)
    pack = onehot(
        (iota((total_rows, span), 0) + 1).astype(f32)
        == jnp.broadcast_to(slot_row, (total_rows, span))
    )
    pack2 = jnp.concatenate([pack, pack], axis=1)

    def local_table():
        span_iota = iota((span, LANES), 0)
        return jnp.concatenate(
            [onehot(span_iota == source[face : face + 1]) for face in range(4)], axis=1
        )

    meta_iota = iota((8, LANES), 0)
    meta_blocks = []
    for face in range(4):
        block = jnp.zeros((8, LANES), f32)
        for row, values in enumerate(
            [flipped.astype(f32), cosine, sine, (position + 1).astype(f32)]
        ):
            block = jnp.where(meta_iota == row, values[face : face + 1], block)
        meta_blocks.append(block)
    meta = jnp.concatenate(meta_blocks, axis=1)
    heads_x = jnp.concatenate(
        [jnp.broadcast_to(head_x[face : face + 1], (8, LANES)) for face in range(4)], axis=0
    )
    heads_y = jnp.concatenate(
        [jnp.broadcast_to(head_y[face : face + 1], (8, LANES)) for face in range(4)], axis=0
    )

    def to_exchange(faces):
        return jnp.concatenate(
            [
                jnp.concatenate(
                    [
                        faces[face * 8 : face * 8 + 8, group * LANES : (group + 1) * LANES]
                        for face in range(4)
                    ],
                    axis=1,
                )
                for group in range(groups)
            ],
            axis=0,
        )

    def from_exchange(block):
        return jnp.concatenate(
            [
                jnp.concatenate(
                    [
                        block[group * 8 : group * 8 + 8, face * LANES : (face + 1) * LANES]
                        for group in range(groups)
                    ],
                    axis=1,
                )
                for face in range(4)
            ],
            axis=0,
        )

    data_lanes = groups * 8
    field_lanes = outer_levels * 8
    lane = iota((total_rows, LANES), 1)
    node_lane = lane % 8
    in_data = lane < data_lanes

    def copy_of(turn_index, index):
        rows = pl.ds(offsets[index], rows_of[index])
        return pltpu.make_async_remote_copy(
            src_ref=sent.at[turn_index, rows],
            dst_ref=arrived.at[turn_index, rows],
            send_sem=send_sem.at[turn_index, index],
            recv_sem=recv_sem.at[turn_index, index],
            device_id=places[index],
            device_id_type=pl.DeviceIdType.MESH,
        )

    def post(turn_index, block, flags):
        if flags is None:
            pieces = [block, meta]
            if data_lanes + 8 < LANES:
                pieces.append(jnp.zeros((LANES - data_lanes - 8, span), f32))
            block = jnp.concatenate(pieces, axis=0)
        high, low = halves(block)
        message = dot_t(pack2, jnp.concatenate([high, low], axis=1))
        if flags is None:
            flags = [
                jnp.broadcast_to(
                    message[:, data_lanes + index : data_lanes + index + 1], message.shape
                )
                for index in range(3)
            ]
        else:
            rest = jnp.zeros((total_rows, LANES - data_lanes), f32)
            message = jnp.concatenate([message, rest], axis=1)
        flip, cos, sin = flags
        mirrored = message
        for node, shift in ((0, LANES - 4), (1, LANES - 2), (3, 2), (4, 4)):
            mirrored = jnp.where(
                node_lane == node, pltpu.roll(message, shift, axis=1), mirrored
            )
        aligned = jnp.where(in_data & (flip > 0.5), mirrored, message)
        field = lane // field_lanes
        turned_u = cos * aligned - sin * pltpu.roll(aligned, LANES - field_lanes, axis=1)
        turned_v = cos * aligned + sin * pltpu.roll(aligned, field_lanes, axis=1)
        aligned = jnp.where(field == 1, turned_u, jnp.where(field == 2, turned_v, aligned))
        sent[turn_index] = aligned
        if turn_index == 0:
            pl.semaphore_wait(barrier, link_count)
        for index in range(link_count):
            copy_of(turn_index, index).start()
        return flags

    def gather_local(block):
        rows = block.shape[0]
        high, low = halves(block)
        both = dot(jnp.concatenate([high, low], axis=0), local_table())
        return both[:rows] + both[rows:]

    def await_all(turn_index):
        for index in range(link_count):
            copy_of(turn_index, index).wait_recv()

    def spread_table():
        message = arrived[0]
        spot = jnp.broadcast_to(
            message[:, data_lanes + 3 : data_lanes + 4], (total_rows, span)
        )
        return onehot((iota((total_rows, span), 1) + 1).astype(f32) == spot)

    def collect(turn_index, spread):
        message = arrived[turn_index]
        high, low = halves(jnp.transpose(message)[:data_lanes])
        both = dot(jnp.concatenate([high, low], axis=0), spread)
        return both[:data_lanes] + both[data_lanes:]

    row = iota((columns, columns), 0)
    col = iota((columns, columns), 1)
    to_level = onehot(row == (col % elems) * levels + col // elems)
    to_elem = onehot(row == (col % levels) * elems + col // levels)

    padded[...] = jnp.zeros_like(padded)
    for load in loads[3:]:
        load.wait()
    for field in range(4):
        padded[field, :25] = state[:, field, :]
    nodal = permute(padded[...].reshape(128, columns), to_level)
    values = jnp.concatenate(
        [nodal[field * 32 : field * 32 + 32] for field in range(4)], axis=1
    )
    high, low = halves(values)
    faces_in = dot(tables[192:224, :64], jnp.concatenate([high, low], axis=0))

    def fields_of(wide):
        return [wide[:, field * columns : (field + 1) * columns] for field in range(4)]

    def elementwise_lanes(wide):
        return permute(jnp.concatenate(fields_of(wide), axis=0), to_elem)

    def early_part(values, faces_in, faces_out, grad_x, grad_y, face_gx, face_gy, own_slope):
        face_of_row = iota((32, columns), 0) // 8
        normal_x = jnp.where(face_of_row == 0, 1.0, 0.0) - jnp.where(face_of_row == 2, 1.0, 0.0)
        normal_y = jnp.where(face_of_row == 1, 1.0, 0.0) - jnp.where(face_of_row == 3, 1.0, 0.0)

        def flux_of(faces):
            speed = faces[1] * normal_x + faces[2] * normal_y
            return [speed, faces[0] * normal_x, faces[0] * normal_y, faces[3] * speed], speed

        inside, outside = fields_of(faces_in), fields_of(faces_out)
        gx_in, gy_in = fields_of(face_gx), fields_of(face_gy)
        slope_own = fields_of(own_slope)
        flux_in, speed_in = flux_of(inside)
        flux_out, speed_out = flux_of(outside)
        wave = 1.0 + jnp.maximum(jnp.abs(speed_in), jnp.abs(speed_out))
        terms = []
        for field in range(4):
            slope_in = gx_in[field] * normal_x + gy_in[field] * normal_y
            jump = outside[field] - inside[field]
            terms.append(
                0.5 * (flux_in[field] - flux_out[field])
                - 0.5 * viscosity * (slope_in - slope_own[field])
                + (0.5 * wave + viscosity * penalty) * jump
            )
        face_term = jnp.concatenate(terms, axis=1)
        pressure, vel_u, vel_v, theta = fields_of(values)
        nothing = jnp.zeros_like(pressure)
        flux_x = jnp.concatenate([vel_u, pressure, nothing, theta * vel_u], axis=1)
        flux_y = jnp.concatenate([vel_v, nothing, pressure, theta * vel_v], axis=1)
        tendency = dot3(
            tables[128:160, :288],
            jnp.concatenate(
                [flux_x - viscosity * grad_x, flux_y - viscosity * grad_y, face_term], axis=0
            ),
        )

        return elementwise_lanes(tendency)

    block_in = to_exchange(faces_in)
    flags = post(0, block_in, None)
    always = device_pos >= 0

    @pl.when(always)
    def _():
        own = from_exchange(gather_local(block_in))
        own_faces[...] = own
        early_grads[...] = dot3(
            tables[:128, :192], jnp.concatenate([values, own - faces_in], axis=0)
        )

    await_all(0)
    spread = spread_table()
    far_faces = from_exchange(collect(0, spread))
    face_grads = early_grads[64:128] + dot3(tables[64:128, 192:288], far_faces)
    face_gx, face_gy = face_grads[:32], face_grads[32:]
    wide_x = jnp.concatenate([heads_x] * groups, axis=1)
    wide_y = jnp.concatenate([heads_y] * groups, axis=1)
    block_grad = to_exchange(face_gx * wide_x + face_gy * wide_y)
    post(1, block_grad, flags)

    @pl.when(always)
    def _():
        own_slope = from_exchange(gather_local(block_grad))
        grads = early_grads[:64] + dot3(tables[:64, 192:288], far_faces)
        faces_out = own_faces[...] + far_faces
        grad_x, grad_y = grads[:32], grads[32:]
        early_change[...] = early_part(
            values, faces_in, faces_out, grad_x, grad_y, face_gx, face_gy, own_slope
        )

    await_all(1)
    far_slope = from_exchange(collect(1, spread))
    late = elementwise_lanes(dot3(tables[160:192, :96], far_slope))
    total = early_change[...] + late
    for field in range(4):
        change[:, field, :] = total[field * 32 : field * 32 + 25]

    for turn_index in range(2):
        for index in range(link_count):
            copy_of(turn_index, index).wait_send()


def direct_kernel(
    plan,
    state_hbm,
    neighbor_hbm,
    neighbor_face_hbm,
    seam_hbm,
    tables_hbm,
    register_hbm,
    own_part,
    late_part,
    sideways,
    state,
    neighbor,
    neighbor_face,
    seam,
    tables,
    padded,
    sent,
    arrived,
    notice,
    notices,
    spread,
    known,
    register,
    load_sem,
    send_sem,
    recv_sem,
    notice_send_sem,
    notice_recv_sem,
):
    elems, levels, curve_count, strip_count, links, rows_of, offsets = plan
    columns = elems * levels
    span = 4 * columns
    inner = LANES // elems
    outer_levels = levels // inner
    total_rows = offsets[-1] + rows_of[-1]
    link_count = len(links)
    link_rows = -(-link_count // 8) * 8
    half = LANES // outer_levels

    curve_pos = lax.axis_index("curve")
    strip_pos = lax.axis_index("sub")
    device_pos = curve_pos * strip_count + strip_pos

    def place_at(curve_step, strip_step):
        return (
            lax.rem(curve_pos + curve_step + curve_count, curve_count),
            lax.rem(strip_pos + strip_step + strip_count, strip_count),
        )

    places = [place_at(step, 0) if axis == "curve" else place_at(0, step) for axis, step in links]
    others = [
        place_at(curve_step, strip_step)
        for curve_step in range(curve_count)
        for strip_step in range(strip_count)
        if curve_step or strip_step
    ]

    barrier = pltpu.get_barrier_semaphore()
    for place in others:
        pl.semaphore_signal(
            barrier, inc=1, device_id=place, device_id_type=pl.DeviceIdType.MESH
        )
    loads = [
        pltpu.make_async_copy(source_ref, target_ref, load_sem.at[index])
        for index, (source_ref, target_ref) in enumerate(
            [
                (neighbor_hbm, neighbor),
                (neighbor_face_hbm, neighbor_face),
                (seam_hbm, seam),
                (state_hbm, state),
                (tables_hbm, tables),
                (register_hbm, register),
            ]
        )
    ]
    for load in loads:
        load.start()
    padded[...] = jnp.zeros_like(padded)

    def copy_of(index):
        rows = pl.ds(offsets[index], rows_of[index])
        return pltpu.make_async_remote_copy(
            src_ref=sent.at[rows],
            dst_ref=arrived.at[rows],
            send_sem=send_sem.at[index],
            recv_sem=recv_sem.at[index],
            device_id=places[index],
            device_id_type=pl.DeviceIdType.MESH,
        )

    def notice_of(index):
        return pltpu.make_async_remote_copy(
            src_ref=notice.at[pl.ds(0, 1)],
            dst_ref=notices.at[pl.ds(index, 1)],
            send_sem=notice_send_sem.at[index],
            recv_sem=notice_recv_sem.at[index],
            device_id=others[index],
            device_id_type=pl.DeviceIdType.MESH,
        )

    for load in loads[:3]:
        load.wait()

    def widen(ref):
        block = ref[...]
        return jnp.concatenate([block] * inner, axis=1)

    across = widen(neighbor)
    face_back = widen(neighbor_face)
    codes = widen(seam)
    owner = across // elems
    place_in = across % elems
    turn = codes % 4
    flipped = codes // 4
    own_face = iota((4, LANES), 0)
    quarter = (face_back + turn - own_face + 4) % 4
    odd = jnp.where(quarter % 2 == 1, 1.0, 0.0)
    notice[...] = jnp.broadcast_to(jnp.sum(odd, axis=0, keepdims=True), (8, LANES))
    side = jnp.where(quarter == 0, 1.0, -1.0)
    cosine = jnp.where(turn == 0, 1.0, 0.0) - jnp.where(turn == 2, 1.0, 0.0)
    sine = jnp.where(turn == 3, 1.0, 0.0) - jnp.where(turn == 1, 1.0, 0.0)

    link_iota = iota((link_rows, LANES), 0)
    target = jnp.full((link_rows, LANES), -1, jnp.int32)
    base = jnp.zeros((link_rows, LANES), f32)
    base_back = jnp.zeros((link_rows, LANES), f32)
    for index, place in enumerate(places):
        here = link_iota == index
        target = jnp.where(here, place[0] * strip_count + place[1], target)
        base = jnp.where(here, float(offsets[index] + 1), base)
        base_back = jnp.where(here, float(offsets[index ^ 1] + 1), base_back)
    member = [
        jnp.where(owner[face : face + 1] == target, 1.0, 0.0) for face in range(4)
    ]
    from_lane = iota((LANES, 2 * LANES), 0)
    to_lane = iota((LANES, 2 * LANES), 1)
    same = from_lane // elems == (to_lane % LANES) // elems
    earlier = same & ((from_lane < to_lane) | (to_lane >= LANES))
    counts = dot(jnp.concatenate(member, axis=0).astype(bf16), onehot(earlier))
    before = jnp.zeros((link_rows, LANES), f32)
    slot_rows = []
    for face in range(4):
        part = counts[face * link_rows : (face + 1) * link_rows]
        rank = part[:, :LANES] + before
        before = before + part[:, LANES:]
        slot_rows.append(
            jnp.sum(member[face] * (base + inner * rank), axis=0, keepdims=True)
        )

    stretch = onehot(iota((LANES, columns), 0) == iota((LANES, columns), 1) // levels)

    def stretched(per_face):
        rows = []
        for values in per_face:
            rows.append(values)
            rows.append(jnp.zeros_like(values))
        wide = dot(jnp.concatenate(rows, axis=0).astype(bf16), stretch)
        return [wide[8 * index : 8 * index + 8] for index in range(len(per_face))]

    slot, flip_wide, cos_wide, sin_wide, side_wide = stretched(
        [jnp.concatenate(slot_rows, axis=0), flipped.astype(f32), cosine, sine, side]
    )
    level = iota((8, columns), 1) % levels

    def rows_for(slot, stride):
        spot = slot + (level % inner + level // inner * stride).astype(f32)
        return jnp.where(slot > 0.5, spot, 0.0)

    def hot_rows(count, spots):
        count_iota = (iota((count, columns), 0) + 1).astype(f32)
        return jnp.concatenate(
            [
                onehot(
                    count_iota == jnp.broadcast_to(spots[face : face + 1], (count, columns))
                )
                for face in range(4)
            ],
            axis=1,
        )

    pack = hot_rows(outer_levels * total_rows, rows_for(slot, total_rows))

    def over_faces(wide, rows):
        return jnp.concatenate(
            [jnp.broadcast_to(wide[face : face + 1], (rows, columns)) for face in range(4)],
            axis=1,
        )

    def to_fields(block):
        return jnp.concatenate(
            [
                jnp.concatenate(
                    [
                        block[face * 8 : face * 8 + 8, field * columns : (field + 1) * columns]
                        for face in range(4)
                    ],
                    axis=1,
                )
                for field in range(4)
            ],
            axis=0,
        )

    def to_faces(block):
        return jnp.concatenate(
            [
                jnp.concatenate(
                    [
                        block[field * 8 : field * 8 + 8, face * columns : (face + 1) * columns]
                        for field in range(4)
                    ],
                    axis=1,
                )
                for face in range(4)
            ],
            axis=0,
        )

    for load in loads[3:5]:
        load.wait()
    for field in range(4):
        padded[field, :25] = state[:, field, :]
    values = jnp.concatenate([padded[field] for field in range(4)], axis=1)
    on_faces = dot3(tables[:64, :96], values)
    traces = to_fields(on_faces[:32])
    slopes = to_fields(on_faces[32:])
    row32 = iota((32, span), 0)
    marked = jnp.where(row32 == 5, over_faces(flip_wide, 32), traces)
    marked = jnp.where(row32 == 13, over_faces(cos_wide, 32), marked)
    marked = jnp.where(row32 == 21, over_faces(sin_wide, 32), marked)
    slopes_out = slopes * over_faces(side_wide, 32)
    high, low = halves(jnp.concatenate([marked, slopes_out], axis=0))
    stacked = dot_t(pack, jnp.concatenate([high, low], axis=0))
    lane = iota((total_rows, LANES), 1)
    message = jnp.zeros((total_rows, LANES), f32)
    for index in range(outer_levels):
        part = stacked[index * total_rows : (index + 1) * total_rows]
        part = part + pltpu.roll(part, half, axis=1)
        message = jnp.where(lane // half == index, part, message)
    flip, cos, sin = [
        jnp.broadcast_to(message[:, spot : spot + 1], message.shape) for spot in (5, 13, 21)
    ]
    node_lane = lane % 8
    field_lane = lane % 32 // 8
    mirrored = message
    for node, shift in ((0, LANES - 4), (1, LANES - 2), (3, 2), (4, 4)):
        mirrored = jnp.where(node_lane == node, pltpu.roll(message, shift, axis=1), mirrored)
    aligned = jnp.where(flip > 0.5, mirrored, message)
    turned_u = cos * aligned - sin * pltpu.roll(aligned, LANES - 8, axis=1)
    turned_v = cos * aligned + sin * pltpu.roll(aligned, 8, axis=1)
    sent[...] = jnp.where(
        field_lane == 1, turned_u, jnp.where(field_lane == 2, turned_v, aligned)
    )
    pl.semaphore_wait(barrier, len(others))
    for index in range(link_count):
        copy_of(index).start()
    for index in range(len(others)):
        notice_of(index).start()
    always = device_pos >= 0

    @pl.when(always)
    def _():
        first_of = owner * (4 * elems)
        key = (first_of + face_back * elems + place_in).astype(f32)
        first_of = first_of.astype(f32)
        key_down = jnp.transpose(jnp.concatenate([key, key], axis=0))
        back_rows = []
        for face in range(4):
            smaller = jnp.zeros((elems, LANES), f32)
            for other in range(4):
                rival = jnp.broadcast_to(key_down[:elems, other : other + 1], (elems, LANES))
                mine = (rival < key[face : face + 1]) & (rival >= first_of[face : face + 1])
                smaller = smaller + jnp.where(mine, 1.0, 0.0)
            rank = jnp.sum(smaller, axis=0, keepdims=True)
            back_rows.append(
                jnp.sum(member[face] * (base_back + inner * rank), axis=0, keepdims=True)
            )
        at_home = owner == device_pos
        homes = [
            jnp.where(at_home & (face_back == face), place_in + 1, 0).astype(f32)
            for face in range(4)
        ]
        back, *homes = stretched([jnp.concatenate(back_rows, axis=0)] + homes)
        spread[...] = hot_rows(outer_levels * LANES, rows_for(back, LANES))

        both_high, both_low = halves(jnp.concatenate([traces, slopes_out], axis=0))
        both = jnp.concatenate([both_high, both_low], axis=0)
        found = jnp.zeros((128, span), f32)
        for face in range(4):
            spots = jnp.where(
                homes[face] > 0.5, homes[face] * levels + (level - levels + 1).astype(f32), 0.0
            )
            found = found + dot(
                both[:, face * columns : (face + 1) * columns], hot_rows(columns, spots)
            )
        found = found[:64] + found[64:]
        known[:32] = traces
        known[32:64] = found[:32]
        known[64:96] = found[32:] - slopes
        known[96:128] = over_faces(
            0.5 + viscosity * penalty - 0.25 * lift_gain * viscosity * (1.0 + side_wide), 32
        )
        pressure, vel_u, vel_v, theta = [
            values[:, field * columns : (field + 1) * columns] for field in range(4)
        ]
        nothing = jnp.zeros_like(pressure)
        flux_x = jnp.concatenate([vel_u, pressure, nothing, theta * vel_u], axis=1)
        flux_y = jnp.concatenate([vel_v, nothing, pressure, theta * vel_v], axis=1)
        loads[5].wait()
        for field in range(4):
            padded[field, :25] = register[:, field, :]
        held = jnp.concatenate([padded[field] for field in range(4)], axis=1)
        own = dot3(tables[64:96, :288], jnp.concatenate([flux_x, flux_y, values], axis=0))
        own = section_a * held + step_size * own
        for field in range(4):
            own_part[:, field, :] = own[:25, field * columns : (field + 1) * columns]

    for index in range(link_count):
        copy_of(index).wait_recv()
    filler = jnp.zeros((LANES - total_rows, LANES), f32)
    turned = jnp.transpose(jnp.concatenate([arrived[...], filler], axis=0))
    turned = jnp.concatenate(
        [turned[half * index : half * (index + 1)] for index in range(outer_levels)], axis=1
    )
    high, low = halves(turned)
    far = dot(jnp.concatenate([high, low], axis=0), spread[...])
    far = far[:half] + far[half:]
    inside = known[:32]
    outside = known[32:64] + far[:32]
    jump = outside - inside
    slope_term = (0.5 * viscosity) * (known[64:96] + far[32:])
    weight = known[96:128]
    terms = []
    for face in range(4):
        sides = slice(face * columns, (face + 1) * columns)
        ins = [inside[field * 8 : field * 8 + 8, sides] for field in range(4)]
        outs = [outside[field * 8 : field * 8 + 8, sides] for field in range(4)]
        step = [jump[field * 8 : field * 8 + 8, sides] for field in range(4)]
        normal = 1 + face % 2
        sign = 1.0 if face < 2 else -1.0
        raw_in, raw_out = ins[normal], outs[normal]
        wave = weight[:8, sides] + 0.5 * jnp.maximum(jnp.abs(raw_in), jnp.abs(raw_out))
        drops = [
            (-0.5 * sign) * step[normal],
            None,
            None,
            (0.5 * sign) * (ins[3] * raw_in - outs[3] * raw_out),
        ]
        drops[normal] = (-0.5 * sign) * step[0]
        rows = []
        for field in range(4):
            term = wave * step[field] + slope_term[field * 8 : field * 8 + 8, sides]
            rows.append(term if drops[field] is None else term + drops[field])
        terms.append(jnp.concatenate(rows, axis=0))
    face_term = jnp.concatenate(terms, axis=1)
    late = dot3(
        tables[96:128, :192], jnp.concatenate([to_faces(face_term), to_faces(jump)], axis=0)
    )
    for field in range(4):
        late_part[:, field, :] = late[:25, field * columns : (field + 1) * columns]

    for index in range(len(others)):
        notice_of(index).wait_recv()
    heard = jnp.max(notices[: len(others)]) + jnp.max(notice[...])
    sideways[0] = jnp.where(heard > 0.5, 1, 0)
    for index in range(link_count):
        copy_of(index).wait_send()
    for index in range(len(others)):
        notice_of(index).wait_send()


def body(curve_count, strip_count, state, register, neighbor, neighbor_face, seam):
    elems = neighbor.shape[1]
    columns = state.shape[2]
    levels = columns // elems
    inner = LANES // elems
    outer_levels = levels // inner
    reach = min(7, (curve_count - 1) // 2)
    slots = (TW + reach - 1) // reach
    links, rows_of = [], []
    for distance in range(reach, 0, -1):
        for direction in (1, -1):
            links.append(("curve", direction * distance))
            rows_of.append(-(-slots * inner // 8) * 8)
    for direction in (1, -1):
        links.append(("sub", direction))
        rows_of.append(-(-TW * inner // 8) * 8)
    offsets = [sum(rows_of[:index]) for index in range(len(links))]
    total_rows = sum(rows_of)
    plan = (elems, levels, curve_count, strip_count, links, rows_of, offsets)
    vmem = pl.BlockSpec(memory_space=pltpu.VMEM)
    nodes_first = jnp.transpose(state, (1, 0, 2))
    register_first = jnp.transpose(register, (1, 0, 2))
    shape = nodes_first.shape

    def call(kernel, tables, more, outputs, out_specs, scratch, collective_id):
        operands = (nodes_first, neighbor, neighbor_face, seam, jnp.asarray(tables), *more)
        return pl.pallas_call(
            functools.partial(kernel, plan),
            out_shape=outputs,
            in_specs=[pl.BlockSpec(memory_space=pl.ANY)] * len(operands),
            out_specs=out_specs,
            scratch_shapes=[
                pltpu.VMEM(nodes_first.shape, f32),
                pltpu.VMEM(neighbor.shape, jnp.int32),
                pltpu.VMEM(neighbor.shape, jnp.int32),
                pltpu.VMEM(neighbor.shape, jnp.int32),
                pltpu.VMEM(tables.shape, bf16),
                pltpu.VMEM((4, 32, columns), f32),
            ]
            + scratch,
            compiler_params=pltpu.CompilerParams(
                collective_id=collective_id, has_side_effects=True
            ),
        )(*[pltpu.with_memory_space_constraint(operand, pltpu.HBM) for operand in operands])

    def two_rounds():
        change = call(
            two_round_kernel,
            build_tables(),
            (),
            pltpu.VMEM(nodes_first.shape, f32),
            vmem,
            [
                pltpu.VMEM((2, total_rows, LANES), f32),
                pltpu.VMEM((2, total_rows, LANES), f32),
                pltpu.VMEM((32, 4 * columns), f32),
                pltpu.VMEM((128, 4 * columns), f32),
                pltpu.VMEM((128, columns), f32),
                pltpu.SemaphoreType.DMA((5,)),
                pltpu.SemaphoreType.DMA((2, len(links))),
                pltpu.SemaphoreType.DMA((2, len(links))),
            ],
            0,
        )
        return section_a * register_first, change

    others = curve_count * strip_count - 1
    if others < DIRECT_LIMIT and total_rows <= LANES and outer_levels * 64 == LANES:
        *parts, sideways = call(
            direct_kernel,
            build_direct_tables(),
            (register_first,),
            (pltpu.VMEM(shape, f32), pltpu.VMEM(shape, f32), pltpu.SMEM((1,), jnp.int32)),
            (vmem, vmem, pl.BlockSpec(memory_space=pltpu.SMEM)),
            [
                pltpu.VMEM((total_rows, LANES), f32),
                pltpu.VMEM((total_rows, LANES), f32),
                pltpu.VMEM((8, LANES), f32),
                pltpu.VMEM((-(-others // 8) * 8, LANES), f32),
                pltpu.VMEM((outer_levels * LANES, 4 * columns), bf16),
                pltpu.VMEM((128, 4 * columns), f32),
                pltpu.VMEM(shape, f32),
                pltpu.SemaphoreType.DMA((6,)),
                pltpu.SemaphoreType.DMA((len(links),)),
                pltpu.SemaphoreType.DMA((len(links),)),
                pltpu.SemaphoreType.DMA((others,)),
                pltpu.SemaphoreType.DMA((others,)),
            ],
            1,
        )
        own, late = lax.cond(
            sideways[0] == 0, lambda kept: tuple(kept), lambda _: two_rounds(), parts
        )
    else:
        own, late = two_rounds()
    next_register = jnp.transpose(own, (1, 0, 2)) + step_size * jnp.transpose(late, (1, 0, 2))
    return state + section_b * next_register, next_register


def solution(mesh):
    wide = P(None, None, ("curve", "sub"))
    flat = P(None, ("curve", "sub"))
    return jax.shard_map(
        functools.partial(body, mesh.shape["curve"], mesh.shape["sub"]),
        mesh=mesh,
        in_specs=(wide, wide, flat, flat, flat),
        out_specs=(wide, wide),
        check_vma=False,
    )
```

```python
import functools
import math

import jax
import jax.numpy as jnp
import ml_dtypes
import numpy as np
from jax import lax
from jax.experimental import pallas as pl
from jax.experimental.pallas import tpu as pltpu
from jax.sharding import PartitionSpec as P

TW = 8
LANES = 128
DIRECT_LIMIT = 64

lift_gain = 10.0
step_size = 0.02
viscosity = 0.05
penalty = 2.0
section_a = -567301805773.0 / 1357537059087.0
section_b = 2404267990393.0 / 2016746695238.0

f32 = jnp.float32
bf16 = jnp.bfloat16


def build_derivative():
    points = np.array([-1.0, -math.sqrt(3.0 / 7.0), 0.0, math.sqrt(3.0 / 7.0), 1.0])
    weights = np.array(
        [
            1.0 / np.prod([points[row] - points[col] for col in range(5) if col != row])
            for row in range(5)
        ]
    )
    table = np.zeros((5, 5))
    for row in range(5):
        for col in range(5):
            if row != col:
                table[row, col] = weights[col] / weights[row] / (points[row] - points[col])
        table[row, row] = -np.sum(table[row])
    return table


def face_node(face, node):
    return [(4, node), (node, 4), (0, node), (node, 0)][face]


def split_const(table):
    high = table.astype(ml_dtypes.bfloat16)
    low = (table - high.astype(np.float64)).astype(ml_dtypes.bfloat16)
    return np.concatenate([high, low, high], axis=1)


def element_tables():
    d = build_derivative()
    eye = np.eye(5)
    dx = np.zeros((32, 32))
    dy = np.zeros((32, 32))
    dx[:25, :25] = np.kron(d, eye)
    dy[:25, :25] = np.kron(eye, d)
    pick = np.zeros((32, 32))
    for face in range(4):
        for node in range(5):
            a, b = face_node(face, node)
            pick[face * 8 + node, a * 5 + b] = 1.0
    normal_x = np.repeat([1.0, 0.0, -1.0, 0.0], 8)
    normal_y = np.repeat([0.0, 1.0, 0.0, -1.0], 8)
    lift_x = pick.T * normal_x[None] * (0.5 * lift_gain)
    lift_y = pick.T * normal_y[None] * (0.5 * lift_gain)
    return dx, dy, pick, normal_x, normal_y, lift_x, lift_y


def build_tables():
    dx, dy, pick, _, _, lift_x, lift_y = element_tables()
    grad_x = np.concatenate([dx, lift_x], axis=1)
    grad_y = np.concatenate([dy, lift_y], axis=1)
    grad = np.concatenate([grad_x, grad_y, pick @ grad_x, pick @ grad_y], axis=0)
    volume = np.concatenate([-dx, -dy, lift_gain * pick.T], axis=1)
    late = lift_gain * 0.5 * viscosity * pick.T
    out = np.zeros((224, 384), ml_dtypes.bfloat16)
    out[:128, :192] = split_const(grad)
    out[:128, 192:288] = split_const(grad[:, 32:])
    out[128:160, :288] = split_const(volume)
    out[160:192, :96] = split_const(late)
    out[192:224, :32] = pick.astype(ml_dtypes.bfloat16)
    out[192:224, 32:64] = pick.astype(ml_dtypes.bfloat16)
    return out


def build_direct_tables():
    dx, dy, pick, normal_x, normal_y, lift_x, lift_y = element_tables()
    slope = normal_x[:, None] * (pick @ dx) + normal_y[:, None] * (pick @ dy)
    base = np.concatenate([-dx, -dy, viscosity * (dx @ dx + dy @ dy)], axis=1)
    jump = viscosity * (dx @ lift_x + dy @ lift_y)
    late = np.concatenate([lift_gain * pick.T, jump], axis=1)
    mirror = np.arange(32).reshape(4, 8)
    mirror[:, :5] = mirror[:, 4::-1]
    mirror = mirror.reshape(-1)
    first = np.zeros((128, LANES), ml_dtypes.bfloat16)
    first[:, :96] = split_const(
        np.concatenate([pick, slope, pick[mirror], slope[mirror]], axis=0)
    )
    out = np.zeros((64, 384), ml_dtypes.bfloat16)
    out[:32, :288] = split_const(base)
    out[32:, :192] = split_const(late)
    return first, out


def halves(x):
    high = x.astype(bf16)
    low = (x - high.astype(f32)).astype(bf16)
    return high, low


def dot(a, b):
    return lax.dot_general(a, b, (((1,), (0,)), ((), ())), preferred_element_type=f32)


def dot_t(a, b):
    return lax.dot_general(a, b, (((1,), (1,)), ((), ())), preferred_element_type=f32)


def dot3(table, x):
    high, low = halves(x)
    return dot(table, jnp.concatenate([high, high, low], axis=0))


def onehot(mask):
    return jnp.where(mask, 1.0, 0.0).astype(bf16)


def permute(x, perm):
    rows = x.shape[0]
    high, low = halves(x)
    both = dot(jnp.concatenate([high, low], axis=0), perm)
    return both[:rows] + both[rows:]


def iota(shape, dim):
    return lax.broadcasted_iota(jnp.int32, shape, dim)


def two_round_kernel(
    plan,
    state_hbm,
    neighbor_hbm,
    neighbor_face_hbm,
    seam_hbm,
    tables_hbm,
    change,
    state,
    neighbor,
    neighbor_face,
    seam,
    tables,
    padded,
    sent,
    arrived,
    own_faces,
    early_grads,
    early_change,
    load_sem,
    send_sem,
    recv_sem,
):
    elems, levels, curve_count, strip_count, links, rows_of, offsets = plan
    columns = elems * levels
    inner = LANES // elems
    outer_levels = levels // inner
    groups = 4 * outer_levels
    span = 4 * LANES
    total_rows = offsets[-1] + rows_of[-1]
    link_count = len(links)
    link_rows = -(-link_count // 8) * 8

    curve_pos = lax.axis_index("curve")
    strip_pos = lax.axis_index("sub")
    device_pos = curve_pos * strip_count + strip_pos
    places = []
    for axis, step in links:
        if axis == "curve":
            places.append((lax.rem(curve_pos + step + curve_count, curve_count), strip_pos))
        else:
            places.append((curve_pos, lax.rem(strip_pos + step + strip_count, strip_count)))

    barrier = pltpu.get_barrier_semaphore()
    for place in places:
        pl.semaphore_signal(
            barrier, inc=1, device_id=place, device_id_type=pl.DeviceIdType.MESH
        )
    loads = [
        pltpu.make_async_copy(source_ref, target_ref, load_sem.at[index])
        for index, (source_ref, target_ref) in enumerate(
            [
                (neighbor_hbm, neighbor),
                (neighbor_face_hbm, neighbor_face),
                (seam_hbm, seam),
                (state_hbm, state),
                (tables_hbm, tables),
            ]
        )
    ]
    for load in loads:
        load.start()
    for load in loads[:3]:
        load.wait()

    def widen(ref):
        block = ref[...]
        return jnp.concatenate([block] * inner, axis=1)

    across = widen(neighbor)
    face_back = widen(neighbor_face)
    codes = widen(seam)
    owner = across // elems
    place_in = across % elems
    turn = codes % 4
    flipped = codes // 4
    sub_level = iota((4, LANES), 1) // elems
    position = face_back * LANES + sub_level * elems + place_in
    source = jnp.where(owner == device_pos, position, -1)
    heading = (face_back + turn) % 4
    cosine = jnp.where(turn == 0, 1.0, 0.0) - jnp.where(turn == 2, 1.0, 0.0)
    sine = jnp.where(turn == 3, 1.0, 0.0) - jnp.where(turn == 1, 1.0, 0.0)
    head_x = jnp.where(heading == 0, 1.0, 0.0) - jnp.where(heading == 2, 1.0, 0.0)
    head_y = jnp.where(heading == 1, 1.0, 0.0) - jnp.where(heading == 3, 1.0, 0.0)

    link_iota = iota((link_rows, LANES), 0)
    target = jnp.full((link_rows, LANES), -1, jnp.int32)
    base = jnp.zeros((link_rows, LANES), f32)
    for index, place in enumerate(places):
        target = jnp.where(link_iota == index, place[0] * strip_count + place[1], target)
        base = jnp.where(link_iota == index, float(offsets[index] + 1), base)
    base = base + (iota((link_rows, LANES), 1) // elems).astype(f32)
    member = [
        jnp.where(owner[face : face + 1] == target, 1.0, 0.0) for face in range(4)
    ]
    from_lane = iota((LANES, 2 * LANES), 0)
    to_lane = iota((LANES, 2 * LANES), 1)
    same = from_lane // elems == (to_lane % LANES) // elems
    earlier = same & ((from_lane < to_lane) | (to_lane >= LANES))
    counts = dot(jnp.concatenate(member, axis=0).astype(bf16), onehot(earlier))
    before = jnp.zeros((link_rows, LANES), f32)
    slot_rows = []
    for face in range(4):
        part = counts[face * link_rows : (face + 1) * link_rows]
        rank = part[:, :LANES] + before
        before = before + part[:, LANES:]
        slot_rows.append(
            jnp.sum(member[face] * (base + inner * rank), axis=0, keepdims=True)
        )
    slot_row = jnp.concatenate(slot_rows, axis=1)
    pack = onehot(
        (iota((total_rows, span), 0) + 1).astype(f32)
        == jnp.broadcast_to(slot_row, (total_rows, span))
    )
    pack2 = jnp.concatenate([pack, pack], axis=1)

    def local_table():
        span_iota = iota((span, LANES), 0)
        return jnp.concatenate(
            [onehot(span_iota == source[face : face + 1]) for face in range(4)], axis=1
        )

    meta_iota = iota((8, LANES), 0)
    meta_blocks = []
    for face in range(4):
        block = jnp.zeros((8, LANES), f32)
        for row, values in enumerate(
            [flipped.astype(f32), cosine, sine, (position + 1).astype(f32)]
        ):
            block = jnp.where(meta_iota == row, values[face : face + 1], block)
        meta_blocks.append(block)
    meta = jnp.concatenate(meta_blocks, axis=1)
    heads_x = jnp.concatenate(
        [jnp.broadcast_to(head_x[face : face + 1], (8, LANES)) for face in range(4)], axis=0
    )
    heads_y = jnp.concatenate(
        [jnp.broadcast_to(head_y[face : face + 1], (8, LANES)) for face in range(4)], axis=0
    )

    def to_exchange(faces):
        return jnp.concatenate(
            [
                jnp.concatenate(
                    [
                        faces[face * 8 : face * 8 + 8, group * LANES : (group + 1) * LANES]
                        for face in range(4)
                    ],
                    axis=1,
                )
                for group in range(groups)
            ],
            axis=0,
        )

    def from_exchange(block):
        return jnp.concatenate(
            [
                jnp.concatenate(
                    [
                        block[group * 8 : group * 8 + 8, face * LANES : (face + 1) * LANES]
                        for group in range(groups)
                    ],
                    axis=1,
                )
                for face in range(4)
            ],
            axis=0,
        )

    data_lanes = groups * 8
    field_lanes = outer_levels * 8
    lane = iota((total_rows, LANES), 1)
    node_lane = lane % 8
    in_data = lane < data_lanes

    def copy_of(turn_index, index):
        rows = pl.ds(offsets[index], rows_of[index])
        return pltpu.make_async_remote_copy(
            src_ref=sent.at[turn_index, rows],
            dst_ref=arrived.at[turn_index, rows],
            send_sem=send_sem.at[turn_index, index],
            recv_sem=recv_sem.at[turn_index, index],
            device_id=places[index],
            device_id_type=pl.DeviceIdType.MESH,
        )

    def post(turn_index, block, flags):
        if flags is None:
            pieces = [block, meta]
            if data_lanes + 8 < LANES:
                pieces.append(jnp.zeros((LANES - data_lanes - 8, span), f32))
            block = jnp.concatenate(pieces, axis=0)
        high, low = halves(block)
        message = dot_t(pack2, jnp.concatenate([high, low], axis=1))
        if flags is None:
            flags = [
                jnp.broadcast_to(
                    message[:, data_lanes + index : data_lanes + index + 1], message.shape
                )
                for index in range(3)
            ]
        else:
            rest = jnp.zeros((total_rows, LANES - data_lanes), f32)
            message = jnp.concatenate([message, rest], axis=1)
        flip, cos, sin = flags
        mirrored = message
        for node, shift in ((0, LANES - 4), (1, LANES - 2), (3, 2), (4, 4)):
            mirrored = jnp.where(
                node_lane == node, pltpu.roll(message, shift, axis=1), mirrored
            )
        aligned = jnp.where(in_data & (flip > 0.5), mirrored, message)
        field = lane // field_lanes
        turned_u = cos * aligned - sin * pltpu.roll(aligned, LANES - field_lanes, axis=1)
        turned_v = cos * aligned + sin * pltpu.roll(aligned, field_lanes, axis=1)
        aligned = jnp.where(field == 1, turned_u, jnp.where(field == 2, turned_v, aligned))
        sent[turn_index] = aligned
        if turn_index == 0:
            pl.semaphore_wait(barrier, link_count)
        for index in range(link_count):
            copy_of(turn_index, index).start()
        return flags

    def gather_local(block):
        rows = block.shape[0]
        high, low = halves(block)
        both = dot(jnp.concatenate([high, low], axis=0), local_table())
        return both[:rows] + both[rows:]

    def await_all(turn_index):
        for index in range(link_count):
            copy_of(turn_index, index).wait_recv()

    def spread_table():
        message = arrived[0]
        spot = jnp.broadcast_to(
            message[:, data_lanes + 3 : data_lanes + 4], (total_rows, span)
        )
        return onehot((iota((total_rows, span), 1) + 1).astype(f32) == spot)

    def collect(turn_index, spread):
        message = arrived[turn_index]
        high, low = halves(jnp.transpose(message)[:data_lanes])
        both = dot(jnp.concatenate([high, low], axis=0), spread)
        return both[:data_lanes] + both[data_lanes:]

    row = iota((columns, columns), 0)
    col = iota((columns, columns), 1)
    to_level = onehot(row == (col % elems) * levels + col // elems)
    to_elem = onehot(row == (col % levels) * elems + col // levels)

    padded[...] = jnp.zeros_like(padded)
    for load in loads[3:]:
        load.wait()
    for field in range(4):
        padded[field, :25] = state[:, field, :]
    nodal = permute(padded[...].reshape(128, columns), to_level)
    values = jnp.concatenate(
        [nodal[field * 32 : field * 32 + 32] for field in range(4)], axis=1
    )
    high, low = halves(values)
    faces_in = dot(tables[192:224, :64], jnp.concatenate([high, low], axis=0))

    def fields_of(wide):
        return [wide[:, field * columns : (field + 1) * columns] for field in range(4)]

    def elementwise_lanes(wide):
        return permute(jnp.concatenate(fields_of(wide), axis=0), to_elem)

    def early_part(values, faces_in, faces_out, grad_x, grad_y, face_gx, face_gy, own_slope):
        face_of_row = iota((32, columns), 0) // 8
        normal_x = jnp.where(face_of_row == 0, 1.0, 0.0) - jnp.where(face_of_row == 2, 1.0, 0.0)
        normal_y = jnp.where(face_of_row == 1, 1.0, 0.0) - jnp.where(face_of_row == 3, 1.0, 0.0)

        def flux_of(faces):
            speed = faces[1] * normal_x + faces[2] * normal_y
            return [speed, faces[0] * normal_x, faces[0] * normal_y, faces[3] * speed], speed

        inside, outside = fields_of(faces_in), fields_of(faces_out)
        gx_in, gy_in = fields_of(face_gx), fields_of(face_gy)
        slope_own = fields_of(own_slope)
        flux_in, speed_in = flux_of(inside)
        flux_out, speed_out = flux_of(outside)
        wave = 1.0 + jnp.maximum(jnp.abs(speed_in), jnp.abs(speed_out))
        terms = []
        for field in range(4):
            slope_in = gx_in[field] * normal_x + gy_in[field] * normal_y
            jump = outside[field] - inside[field]
            terms.append(
                0.5 * (flux_in[field] - flux_out[field])
                - 0.5 * viscosity * (slope_in - slope_own[field])
                + (0.5 * wave + viscosity * penalty) * jump
            )
        face_term = jnp.concatenate(terms, axis=1)
        pressure, vel_u, vel_v, theta = fields_of(values)
        nothing = jnp.zeros_like(pressure)
        flux_x = jnp.concatenate([vel_u, pressure, nothing, theta * vel_u], axis=1)
        flux_y = jnp.concatenate([vel_v, nothing, pressure, theta * vel_v], axis=1)
        tendency = dot3(
            tables[128:160, :288],
            jnp.concatenate(
                [flux_x - viscosity * grad_x, flux_y - viscosity * grad_y, face_term], axis=0
            ),
        )

        return elementwise_lanes(tendency)

    block_in = to_exchange(faces_in)
    flags = post(0, block_in, None)
    always = device_pos >= 0

    @pl.when(always)
    def _():
        own = from_exchange(gather_local(block_in))
        own_faces[...] = own
        early_grads[...] = dot3(
            tables[:128, :192], jnp.concatenate([values, own - faces_in], axis=0)
        )

    await_all(0)
    spread = spread_table()
    far_faces = from_exchange(collect(0, spread))
    face_grads = early_grads[64:128] + dot3(tables[64:128, 192:288], far_faces)
    face_gx, face_gy = face_grads[:32], face_grads[32:]
    wide_x = jnp.concatenate([heads_x] * groups, axis=1)
    wide_y = jnp.concatenate([heads_y] * groups, axis=1)
    block_grad = to_exchange(face_gx * wide_x + face_gy * wide_y)
    post(1, block_grad, flags)

    @pl.when(always)
    def _():
        own_slope = from_exchange(gather_local(block_grad))
        grads = early_grads[:64] + dot3(tables[:64, 192:288], far_faces)
        faces_out = own_faces[...] + far_faces
        grad_x, grad_y = grads[:32], grads[32:]
        early_change[...] = early_part(
            values, faces_in, faces_out, grad_x, grad_y, face_gx, face_gy, own_slope
        )

    await_all(1)
    far_slope = from_exchange(collect(1, spread))
    late = elementwise_lanes(dot3(tables[160:192, :96], far_slope))
    total = early_change[...] + late
    for field in range(4):
        change[:, field, :] = total[field * 32 : field * 32 + 25]

    for turn_index in range(2):
        for index in range(link_count):
            copy_of(turn_index, index).wait_send()


def direct_kernel(
    plan,
    state_hbm,
    neighbor_hbm,
    neighbor_face_hbm,
    seam_hbm,
    face_tables_hbm,
    tables_hbm,
    register_hbm,
    own_part,
    late_part,
    sideways,
    state,
    indices,
    face_tables,
    tables,
    padded,
    sent,
    arrived,
    notice,
    notices,
    verdict,
    spread,
    known,
    register,
    index_sem,
    load_sem,
    send_sem,
    recv_sem,
    notice_send_sem,
    notice_recv_sem,
    verdict_send_sem,
    verdict_recv_sem,
):
    elems, levels, curve_count, strip_count, links, rows_of, offsets = plan
    columns = elems * levels
    span = 4 * columns
    inner = LANES // elems
    outer_levels = levels // inner
    total_rows = offsets[-1] + rows_of[-1]
    link_count = len(links)
    link_rows = -(-link_count // 8) * 8
    half = LANES // outer_levels

    curve_pos = lax.axis_index("curve")
    strip_pos = lax.axis_index("sub")
    device_pos = curve_pos * strip_count + strip_pos

    def place_at(curve_step, strip_step):
        return (
            lax.rem(curve_pos + curve_step + curve_count, curve_count),
            lax.rem(strip_pos + strip_step + strip_count, strip_count),
        )

    places = [place_at(step, 0) if axis == "curve" else place_at(0, step) for axis, step in links]
    device_count = curve_count * strip_count
    herald = device_count // 2 - 1
    collectors = (0, 1, herald)
    collects = (device_pos < 2) | (device_pos == herald)

    def place_of(position):
        return (position // strip_count, position % strip_count)

    def tell(place):
        pl.semaphore_signal(
            barrier, inc=1, device_id=place, device_id_type=pl.DeviceIdType.MESH
        )

    def notice_to(position):
        return pltpu.make_async_remote_copy(
            src_ref=notice.at[pl.ds(0, 1)],
            dst_ref=notices.at[pl.ds(device_pos, 1)],
            send_sem=notice_send_sem,
            recv_sem=notice_recv_sem,
            device_id=place_of(position),
            device_id_type=pl.DeviceIdType.MESH,
        )

    def verdict_to(position):
        return pltpu.make_async_remote_copy(
            src_ref=notice.at[pl.ds(8, 1)],
            dst_ref=verdict.at[pl.ds(0, 1)],
            send_sem=verdict_send_sem,
            recv_sem=verdict_recv_sem,
            device_id=place_of(position),
            device_id_type=pl.DeviceIdType.MESH,
        )

    def rows_done(ref, count, semaphore):
        rows = ref.at[pl.ds(0, count)]
        return pltpu.make_async_copy(rows, rows, semaphore)

    def copy_of(index):
        rows = pl.ds(offsets[index], rows_of[index])
        return pltpu.make_async_remote_copy(
            src_ref=sent.at[rows],
            dst_ref=arrived.at[rows],
            send_sem=send_sem,
            recv_sem=recv_sem,
            device_id=places[index],
            device_id_type=pl.DeviceIdType.MESH,
        )

    index_loads = [
        pltpu.make_async_copy(source_ref, indices.at[index], index_sem)
        for index, source_ref in enumerate((neighbor_hbm, neighbor_face_hbm, seam_hbm))
    ]
    loads = [
        pltpu.make_async_copy(source_ref, target_ref, load_sem.at[index])
        for index, (source_ref, target_ref) in enumerate(
            [
                (face_tables_hbm, face_tables),
                (tables_hbm, tables),
                (register_hbm, register),
            ]
        )
    ]
    nodes = state.shape[0]
    piece = -(-nodes // 5)
    state_loads = [
        pltpu.make_async_copy(
            state_hbm.at[pl.ds(start, min(piece, nodes - start))],
            state.at[pl.ds(start, min(piece, nodes - start))],
            load_sem.at[3],
        )
        for start in range(0, nodes, piece)
    ]
    for load in index_loads + state_loads + loads:
        load.start()
    notices[...] = jnp.zeros_like(notices)
    barrier = pltpu.get_barrier_semaphore()
    for place in places:
        tell(place)
    for collector in collectors:

        @pl.when(device_pos == collector)
        def _():
            for position in range(device_count - 1, -1, -1):
                if position != collector:
                    tell(place_of(position))

    padded[...] = jnp.zeros_like(padded)
    level = iota((8, columns), 1) % levels
    link_iota = iota((link_rows, LANES), 0)
    wide_iota = iota((link_rows, columns), 0)
    target = jnp.full((link_rows, LANES), -1, jnp.int32)
    base_wide = jnp.zeros((link_rows, columns), f32)
    base_back = jnp.zeros((link_rows, LANES), f32)
    for index, place in enumerate(places):
        target = jnp.where(link_iota == index, place[0] * strip_count + place[1], target)
        base_wide = jnp.where(wide_iota == index, float(offsets[index] + 1), base_wide)
        base_back = jnp.where(link_iota == index, float(offsets[index ^ 1] + 1), base_back)
    from_elem = iota((LANES, columns), 0)
    to_elem = iota((LANES, columns), 1) // levels
    reach = jnp.concatenate(
        [
            onehot((from_elem < elems) & (from_elem < to_elem)),
            onehot(from_elem < elems),
            onehot(from_elem == to_elem),
        ],
        axis=1,
    )
    pltpu.make_async_copy(indices, indices, index_sem).wait()

    across, face_back, codes = [
        jnp.concatenate([indices[index]] * inner, axis=1) for index in range(3)
    ]
    owner = across // elems
    place_in = across % elems
    turn = codes % 4
    flipped = codes // 4
    own_face = iota((4, LANES), 0)
    quarter = (face_back + turn - own_face + 4) % 4
    odd = jnp.where(quarter % 2 == 1, 1.0, 0.0)
    notice[:8] = jnp.broadcast_to(jnp.sum(odd, axis=0, keepdims=True), (8, LANES))
    early = device_pos >= device_count - strip_count // 2

    def meet_and_notify():
        pl.semaphore_wait(barrier, link_count + len(collectors) - jnp.where(collects, 1, 0))
        for collector in collectors:

            @pl.when(device_pos != collector)
            def _():
                notice_to(collector).start()

    pl.when(early)(meet_and_notify)
    side = jnp.where(quarter == 0, 1.0, -1.0)
    cosine = jnp.where(turn == 0, 1.0, 0.0) - jnp.where(turn == 2, 1.0, 0.0)
    sine = jnp.where(turn == 3, 1.0, 0.0) - jnp.where(turn == 1, 1.0, 0.0)

    member = [
        jnp.where(owner[face : face + 1] == target, 1.0, 0.0) for face in range(4)
    ]
    extras = [
        jnp.concatenate([part, jnp.zeros_like(part)], axis=0)
        for part in (flipped.astype(f32), cosine, sine, side)
    ]
    wide = dot(jnp.concatenate(member + extras, axis=0).astype(bf16), reach)
    before = jnp.zeros((link_rows, columns), f32)
    spots = []
    for face in range(4):
        part = wide[face * link_rows : (face + 1) * link_rows]
        rank = part[:, :columns] + before
        before = before + part[:, columns : 2 * columns]
        chosen = part[:, 2 * columns :] * (base_wide + inner * rank)
        spots.append(jnp.sum(chosen, axis=0, keepdims=True))
    extra_row = 4 * link_rows
    flip_wide, cos_wide, sin_wide, side_wide = [
        wide[extra_row + 8 * index : extra_row + 8 * index + 8, 2 * columns :]
        for index in range(4)
    ]

    def stretched(per_face):
        rows = []
        for values in per_face:
            rows.append(values)
            rows.append(jnp.zeros_like(values))
        wide = dot(jnp.concatenate(rows, axis=0).astype(bf16), reach[:, 2 * columns :])
        return [wide[8 * index : 8 * index + 8] for index in range(len(per_face))]

    def rows_for(slot, stride):
        spot = slot + (level[:1] % inner + level[:1] // inner * stride).astype(f32)
        return jnp.where(slot > 0.5, spot, 0.0)

    def hot_rows(count, spots):
        count_iota = (iota((count, columns), 0) + 1).astype(f32)
        return jnp.concatenate(
            [
                onehot(
                    count_iota == jnp.broadcast_to(spots[face], (count, columns))
                )
                for face in range(4)
            ],
            axis=1,
        )

    pack = hot_rows(total_rows, [rows_for(spot, 0) for spot in spots])

    def over_faces(wide, rows):
        return jnp.concatenate(
            [jnp.broadcast_to(wide[face : face + 1], (rows, columns)) for face in range(4)],
            axis=1,
        )

    def to_fields(block):
        return jnp.concatenate(
            [
                jnp.concatenate(
                    [
                        block[face * 8 : face * 8 + 8, field * columns : (field + 1) * columns]
                        for face in range(4)
                    ],
                    axis=1,
                )
                for field in range(4)
            ],
            axis=0,
        )

    def to_faces(block):
        return jnp.concatenate(
            [
                jnp.concatenate(
                    [
                        block[field * 8 : field * 8 + 8, face * columns : (face + 1) * columns]
                        for field in range(4)
                    ],
                    axis=1,
                )
                for face in range(4)
            ],
            axis=0,
        )

    flip_all, cos_all, sin_all, side_all = [
        over_faces(wide, 8) for wide in (flip_wide, cos_wide, sin_wide, side_wide)
    ]
    level_all = iota((half, span), 1) % levels // inner

    loads[0].wait()
    pltpu.make_async_copy(state, state, load_sem.at[3]).wait()
    for field in range(4):
        padded[field, :25] = state[:, field, :]
    values = jnp.concatenate([padded[field] for field in range(4)], axis=1)
    on_faces = dot3(face_tables[:, :96], values)
    traces, slopes, flipped_traces, flipped_slopes = [
        to_fields(on_faces[32 * part : 32 * part + 32]) for part in range(4)
    ]

    def aligned(plain, mirrored):
        parts = [
            jnp.where(
                flip_all > 0.5,
                mirrored[field * 8 : field * 8 + 8],
                plain[field * 8 : field * 8 + 8],
            )
            for field in range(4)
        ]
        parts[1], parts[2] = (
            cos_all * parts[1] - sin_all * parts[2],
            cos_all * parts[2] + sin_all * parts[1],
        )
        return parts

    message = aligned(traces, flipped_traces) + [
        side_all * part for part in aligned(slopes, flipped_slopes)
    ]
    high, low = halves(jnp.concatenate(message, axis=0))
    pieces = []
    for part in (high, low):
        for index in range(outer_levels):
            pieces.append(jnp.where(level_all == index, part, jnp.zeros_like(part)))
    stacked = dot_t(pack, jnp.concatenate(pieces, axis=0))
    sent[...] = stacked[:, :LANES] + stacked[:, LANES:]
    pl.when(jnp.logical_not(early))(meet_and_notify)
    for index in range(link_count):
        copy_of(index).start()
    always = device_pos >= 0

    @pl.when(always)
    def _():
        first_of = owner * (4 * elems)
        key = (first_of + face_back * elems + place_in).astype(f32)
        first_of = first_of.astype(f32)
        key_down = jnp.transpose(jnp.concatenate([key, key], axis=0))
        back_rows = []
        for face in range(4):
            smaller = jnp.zeros((elems, LANES), f32)
            for other in range(4):
                rival = jnp.broadcast_to(key_down[:elems, other : other + 1], (elems, LANES))
                mine = (rival < key[face : face + 1]) & (rival >= first_of[face : face + 1])
                smaller = smaller + jnp.where(mine, 1.0, 0.0)
            rank = jnp.sum(smaller, axis=0, keepdims=True)
            back_rows.append(
                jnp.sum(member[face] * (base_back + inner * rank), axis=0, keepdims=True)
            )
        at_home = owner == device_pos
        homes = [
            jnp.where(at_home & (face_back == face), place_in + 1, 0).astype(f32)
            for face in range(4)
        ]
        back, *homes = stretched([jnp.concatenate(back_rows, axis=0)] + homes)
        spread[...] = hot_rows(
            outer_levels * LANES,
            [rows_for(back[face : face + 1], LANES) for face in range(4)],
        )

        slopes_out = slopes * over_faces(side_wide, 32)
        both_high, both_low = halves(jnp.concatenate([traces, slopes_out], axis=0))
        both = jnp.concatenate([both_high, both_low], axis=0)
        found = jnp.zeros((128, span), f32)
        for face in range(4):
            home_spot = jnp.where(
                homes[face] > 0.5, homes[face] * levels + (level - levels + 1).astype(f32), 0.0
            )
            found = found + dot(
                both[:, face * columns : (face + 1) * columns],
                hot_rows(columns, [home_spot[into : into + 1] for into in range(4)]),
            )
        found = found[:64] + found[64:]
        known[:32] = traces
        known[32:64] = found[:32]
        known[64:96] = found[32:] - slopes
        known[96:128] = over_faces(
            0.5 + viscosity * penalty - 0.25 * lift_gain * viscosity * (1.0 + side_wide), 32
        )
        pressure, vel_u, vel_v, theta = [
            values[:, field * columns : (field + 1) * columns] for field in range(4)
        ]
        nothing = jnp.zeros_like(pressure)
        flux_x = jnp.concatenate([vel_u, pressure, nothing, theta * vel_u], axis=1)
        flux_y = jnp.concatenate([vel_v, nothing, pressure, theta * vel_v], axis=1)
        loads[1].wait()
        loads[2].wait()
        for field in range(4):
            padded[field, :25] = register[:, field, :]
        held = jnp.concatenate([padded[field] for field in range(4)], axis=1)
        own = dot3(tables[:32, :288], jnp.concatenate([flux_x, flux_y, values], axis=0))
        own = section_a * held + step_size * own
        for field in range(4):
            own_part[:, field, :] = own[:25, field * columns : (field + 1) * columns]

    rows_done(arrived, total_rows, recv_sem).wait()
    filler = jnp.zeros((LANES - total_rows, LANES), f32)
    turned = jnp.transpose(jnp.concatenate([arrived[...], filler], axis=0))
    turned = jnp.concatenate(
        [turned[half * index : half * (index + 1)] for index in range(outer_levels)], axis=1
    )
    high, low = halves(turned)
    far = dot(jnp.concatenate([high, low], axis=0), spread[...])
    far = far[:half] + far[half:]
    inside = known[:32]
    outside = known[32:64] + far[:32]
    jump = outside - inside
    slope_term = (0.5 * viscosity) * (known[64:96] + far[32:])
    weight = known[96:128]
    terms = []
    for face in range(4):
        sides = slice(face * columns, (face + 1) * columns)
        ins = [inside[field * 8 : field * 8 + 8, sides] for field in range(4)]
        outs = [outside[field * 8 : field * 8 + 8, sides] for field in range(4)]
        step = [jump[field * 8 : field * 8 + 8, sides] for field in range(4)]
        normal = 1 + face % 2
        sign = 1.0 if face < 2 else -1.0
        raw_in, raw_out = ins[normal], outs[normal]
        wave = weight[:8, sides] + 0.5 * jnp.maximum(jnp.abs(raw_in), jnp.abs(raw_out))
        drops = [
            (-0.5 * sign) * step[normal],
            None,
            None,
            (0.5 * sign) * (ins[3] * raw_in - outs[3] * raw_out),
        ]
        drops[normal] = (-0.5 * sign) * step[0]
        rows = []
        for field in range(4):
            term = wave * step[field] + slope_term[field * 8 : field * 8 + 8, sides]
            rows.append(term if drops[field] is None else term + drops[field])
        terms.append(jnp.concatenate(rows, axis=0))
    face_term = jnp.concatenate(terms, axis=1)
    late = dot3(
        tables[32:, :192], jnp.concatenate([to_faces(face_term), to_faces(jump)], axis=0)
    )
    for field in range(4):
        late_part[:, field, :] = late[:25, field * columns : (field + 1) * columns]

    @pl.when(collects)
    def _():
        rows_done(notices, device_count - 1, notice_recv_sem).wait()
        heard = jnp.max(notices[...], axis=0, keepdims=True) + notice[:1]
        notice[8:] = jnp.broadcast_to(heard, (8, LANES))

        @pl.when(device_pos == herald)
        def _():
            for position in range(device_count):
                if position not in collectors:
                    verdict_to(position).start()

        sideways[0] = jnp.where(jnp.max(heard) > 0.5, 1, 0)

        @pl.when(device_pos == herald)
        def _():
            rows_done(notices, device_count - len(collectors), verdict_send_sem).wait()

        rows_done(notice, len(collectors) - 1, notice_send_sem).wait()

    @pl.when(jnp.logical_not(collects))
    def _():
        rows_done(notice, len(collectors), notice_send_sem).wait()
        rows_done(verdict, 1, verdict_recv_sem).wait()
        sideways[0] = jnp.where(jnp.max(verdict[:1]) > 0.5, 1, 0)

    rows_done(sent, total_rows, send_sem).wait()


def body(curve_count, strip_count, state, register, neighbor, neighbor_face, seam):
    elems = neighbor.shape[1]
    columns = state.shape[2]
    levels = columns // elems
    inner = LANES // elems
    outer_levels = levels // inner
    reach = min(7, (curve_count - 1) // 2)
    slots = (TW + reach - 1) // reach
    links, rows_of = [], []
    for distance in range(reach, 0, -1):
        for direction in (1, -1):
            links.append(("curve", direction * distance))
            rows_of.append(-(-slots * inner // 8) * 8)
    for direction in (1, -1):
        links.append(("sub", direction))
        rows_of.append(-(-TW * inner // 8) * 8)
    offsets = [sum(rows_of[:index]) for index in range(len(links))]
    total_rows = sum(rows_of)
    plan = (elems, levels, curve_count, strip_count, links, rows_of, offsets)
    vmem = pl.BlockSpec(memory_space=pltpu.VMEM)
    nodes_first = jnp.transpose(state, (1, 0, 2))
    register_first = jnp.transpose(register, (1, 0, 2))
    shape = nodes_first.shape

    def call(kernel, tables, more, outputs, out_specs, scratch, collective_id):
        tables = [jnp.asarray(table) for table in tables]
        operands = (nodes_first, neighbor, neighbor_face, seam, *tables, *more)
        return pl.pallas_call(
            functools.partial(kernel, plan),
            out_shape=outputs,
            in_specs=[pl.BlockSpec(memory_space=pl.ANY)] * len(operands),
            out_specs=out_specs,
            scratch_shapes=scratch,
            compiler_params=pltpu.CompilerParams(
                collective_id=collective_id, has_side_effects=True
            ),
        )(*[pltpu.with_memory_space_constraint(operand, pltpu.HBM) for operand in operands])

    def two_rounds():
        change = call(
            two_round_kernel,
            (build_tables(),),
            (),
            pltpu.VMEM(nodes_first.shape, f32),
            vmem,
            [
                pltpu.VMEM(shape, f32),
                pltpu.VMEM(neighbor.shape, jnp.int32),
                pltpu.VMEM(neighbor.shape, jnp.int32),
                pltpu.VMEM(neighbor.shape, jnp.int32),
                pltpu.VMEM((224, 384), bf16),
                pltpu.VMEM((4, 32, columns), f32),
                pltpu.VMEM((2, total_rows, LANES), f32),
                pltpu.VMEM((2, total_rows, LANES), f32),
                pltpu.VMEM((32, 4 * columns), f32),
                pltpu.VMEM((128, 4 * columns), f32),
                pltpu.VMEM((128, columns), f32),
                pltpu.SemaphoreType.DMA((5,)),
                pltpu.SemaphoreType.DMA((2, len(links))),
                pltpu.SemaphoreType.DMA((2, len(links))),
            ],
            0,
        )
        return section_a * register_first, change

    device_count = curve_count * strip_count
    if device_count <= DIRECT_LIMIT and total_rows <= LANES and outer_levels * 64 == LANES:
        *parts, sideways = call(
            direct_kernel,
            build_direct_tables(),
            (register_first,),
            (pltpu.VMEM(shape, f32), pltpu.VMEM(shape, f32), pltpu.SMEM((1,), jnp.int32)),
            (vmem, vmem, pl.BlockSpec(memory_space=pltpu.SMEM)),
            [
                pltpu.VMEM(shape, f32),
                pltpu.VMEM((3, *neighbor.shape), jnp.int32),
                pltpu.VMEM((128, LANES), bf16),
                pltpu.VMEM((64, 384), bf16),
                pltpu.VMEM((4, 32, columns), f32),
                pltpu.VMEM((total_rows, LANES), f32),
                pltpu.VMEM((total_rows, LANES), f32),
                pltpu.VMEM((16, LANES), f32),
                pltpu.VMEM((-(-device_count // 8) * 8, LANES), f32),
                pltpu.VMEM((8, LANES), f32),
                pltpu.VMEM((outer_levels * LANES, 4 * columns), bf16),
                pltpu.VMEM((128, 4 * columns), f32),
                pltpu.VMEM(shape, f32),
                pltpu.SemaphoreType.DMA,
                pltpu.SemaphoreType.DMA((4,)),
                pltpu.SemaphoreType.DMA,
                pltpu.SemaphoreType.DMA,
                pltpu.SemaphoreType.DMA,
                pltpu.SemaphoreType.DMA,
                pltpu.SemaphoreType.DMA,
                pltpu.SemaphoreType.DMA,
            ],
            1,
        )
        own, late = lax.cond(
            sideways[0] == 0, lambda kept: tuple(kept), lambda _: two_rounds(), parts
        )
    else:
        own, late = two_rounds()
    next_register = jnp.transpose(own, (1, 0, 2)) + step_size * jnp.transpose(late, (1, 0, 2))
    return state + section_b * next_register, next_register


def solution(mesh):
    wide = P(None, None, ("curve", "sub"))
    flat = P(None, ("curve", "sub"))
    return jax.shard_map(
        functools.partial(body, mesh.shape["curve"], mesh.shape["sub"]),
        mesh=mesh,
        in_specs=(wide, wide, flat, flat, flat),
        out_specs=(wide, wide),
        check_vma=False,
    )
```

```python
import functools
import math

import jax
import jax.numpy as jnp
import ml_dtypes
import numpy as np
from jax import lax
from jax.experimental import pallas as pl
from jax.experimental.pallas import tpu as pltpu
from jax.sharding import PartitionSpec as P

TW = 8
LANES = 128
DIRECT_LIMIT = 64

lift_gain = 10.0
step_size = 0.02
viscosity = 0.05
penalty = 2.0
section_a = -567301805773.0 / 1357537059087.0
section_b = 2404267990393.0 / 2016746695238.0

f32 = jnp.float32
bf16 = jnp.bfloat16


def build_derivative():
    points = np.array([-1.0, -math.sqrt(3.0 / 7.0), 0.0, math.sqrt(3.0 / 7.0), 1.0])
    weights = np.array(
        [
            1.0 / np.prod([points[row] - points[col] for col in range(5) if col != row])
            for row in range(5)
        ]
    )
    table = np.zeros((5, 5))
    for row in range(5):
        for col in range(5):
            if row != col:
                table[row, col] = weights[col] / weights[row] / (points[row] - points[col])
        table[row, row] = -np.sum(table[row])
    return table


def face_node(face, node):
    return [(4, node), (node, 4), (0, node), (node, 0)][face]


def split_const(table):
    high = table.astype(ml_dtypes.bfloat16)
    low = (table - high.astype(np.float64)).astype(ml_dtypes.bfloat16)
    return np.concatenate([high, low, high], axis=1)


def element_tables():
    d = build_derivative()
    eye = np.eye(5)
    dx = np.zeros((32, 32))
    dy = np.zeros((32, 32))
    dx[:25, :25] = np.kron(d, eye)
    dy[:25, :25] = np.kron(eye, d)
    pick = np.zeros((32, 32))
    for face in range(4):
        for node in range(5):
            a, b = face_node(face, node)
            pick[face * 8 + node, a * 5 + b] = 1.0
    normal_x = np.repeat([1.0, 0.0, -1.0, 0.0], 8)
    normal_y = np.repeat([0.0, 1.0, 0.0, -1.0], 8)
    lift_x = pick.T * normal_x[None] * (0.5 * lift_gain)
    lift_y = pick.T * normal_y[None] * (0.5 * lift_gain)
    return dx, dy, pick, normal_x, normal_y, lift_x, lift_y


def build_tables():
    dx, dy, pick, _, _, lift_x, lift_y = element_tables()
    grad_x = np.concatenate([dx, lift_x], axis=1)
    grad_y = np.concatenate([dy, lift_y], axis=1)
    grad = np.concatenate([grad_x, grad_y, pick @ grad_x, pick @ grad_y], axis=0)
    volume = np.concatenate([-dx, -dy, lift_gain * pick.T], axis=1)
    late = lift_gain * 0.5 * viscosity * pick.T
    out = np.zeros((224, 384), ml_dtypes.bfloat16)
    out[:128, :192] = split_const(grad)
    out[:128, 192:288] = split_const(grad[:, 32:])
    out[128:160, :288] = split_const(volume)
    out[160:192, :96] = split_const(late)
    out[192:224, :32] = pick.astype(ml_dtypes.bfloat16)
    out[192:224, 32:64] = pick.astype(ml_dtypes.bfloat16)
    return out


def build_direct_tables():
    dx, dy, pick, normal_x, normal_y, lift_x, lift_y = element_tables()
    slope = normal_x[:, None] * (pick @ dx) + normal_y[:, None] * (pick @ dy)
    base = np.concatenate([-dx, -dy, viscosity * (dx @ dx + dy @ dy)], axis=1)
    jump = viscosity * (dx @ lift_x + dy @ lift_y)
    late = np.concatenate([lift_gain * pick.T, jump], axis=1)
    mirror = np.arange(32).reshape(4, 8)
    mirror[:, :5] = mirror[:, 4::-1]
    mirror = mirror.reshape(-1)
    first = np.zeros((128, LANES), ml_dtypes.bfloat16)
    first[:, :96] = split_const(
        np.concatenate([pick, slope, pick[mirror], slope[mirror]], axis=0)
    )
    out = np.zeros((64, 384), ml_dtypes.bfloat16)
    out[:32, :288] = split_const(base)
    out[32:, :192] = split_const(late)
    return first, out


def halves(x):
    high = x.astype(bf16)
    low = (x - high.astype(f32)).astype(bf16)
    return high, low


def dot(a, b):
    return lax.dot_general(a, b, (((1,), (0,)), ((), ())), preferred_element_type=f32)


def dot_t(a, b):
    return lax.dot_general(a, b, (((1,), (1,)), ((), ())), preferred_element_type=f32)


def dot3(table, x):
    high, low = halves(x)
    return dot(table, jnp.concatenate([high, high, low], axis=0))


def onehot(mask):
    return jnp.where(mask, 1.0, 0.0).astype(bf16)


def permute(x, perm):
    rows = x.shape[0]
    high, low = halves(x)
    both = dot(jnp.concatenate([high, low], axis=0), perm)
    return both[:rows] + both[rows:]


def iota(shape, dim):
    return lax.broadcasted_iota(jnp.int32, shape, dim)


def two_round_kernel(
    plan,
    state_hbm,
    neighbor_hbm,
    neighbor_face_hbm,
    seam_hbm,
    tables_hbm,
    change,
    state,
    neighbor,
    neighbor_face,
    seam,
    tables,
    padded,
    sent,
    arrived,
    own_faces,
    early_grads,
    early_change,
    load_sem,
    send_sem,
    recv_sem,
):
    elems, levels, curve_count, strip_count, links, rows_of, offsets = plan
    columns = elems * levels
    inner = LANES // elems
    outer_levels = levels // inner
    groups = 4 * outer_levels
    span = 4 * LANES
    total_rows = offsets[-1] + rows_of[-1]
    link_count = len(links)
    link_rows = -(-link_count // 8) * 8

    curve_pos = lax.axis_index("curve")
    strip_pos = lax.axis_index("sub")
    device_pos = curve_pos * strip_count + strip_pos
    places = []
    for axis, step in links:
        if axis == "curve":
            places.append((lax.rem(curve_pos + step + curve_count, curve_count), strip_pos))
        else:
            places.append((curve_pos, lax.rem(strip_pos + step + strip_count, strip_count)))

    barrier = pltpu.get_barrier_semaphore()
    for place in places:
        pl.semaphore_signal(
            barrier, inc=1, device_id=place, device_id_type=pl.DeviceIdType.MESH
        )
    loads = [
        pltpu.make_async_copy(source_ref, target_ref, load_sem.at[index])
        for index, (source_ref, target_ref) in enumerate(
            [
                (neighbor_hbm, neighbor),
                (neighbor_face_hbm, neighbor_face),
                (seam_hbm, seam),
                (state_hbm, state),
                (tables_hbm, tables),
            ]
        )
    ]
    for load in loads:
        load.start()
    for load in loads[:3]:
        load.wait()

    def widen(ref):
        block = ref[...]
        return jnp.concatenate([block] * inner, axis=1)

    across = widen(neighbor)
    face_back = widen(neighbor_face)
    codes = widen(seam)
    owner = across // elems
    place_in = across % elems
    turn = codes % 4
    flipped = codes // 4
    sub_level = iota((4, LANES), 1) // elems
    position = face_back * LANES + sub_level * elems + place_in
    source = jnp.where(owner == device_pos, position, -1)
    heading = (face_back + turn) % 4
    cosine = jnp.where(turn == 0, 1.0, 0.0) - jnp.where(turn == 2, 1.0, 0.0)
    sine = jnp.where(turn == 3, 1.0, 0.0) - jnp.where(turn == 1, 1.0, 0.0)
    head_x = jnp.where(heading == 0, 1.0, 0.0) - jnp.where(heading == 2, 1.0, 0.0)
    head_y = jnp.where(heading == 1, 1.0, 0.0) - jnp.where(heading == 3, 1.0, 0.0)

    link_iota = iota((link_rows, LANES), 0)
    target = jnp.full((link_rows, LANES), -1, jnp.int32)
    base = jnp.zeros((link_rows, LANES), f32)
    for index, place in enumerate(places):
        target = jnp.where(link_iota == index, place[0] * strip_count + place[1], target)
        base = jnp.where(link_iota == index, float(offsets[index] + 1), base)
    base = base + (iota((link_rows, LANES), 1) // elems).astype(f32)
    member = [
        jnp.where(owner[face : face + 1] == target, 1.0, 0.0) for face in range(4)
    ]
    from_lane = iota((LANES, 2 * LANES), 0)
    to_lane = iota((LANES, 2 * LANES), 1)
    same = from_lane // elems == (to_lane % LANES) // elems
    earlier = same & ((from_lane < to_lane) | (to_lane >= LANES))
    counts = dot(jnp.concatenate(member, axis=0).astype(bf16), onehot(earlier))
    before = jnp.zeros((link_rows, LANES), f32)
    slot_rows = []
    for face in range(4):
        part = counts[face * link_rows : (face + 1) * link_rows]
        rank = part[:, :LANES] + before
        before = before + part[:, LANES:]
        slot_rows.append(
            jnp.sum(member[face] * (base + inner * rank), axis=0, keepdims=True)
        )
    slot_row = jnp.concatenate(slot_rows, axis=1)
    pack = onehot(
        (iota((total_rows, span), 0) + 1).astype(f32)
        == jnp.broadcast_to(slot_row, (total_rows, span))
    )
    pack2 = jnp.concatenate([pack, pack], axis=1)

    def local_table():
        span_iota = iota((span, LANES), 0)
        return jnp.concatenate(
            [onehot(span_iota == source[face : face + 1]) for face in range(4)], axis=1
        )

    meta_iota = iota((8, LANES), 0)
    meta_blocks = []
    for face in range(4):
        block = jnp.zeros((8, LANES), f32)
        for row, values in enumerate(
            [flipped.astype(f32), cosine, sine, (position + 1).astype(f32)]
        ):
            block = jnp.where(meta_iota == row, values[face : face + 1], block)
        meta_blocks.append(block)
    meta = jnp.concatenate(meta_blocks, axis=1)
    heads_x = jnp.concatenate(
        [jnp.broadcast_to(head_x[face : face + 1], (8, LANES)) for face in range(4)], axis=0
    )
    heads_y = jnp.concatenate(
        [jnp.broadcast_to(head_y[face : face + 1], (8, LANES)) for face in range(4)], axis=0
    )

    def to_exchange(faces):
        return jnp.concatenate(
            [
                jnp.concatenate(
                    [
                        faces[face * 8 : face * 8 + 8, group * LANES : (group + 1) * LANES]
                        for face in range(4)
                    ],
                    axis=1,
                )
                for group in range(groups)
            ],
            axis=0,
        )

    def from_exchange(block):
        return jnp.concatenate(
            [
                jnp.concatenate(
                    [
                        block[group * 8 : group * 8 + 8, face * LANES : (face + 1) * LANES]
                        for group in range(groups)
                    ],
                    axis=1,
                )
                for face in range(4)
            ],
            axis=0,
        )

    data_lanes = groups * 8
    field_lanes = outer_levels * 8
    lane = iota((total_rows, LANES), 1)
    node_lane = lane % 8
    in_data = lane < data_lanes

    def copy_of(turn_index, index):
        rows = pl.ds(offsets[index], rows_of[index])
        return pltpu.make_async_remote_copy(
            src_ref=sent.at[turn_index, rows],
            dst_ref=arrived.at[turn_index, rows],
            send_sem=send_sem.at[turn_index, index],
            recv_sem=recv_sem.at[turn_index, index],
            device_id=places[index],
            device_id_type=pl.DeviceIdType.MESH,
        )

    def post(turn_index, block, flags):
        if flags is None:
            pieces = [block, meta]
            if data_lanes + 8 < LANES:
                pieces.append(jnp.zeros((LANES - data_lanes - 8, span), f32))
            block = jnp.concatenate(pieces, axis=0)
        high, low = halves(block)
        message = dot_t(pack2, jnp.concatenate([high, low], axis=1))
        if flags is None:
            flags = [
                jnp.broadcast_to(
                    message[:, data_lanes + index : data_lanes + index + 1], message.shape
                )
                for index in range(3)
            ]
        else:
            rest = jnp.zeros((total_rows, LANES - data_lanes), f32)
            message = jnp.concatenate([message, rest], axis=1)
        flip, cos, sin = flags
        mirrored = message
        for node, shift in ((0, LANES - 4), (1, LANES - 2), (3, 2), (4, 4)):
            mirrored = jnp.where(
                node_lane == node, pltpu.roll(message, shift, axis=1), mirrored
            )
        aligned = jnp.where(in_data & (flip > 0.5), mirrored, message)
        field = lane // field_lanes
        turned_u = cos * aligned - sin * pltpu.roll(aligned, LANES - field_lanes, axis=1)
        turned_v = cos * aligned + sin * pltpu.roll(aligned, field_lanes, axis=1)
        aligned = jnp.where(field == 1, turned_u, jnp.where(field == 2, turned_v, aligned))
        sent[turn_index] = aligned
        if turn_index == 0:
            pl.semaphore_wait(barrier, link_count)
        for index in range(link_count):
            copy_of(turn_index, index).start()
        return flags

    def gather_local(block):
        rows = block.shape[0]
        high, low = halves(block)
        both = dot(jnp.concatenate([high, low], axis=0), local_table())
        return both[:rows] + both[rows:]

    def await_all(turn_index):
        for index in range(link_count):
            copy_of(turn_index, index).wait_recv()

    def spread_table():
        message = arrived[0]
        spot = jnp.broadcast_to(
            message[:, data_lanes + 3 : data_lanes + 4], (total_rows, span)
        )
        return onehot((iota((total_rows, span), 1) + 1).astype(f32) == spot)

    def collect(turn_index, spread):
        message = arrived[turn_index]
        high, low = halves(jnp.transpose(message)[:data_lanes])
        both = dot(jnp.concatenate([high, low], axis=0), spread)
        return both[:data_lanes] + both[data_lanes:]

    row = iota((columns, columns), 0)
    col = iota((columns, columns), 1)
    to_level = onehot(row == (col % elems) * levels + col // elems)
    to_elem = onehot(row == (col % levels) * elems + col // levels)

    padded[...] = jnp.zeros_like(padded)
    for load in loads[3:]:
        load.wait()
    for field in range(4):
        padded[field, :25] = state[:, field, :]
    nodal = permute(padded[...].reshape(128, columns), to_level)
    values = jnp.concatenate(
        [nodal[field * 32 : field * 32 + 32] for field in range(4)], axis=1
    )
    high, low = halves(values)
    faces_in = dot(tables[192:224, :64], jnp.concatenate([high, low], axis=0))

    def fields_of(wide):
        return [wide[:, field * columns : (field + 1) * columns] for field in range(4)]

    def elementwise_lanes(wide):
        return permute(jnp.concatenate(fields_of(wide), axis=0), to_elem)

    def early_part(values, faces_in, faces_out, grad_x, grad_y, face_gx, face_gy, own_slope):
        face_of_row = iota((32, columns), 0) // 8
        normal_x = jnp.where(face_of_row == 0, 1.0, 0.0) - jnp.where(face_of_row == 2, 1.0, 0.0)
        normal_y = jnp.where(face_of_row == 1, 1.0, 0.0) - jnp.where(face_of_row == 3, 1.0, 0.0)

        def flux_of(faces):
            speed = faces[1] * normal_x + faces[2] * normal_y
            return [speed, faces[0] * normal_x, faces[0] * normal_y, faces[3] * speed], speed

        inside, outside = fields_of(faces_in), fields_of(faces_out)
        gx_in, gy_in = fields_of(face_gx), fields_of(face_gy)
        slope_own = fields_of(own_slope)
        flux_in, speed_in = flux_of(inside)
        flux_out, speed_out = flux_of(outside)
        wave = 1.0 + jnp.maximum(jnp.abs(speed_in), jnp.abs(speed_out))
        terms = []
        for field in range(4):
            slope_in = gx_in[field] * normal_x + gy_in[field] * normal_y
            jump = outside[field] - inside[field]
            terms.append(
                0.5 * (flux_in[field] - flux_out[field])
                - 0.5 * viscosity * (slope_in - slope_own[field])
                + (0.5 * wave + viscosity * penalty) * jump
            )
        face_term = jnp.concatenate(terms, axis=1)
        pressure, vel_u, vel_v, theta = fields_of(values)
        nothing = jnp.zeros_like(pressure)
        flux_x = jnp.concatenate([vel_u, pressure, nothing, theta * vel_u], axis=1)
        flux_y = jnp.concatenate([vel_v, nothing, pressure, theta * vel_v], axis=1)
        tendency = dot3(
            tables[128:160, :288],
            jnp.concatenate(
                [flux_x - viscosity * grad_x, flux_y - viscosity * grad_y, face_term], axis=0
            ),
        )

        return elementwise_lanes(tendency)

    block_in = to_exchange(faces_in)
    flags = post(0, block_in, None)
    always = device_pos >= 0

    @pl.when(always)
    def _():
        own = from_exchange(gather_local(block_in))
        own_faces[...] = own
        early_grads[...] = dot3(
            tables[:128, :192], jnp.concatenate([values, own - faces_in], axis=0)
        )

    await_all(0)
    spread = spread_table()
    far_faces = from_exchange(collect(0, spread))
    face_grads = early_grads[64:128] + dot3(tables[64:128, 192:288], far_faces)
    face_gx, face_gy = face_grads[:32], face_grads[32:]
    wide_x = jnp.concatenate([heads_x] * groups, axis=1)
    wide_y = jnp.concatenate([heads_y] * groups, axis=1)
    block_grad = to_exchange(face_gx * wide_x + face_gy * wide_y)
    post(1, block_grad, flags)

    @pl.when(always)
    def _():
        own_slope = from_exchange(gather_local(block_grad))
        grads = early_grads[:64] + dot3(tables[:64, 192:288], far_faces)
        faces_out = own_faces[...] + far_faces
        grad_x, grad_y = grads[:32], grads[32:]
        early_change[...] = early_part(
            values, faces_in, faces_out, grad_x, grad_y, face_gx, face_gy, own_slope
        )

    await_all(1)
    far_slope = from_exchange(collect(1, spread))
    late = elementwise_lanes(dot3(tables[160:192, :96], far_slope))
    total = early_change[...] + late
    for field in range(4):
        change[:, field, :] = total[field * 32 : field * 32 + 25]

    for turn_index in range(2):
        for index in range(link_count):
            copy_of(turn_index, index).wait_send()


def direct_kernel(
    plan,
    state_hbm,
    neighbor_hbm,
    neighbor_face_hbm,
    seam_hbm,
    face_tables_hbm,
    tables_hbm,
    register_hbm,
    own_part,
    late_part,
    sideways,
    state,
    indices,
    face_tables,
    tables,
    padded,
    sent,
    arrived,
    notice,
    notices,
    verdict,
    spread,
    known,
    register,
    ready,
    index_sem,
    load_sem,
    send_sem,
    recv_sem,
    notice_send_sem,
    notice_recv_sem,
    verdict_send_sem,
    verdict_recv_sem,
):
    elems, levels, curve_count, strip_count, links, rows_of, offsets = plan
    columns = elems * levels
    span = 4 * columns
    inner = LANES // elems
    outer_levels = levels // inner
    total_rows = offsets[-1] + rows_of[-1]
    link_count = len(links)
    link_rows = -(-link_count // 8) * 8
    half = LANES // outer_levels

    curve_pos = lax.axis_index("curve")
    strip_pos = lax.axis_index("sub")
    device_pos = curve_pos * strip_count + strip_pos

    def place_at(curve_step, strip_step):
        return (
            lax.rem(curve_pos + curve_step + curve_count, curve_count),
            lax.rem(strip_pos + strip_step + strip_count, strip_count),
        )

    places = [place_at(step, 0) if axis == "curve" else place_at(0, step) for axis, step in links]
    device_count = curve_count * strip_count
    herald = device_count // 2 - 1
    collectors = (0, 1, herald)
    collects = (device_pos < 2) | (device_pos == herald)

    def place_of(position):
        return (position // strip_count, position % strip_count)

    def beyond(index):
        axis, step = links[index]
        if axis == "curve" and step > 0:
            return curve_pos + step >= curve_count
        return None

    def before_start(index):
        axis, step = links[index]
        if axis == "curve" and step < 0:
            return curve_pos + step < 0
        return None

    def tell(place):
        pl.semaphore_signal(
            barrier, inc=1, device_id=place, device_id_type=pl.DeviceIdType.MESH
        )

    def notice_to(position):
        return pltpu.make_async_remote_copy(
            src_ref=notice.at[pl.ds(0, 1)],
            dst_ref=notices.at[pl.ds(device_pos, 1)],
            send_sem=notice_send_sem,
            recv_sem=notice_recv_sem,
            device_id=place_of(position),
            device_id_type=pl.DeviceIdType.MESH,
        )

    def verdict_to(position):
        return pltpu.make_async_remote_copy(
            src_ref=notice.at[pl.ds(8, 1)],
            dst_ref=verdict.at[pl.ds(0, 1)],
            send_sem=verdict_send_sem,
            recv_sem=verdict_recv_sem,
            device_id=place_of(position),
            device_id_type=pl.DeviceIdType.MESH,
        )

    def rows_done(ref, count, semaphore):
        rows = ref.at[pl.ds(0, count)]
        return pltpu.make_async_copy(rows, rows, semaphore)

    def copy_of(index):
        rows = pl.ds(offsets[index], rows_of[index])
        return pltpu.make_async_remote_copy(
            src_ref=sent.at[rows],
            dst_ref=arrived.at[rows],
            send_sem=send_sem,
            recv_sem=recv_sem,
            device_id=places[index],
            device_id_type=pl.DeviceIdType.MESH,
        )

    index_loads = [
        pltpu.make_async_copy(source_ref, indices.at[index], index_sem)
        for index, source_ref in enumerate((neighbor_face_hbm, seam_hbm, neighbor_hbm))
    ]
    loads = [
        pltpu.make_async_copy(source_ref, target_ref, load_sem.at[index])
        for index, (source_ref, target_ref) in enumerate(
            [
                (face_tables_hbm, face_tables),
                (tables_hbm, tables),
                (register_hbm, register),
            ]
        )
    ]
    nodes = state.shape[0]
    piece = -(-nodes // 5)
    state_loads = [
        pltpu.make_async_copy(
            state_hbm.at[pl.ds(start, min(piece, nodes - start))],
            state.at[pl.ds(start, min(piece, nodes - start))],
            load_sem.at[3],
        )
        for start in range(0, nodes, piece)
    ]
    for load in index_loads + state_loads + loads:
        load.start()
    notices[...] = jnp.zeros_like(notices)
    barrier = pltpu.get_barrier_semaphore()
    for index, place in enumerate(places):
        if beyond(index) is None:
            tell(place)
        else:
            pl.when(jnp.logical_not(beyond(index)))(functools.partial(tell, place))
    for collector in collectors:

        @pl.when(device_pos == collector)
        def _():
            for position in range(device_count - 1, -1, -1):
                if position != collector:
                    tell(place_of(position))

    padded[...] = jnp.zeros_like(padded)
    level = iota((8, columns), 1) % levels
    link_iota = iota((link_rows, LANES), 0)
    wide_iota = iota((link_rows, columns), 0)
    target = jnp.full((link_rows, LANES), -1, jnp.int32)
    base_wide = jnp.zeros((link_rows, columns), f32)
    base_back = jnp.zeros((link_rows, LANES), f32)
    for index, place in enumerate(places):
        target = jnp.where(link_iota == index, place[0] * strip_count + place[1], target)
        base_wide = jnp.where(wide_iota == index, float(offsets[index] + 1), base_wide)
        base_back = jnp.where(link_iota == index, float(offsets[index ^ 1] + 1), base_back)
    from_elem = iota((LANES, columns), 0)
    to_elem = iota((LANES, columns), 1) // levels
    reach = jnp.concatenate(
        [
            onehot((from_elem < elems) & (from_elem < to_elem)),
            onehot(from_elem < elems),
            onehot(from_elem == to_elem),
        ],
        axis=1,
    )
    pltpu.make_async_copy(indices, indices, index_sem).wait()

    face_back, codes, across = [
        jnp.concatenate([indices[index]] * inner, axis=1) for index in range(3)
    ]
    owner = across // elems
    place_in = across % elems
    turn = codes % 4
    flipped = codes // 4
    own_face = iota((4, LANES), 0)
    quarter = (face_back + turn - own_face + 4) % 4
    odd = jnp.where(quarter % 2 == 1, 1.0, 0.0)
    notice[:8] = jnp.broadcast_to(jnp.sum(odd, axis=0, keepdims=True), (8, LANES))
    early = device_pos >= device_count - strip_count // 2

    def meet():
        count = link_count + len(collectors) - jnp.where(collects, 1, 0)
        for index in range(link_count):
            if before_start(index) is not None:
                count = count - jnp.where(before_start(index), 1, 0)
        pl.semaphore_wait(barrier, count)
        for index in range(link_count):
            if beyond(index) is not None:

                @pl.when(beyond(index))
                def _():
                    pl.semaphore_signal(
                        ready.at[links[index][1] - 1],
                        inc=1,
                        device_id=places[index],
                        device_id_type=pl.DeviceIdType.MESH,
                    )

    def notify():
        for collector in collectors:

            @pl.when(device_pos != collector)
            def _():
                notice_to(collector).start()

    @pl.when(early)
    def _():
        meet()
        notify()

    side = jnp.where(quarter == 0, 1.0, -1.0)
    cosine = jnp.where(turn == 0, 1.0, 0.0) - jnp.where(turn == 2, 1.0, 0.0)
    sine = jnp.where(turn == 3, 1.0, 0.0) - jnp.where(turn == 1, 1.0, 0.0)

    loads[0].wait()
    pltpu.make_async_copy(state, state, load_sem.at[3]).wait()
    member = [
        jnp.where(owner[face : face + 1] == target, 1.0, 0.0) for face in range(4)
    ]
    extras = [
        jnp.concatenate([part, jnp.zeros_like(part)], axis=0)
        for part in (flipped.astype(f32), cosine, sine, side)
    ]
    wide = dot(jnp.concatenate(member + extras, axis=0).astype(bf16), reach)
    before = jnp.zeros((link_rows, columns), f32)
    spots = []
    for face in range(4):
        part = wide[face * link_rows : (face + 1) * link_rows]
        rank = part[:, :columns] + before
        before = before + part[:, columns : 2 * columns]
        chosen = part[:, 2 * columns :] * (base_wide + inner * rank)
        spots.append(jnp.sum(chosen, axis=0, keepdims=True))
    extra_row = 4 * link_rows
    flip_wide, cos_wide, sin_wide, side_wide = [
        wide[extra_row + 8 * index : extra_row + 8 * index + 8, 2 * columns :]
        for index in range(4)
    ]

    def stretched(per_face):
        rows = []
        for values in per_face:
            rows.append(values)
            rows.append(jnp.zeros_like(values))
        wide = dot(jnp.concatenate(rows, axis=0).astype(bf16), reach[:, 2 * columns :])
        return [wide[8 * index : 8 * index + 8] for index in range(len(per_face))]

    def rows_for(slot, stride):
        spot = slot + (level[:1] % inner + level[:1] // inner * stride).astype(f32)
        return jnp.where(slot > 0.5, spot, 0.0)

    def hot_rows(count, spots):
        count_iota = (iota((count, columns), 0) + 1).astype(f32)
        return jnp.concatenate(
            [
                onehot(
                    count_iota == jnp.broadcast_to(spots[face], (count, columns))
                )
                for face in range(4)
            ],
            axis=1,
        )

    pack = hot_rows(total_rows, [rows_for(spot, 0) for spot in spots])

    def over_faces(wide, rows):
        return jnp.concatenate(
            [jnp.broadcast_to(wide[face : face + 1], (rows, columns)) for face in range(4)],
            axis=1,
        )

    def to_fields(block):
        return jnp.concatenate(
            [
                jnp.concatenate(
                    [
                        block[face * 8 : face * 8 + 8, field * columns : (field + 1) * columns]
                        for face in range(4)
                    ],
                    axis=1,
                )
                for field in range(4)
            ],
            axis=0,
        )

    def to_faces(block):
        return jnp.concatenate(
            [
                jnp.concatenate(
                    [
                        block[field * 8 : field * 8 + 8, face * columns : (face + 1) * columns]
                        for field in range(4)
                    ],
                    axis=1,
                )
                for face in range(4)
            ],
            axis=0,
        )

    flip_all, cos_all, sin_all, side_all = [
        over_faces(wide, 8) for wide in (flip_wide, cos_wide, sin_wide, side_wide)
    ]
    level_all = iota((half, span), 1) % levels // inner

    for field in range(4):
        padded[field, :25] = state[:, field, :]
    values = jnp.concatenate([padded[field] for field in range(4)], axis=1)
    on_faces = dot3(face_tables[:, :96], values)
    traces, slopes, flipped_traces, flipped_slopes = [
        to_fields(on_faces[32 * part : 32 * part + 32]) for part in range(4)
    ]

    def aligned(plain, mirrored):
        parts = [
            jnp.where(
                flip_all > 0.5,
                mirrored[field * 8 : field * 8 + 8],
                plain[field * 8 : field * 8 + 8],
            )
            for field in range(4)
        ]
        parts[1], parts[2] = (
            cos_all * parts[1] - sin_all * parts[2],
            cos_all * parts[2] + sin_all * parts[1],
        )
        return parts

    message = aligned(traces, flipped_traces) + [
        side_all * part for part in aligned(slopes, flipped_slopes)
    ]
    high, low = halves(jnp.concatenate(message, axis=0))
    pieces = []
    for part in (high, low):
        for index in range(outer_levels):
            pieces.append(jnp.where(level_all == index, part, jnp.zeros_like(part)))
    stacked = dot_t(pack, jnp.concatenate(pieces, axis=0))
    sent[...] = stacked[:, :LANES] + stacked[:, LANES:]
    pl.when(jnp.logical_not(early))(meet)
    order = sorted(
        range(link_count), key=lambda index: (links[index][1] < 0, abs(links[index][1]))
    )
    for index in order:
        if before_start(index) is None:
            copy_of(index).start()
        else:
            pl.when(jnp.logical_not(before_start(index)))(copy_of(index).start)
    pl.when(jnp.logical_not(early))(notify)
    always = device_pos >= 0

    @pl.when(always)
    def _():
        first_of = owner * (4 * elems)
        key = (first_of + face_back * elems + place_in).astype(f32)
        first_of = first_of.astype(f32)
        key_down = jnp.transpose(jnp.concatenate([key, key], axis=0))
        back_rows = []
        for face in range(4):
            smaller = jnp.zeros((elems, LANES), f32)
            for other in range(4):
                rival = jnp.broadcast_to(key_down[:elems, other : other + 1], (elems, LANES))
                mine = (rival < key[face : face + 1]) & (rival >= first_of[face : face + 1])
                smaller = smaller + jnp.where(mine, 1.0, 0.0)
            rank = jnp.sum(smaller, axis=0, keepdims=True)
            back_rows.append(
                jnp.sum(member[face] * (base_back + inner * rank), axis=0, keepdims=True)
            )
        at_home = owner == device_pos
        homes = [
            jnp.where(at_home & (face_back == face), place_in + 1, 0).astype(f32)
            for face in range(4)
        ]
        back, *homes = stretched([jnp.concatenate(back_rows, axis=0)] + homes)
        spread[...] = hot_rows(
            outer_levels * LANES,
            [rows_for(back[face : face + 1], LANES) for face in range(4)],
        )

        slopes_out = slopes * over_faces(side_wide, 32)
        both_high, both_low = halves(jnp.concatenate([traces, slopes_out], axis=0))
        both = jnp.concatenate([both_high, both_low], axis=0)
        found = jnp.zeros((128, span), f32)
        for face in range(4):
            home_spot = jnp.where(
                homes[face] > 0.5, homes[face] * levels + (level - levels + 1).astype(f32), 0.0
            )
            found = found + dot(
                both[:, face * columns : (face + 1) * columns],
                hot_rows(columns, [home_spot[into : into + 1] for into in range(4)]),
            )
        found = found[:64] + found[64:]
        known[:32] = traces
        known[32:64] = found[:32]
        known[64:96] = found[32:] - slopes
        known[96:128] = over_faces(
            0.5 + viscosity * penalty - 0.25 * lift_gain * viscosity * (1.0 + side_wide), 32
        )
        pressure, vel_u, vel_v, theta = [
            values[:, field * columns : (field + 1) * columns] for field in range(4)
        ]
        nothing = jnp.zeros_like(pressure)
        flux_x = jnp.concatenate([vel_u, pressure, nothing, theta * vel_u], axis=1)
        flux_y = jnp.concatenate([vel_v, nothing, pressure, theta * vel_v], axis=1)
        loads[1].wait()
        loads[2].wait()
        for field in range(4):
            padded[field, :25] = register[:, field, :]
        held = jnp.concatenate([padded[field] for field in range(4)], axis=1)
        own = dot3(tables[:32, :288], jnp.concatenate([flux_x, flux_y, values], axis=0))
        own = section_a * held + step_size * own
        for field in range(4):
            own_part[:, field, :] = own[:25, field * columns : (field + 1) * columns]

    for index in order:
        if before_start(index) is not None:

            @pl.when(before_start(index))
            def _():
                pl.semaphore_wait(ready.at[-links[index][1] - 1], 1)
                copy_of(index).start()

    rows_done(arrived, total_rows, recv_sem).wait()
    filler = jnp.zeros((LANES - total_rows, LANES), f32)
    turned = jnp.transpose(jnp.concatenate([arrived[...], filler], axis=0))
    turned = jnp.concatenate(
        [turned[half * index : half * (index + 1)] for index in range(outer_levels)], axis=1
    )
    high, low = halves(turned)
    far = dot(jnp.concatenate([high, low], axis=0), spread[...])
    far = far[:half] + far[half:]
    inside = known[:32]
    outside = known[32:64] + far[:32]
    jump = outside - inside
    slope_term = (0.5 * viscosity) * (known[64:96] + far[32:])
    weight = known[96:128]
    terms = []
    for face in range(4):
        sides = slice(face * columns, (face + 1) * columns)
        ins = [inside[field * 8 : field * 8 + 8, sides] for field in range(4)]
        outs = [outside[field * 8 : field * 8 + 8, sides] for field in range(4)]
        step = [jump[field * 8 : field * 8 + 8, sides] for field in range(4)]
        normal = 1 + face % 2
        sign = 1.0 if face < 2 else -1.0
        raw_in, raw_out = ins[normal], outs[normal]
        wave = weight[:8, sides] + 0.5 * jnp.maximum(jnp.abs(raw_in), jnp.abs(raw_out))
        drops = [
            (-0.5 * sign) * step[normal],
            None,
            None,
            (0.5 * sign) * (ins[3] * raw_in - outs[3] * raw_out),
        ]
        drops[normal] = (-0.5 * sign) * step[0]
        rows = []
        for field in range(4):
            term = wave * step[field] + slope_term[field * 8 : field * 8 + 8, sides]
            rows.append(term if drops[field] is None else term + drops[field])
        terms.append(jnp.concatenate(rows, axis=0))
    face_term = jnp.concatenate(terms, axis=1)
    late = dot3(
        tables[32:, :192], jnp.concatenate([to_faces(face_term), to_faces(jump)], axis=0)
    )
    for field in range(4):
        late_part[:, field, :] = late[:25, field * columns : (field + 1) * columns]

    @pl.when(collects)
    def _():
        rows_done(notices, device_count - 1, notice_recv_sem).wait()
        heard = jnp.max(notices[...], axis=0, keepdims=True) + notice[:1]
        notice[8:] = jnp.broadcast_to(heard, (8, LANES))

        @pl.when(device_pos == herald)
        def _():
            for position in range(device_count):
                if position not in collectors:
                    verdict_to(position).start()

        sideways[0] = jnp.where(jnp.max(heard) > 0.5, 1, 0)

        @pl.when(device_pos == herald)
        def _():
            rows_done(notices, device_count - len(collectors), verdict_send_sem).wait()

        rows_done(notice, len(collectors) - 1, notice_send_sem).wait()

    @pl.when(jnp.logical_not(collects))
    def _():
        rows_done(notice, len(collectors), notice_send_sem).wait()
        rows_done(verdict, 1, verdict_recv_sem).wait()
        sideways[0] = jnp.where(jnp.max(verdict[:1]) > 0.5, 1, 0)

    rows_done(sent, total_rows, send_sem).wait()


def closing_kernel(own, late, state, next_state, next_register, new_state, new_register, sems):
    nodes = own.shape[0]
    piece = -(-nodes // 3)
    for start in range(0, nodes, piece):
        rows = pl.ds(start, min(piece, nodes - start))
        fresh = own[rows] + step_size * late[rows]
        new_register[rows] = fresh
        pltpu.make_async_copy(new_register.at[rows], next_register.at[rows], sems.at[0]).start()
        new_state[rows] = state[rows] + section_b * fresh
        pltpu.make_async_copy(new_state.at[rows], next_state.at[rows], sems.at[1]).start()
    pltpu.make_async_copy(new_register, next_register, sems.at[0]).wait()
    pltpu.make_async_copy(new_state, next_state, sems.at[1]).wait()


def body(curve_count, strip_count, state, register, neighbor, neighbor_face, seam):
    elems = neighbor.shape[1]
    columns = state.shape[2]
    levels = columns // elems
    inner = LANES // elems
    outer_levels = levels // inner
    reach = min(7, (curve_count - 1) // 2)
    slots = (TW + reach - 1) // reach
    links, rows_of = [], []
    for distance in range(reach, 0, -1):
        for direction in (1, -1):
            links.append(("curve", direction * distance))
            rows_of.append(-(-slots * inner // 8) * 8)
    for direction in (1, -1):
        links.append(("sub", direction))
        rows_of.append(-(-TW * inner // 8) * 8)
    offsets = [sum(rows_of[:index]) for index in range(len(links))]
    total_rows = sum(rows_of)
    plan = (elems, levels, curve_count, strip_count, links, rows_of, offsets)
    vmem = pl.BlockSpec(memory_space=pltpu.VMEM)
    nodes_first = jnp.transpose(state, (1, 0, 2))
    register_first = jnp.transpose(register, (1, 0, 2))
    shape = nodes_first.shape

    def call(kernel, tables, more, outputs, out_specs, scratch, collective_id):
        tables = [jnp.asarray(table) for table in tables]
        operands = (nodes_first, neighbor, neighbor_face, seam, *tables, *more)
        return pl.pallas_call(
            functools.partial(kernel, plan),
            out_shape=outputs,
            in_specs=[pl.BlockSpec(memory_space=pl.ANY)] * len(operands),
            out_specs=out_specs,
            scratch_shapes=scratch,
            compiler_params=pltpu.CompilerParams(
                collective_id=collective_id, has_side_effects=True
            ),
        )(*[pltpu.with_memory_space_constraint(operand, pltpu.HBM) for operand in operands])

    def two_rounds():
        change = call(
            two_round_kernel,
            (build_tables(),),
            (),
            pltpu.VMEM(nodes_first.shape, f32),
            vmem,
            [
                pltpu.VMEM(shape, f32),
                pltpu.VMEM(neighbor.shape, jnp.int32),
                pltpu.VMEM(neighbor.shape, jnp.int32),
                pltpu.VMEM(neighbor.shape, jnp.int32),
                pltpu.VMEM((224, 384), bf16),
                pltpu.VMEM((4, 32, columns), f32),
                pltpu.VMEM((2, total_rows, LANES), f32),
                pltpu.VMEM((2, total_rows, LANES), f32),
                pltpu.VMEM((32, 4 * columns), f32),
                pltpu.VMEM((128, 4 * columns), f32),
                pltpu.VMEM((128, columns), f32),
                pltpu.SemaphoreType.DMA((5,)),
                pltpu.SemaphoreType.DMA((2, len(links))),
                pltpu.SemaphoreType.DMA((2, len(links))),
            ],
            0,
        )
        return section_a * register_first, change

    device_count = curve_count * strip_count
    if device_count <= DIRECT_LIMIT and total_rows <= LANES and outer_levels * 64 == LANES:
        *parts, sideways = call(
            direct_kernel,
            build_direct_tables(),
            (register_first,),
            (pltpu.VMEM(shape, f32), pltpu.VMEM(shape, f32), pltpu.SMEM((1,), jnp.int32)),
            (vmem, vmem, pl.BlockSpec(memory_space=pltpu.SMEM)),
            [
                pltpu.VMEM(shape, f32),
                pltpu.VMEM((3, *neighbor.shape), jnp.int32),
                pltpu.VMEM((128, LANES), bf16),
                pltpu.VMEM((64, 384), bf16),
                pltpu.VMEM((4, 32, columns), f32),
                pltpu.VMEM((total_rows, LANES), f32),
                pltpu.VMEM((total_rows, LANES), f32),
                pltpu.VMEM((16, LANES), f32),
                pltpu.VMEM((-(-device_count // 8) * 8, LANES), f32),
                pltpu.VMEM((8, LANES), f32),
                pltpu.VMEM((outer_levels * LANES, 4 * columns), bf16),
                pltpu.VMEM((128, 4 * columns), f32),
                pltpu.VMEM(shape, f32),
                pltpu.SemaphoreType.REGULAR((reach,)),
                pltpu.SemaphoreType.DMA,
                pltpu.SemaphoreType.DMA((4,)),
                pltpu.SemaphoreType.DMA,
                pltpu.SemaphoreType.DMA,
                pltpu.SemaphoreType.DMA,
                pltpu.SemaphoreType.DMA,
                pltpu.SemaphoreType.DMA,
                pltpu.SemaphoreType.DMA,
            ],
            1,
        )
        own, late = lax.cond(
            sideways[0] == 0, lambda kept: tuple(kept), lambda _: two_rounds(), parts
        )
    else:
        own, late = two_rounds()
    new = pl.pallas_call(
        closing_kernel,
        out_shape=(jax.ShapeDtypeStruct(shape, f32), jax.ShapeDtypeStruct(shape, f32)),
        in_specs=[vmem] * 3,
        out_specs=(pl.BlockSpec(memory_space=pl.ANY),) * 2,
        scratch_shapes=[
            pltpu.VMEM(shape, f32),
            pltpu.VMEM(shape, f32),
            pltpu.SemaphoreType.DMA((2,)),
        ],
    )(own, late, nodes_first)
    return tuple(jnp.transpose(part, (1, 0, 2)) for part in new)


def solution(mesh):
    wide = P(None, None, ("curve", "sub"))
    flat = P(None, ("curve", "sub"))
    return jax.shard_map(
        functools.partial(body, mesh.shape["curve"], mesh.shape["sub"]),
        mesh=mesh,
        in_specs=(wide, wide, flat, flat, flat),
        out_specs=(wide, wide),
        check_vma=False,
    )
```

```python
import functools
import math

import jax
import jax.numpy as jnp
import ml_dtypes
import numpy as np
from jax import lax
from jax.experimental import pallas as pl
from jax.experimental.pallas import tpu as pltpu
from jax.sharding import PartitionSpec as P

TW = 8
LANES = 128
DIRECT_LIMIT = 64

lift_gain = 10.0
step_size = 0.02
viscosity = 0.05
penalty = 2.0
section_a = -567301805773.0 / 1357537059087.0
section_b = 2404267990393.0 / 2016746695238.0

f32 = jnp.float32
bf16 = jnp.bfloat16


def build_derivative():
    points = np.array([-1.0, -math.sqrt(3.0 / 7.0), 0.0, math.sqrt(3.0 / 7.0), 1.0])
    weights = np.array(
        [
            1.0 / np.prod([points[row] - points[col] for col in range(5) if col != row])
            for row in range(5)
        ]
    )
    table = np.zeros((5, 5))
    for row in range(5):
        for col in range(5):
            if row != col:
                table[row, col] = weights[col] / weights[row] / (points[row] - points[col])
        table[row, row] = -np.sum(table[row])
    return table


def face_node(face, node):
    return [(4, node), (node, 4), (0, node), (node, 0)][face]


def split_const(table):
    high = table.astype(ml_dtypes.bfloat16)
    low = (table - high.astype(np.float64)).astype(ml_dtypes.bfloat16)
    return np.concatenate([high, low, high], axis=1)


def element_tables():
    d = build_derivative()
    eye = np.eye(5)
    dx = np.zeros((32, 32))
    dy = np.zeros((32, 32))
    dx[:25, :25] = np.kron(d, eye)
    dy[:25, :25] = np.kron(eye, d)
    pick = np.zeros((32, 32))
    for face in range(4):
        for node in range(5):
            a, b = face_node(face, node)
            pick[face * 8 + node, a * 5 + b] = 1.0
    normal_x = np.repeat([1.0, 0.0, -1.0, 0.0], 8)
    normal_y = np.repeat([0.0, 1.0, 0.0, -1.0], 8)
    lift_x = pick.T * normal_x[None] * (0.5 * lift_gain)
    lift_y = pick.T * normal_y[None] * (0.5 * lift_gain)
    return dx, dy, pick, normal_x, normal_y, lift_x, lift_y


def build_tables():
    dx, dy, pick, _, _, lift_x, lift_y = element_tables()
    grad_x = np.concatenate([dx, lift_x], axis=1)
    grad_y = np.concatenate([dy, lift_y], axis=1)
    grad = np.concatenate([grad_x, grad_y, pick @ grad_x, pick @ grad_y], axis=0)
    volume = np.concatenate([-dx, -dy, lift_gain * pick.T], axis=1)
    late = lift_gain * 0.5 * viscosity * pick.T
    out = np.zeros((224, 384), ml_dtypes.bfloat16)
    out[:128, :192] = split_const(grad)
    out[:128, 192:288] = split_const(grad[:, 32:])
    out[128:160, :288] = split_const(volume)
    out[160:192, :96] = split_const(late)
    out[192:224, :32] = pick.astype(ml_dtypes.bfloat16)
    out[192:224, 32:64] = pick.astype(ml_dtypes.bfloat16)
    return out


def build_direct_tables():
    dx, dy, pick, normal_x, normal_y, lift_x, lift_y = element_tables()
    slope = normal_x[:, None] * (pick @ dx) + normal_y[:, None] * (pick @ dy)
    base = np.concatenate([-dx, -dy, viscosity * (dx @ dx + dy @ dy)], axis=1)
    jump = viscosity * (dx @ lift_x + dy @ lift_y)
    late = np.concatenate([lift_gain * pick.T, jump], axis=1)
    mirror = np.arange(32).reshape(4, 8)
    mirror[:, :5] = mirror[:, 4::-1]
    mirror = mirror.reshape(-1)
    first = np.zeros((128, LANES), ml_dtypes.bfloat16)
    first[:, :96] = split_const(
        np.concatenate([pick, slope, pick[mirror], slope[mirror]], axis=0)
    )
    out = np.zeros((64, 384), ml_dtypes.bfloat16)
    out[:32, :288] = split_const(base)
    out[32:, :192] = split_const(late)
    return first, out


def halves(x):
    high = x.astype(bf16)
    low = (x - high.astype(f32)).astype(bf16)
    return high, low


def dot(a, b):
    return lax.dot_general(a, b, (((1,), (0,)), ((), ())), preferred_element_type=f32)


def dot_t(a, b):
    return lax.dot_general(a, b, (((1,), (1,)), ((), ())), preferred_element_type=f32)


def dot3(table, x):
    high, low = halves(x)
    return dot(table, jnp.concatenate([high, high, low], axis=0))


def onehot(mask):
    return jnp.where(mask, 1.0, 0.0).astype(bf16)


def permute(x, perm):
    rows = x.shape[0]
    high, low = halves(x)
    both = dot(jnp.concatenate([high, low], axis=0), perm)
    return both[:rows] + both[rows:]


def iota(shape, dim):
    return lax.broadcasted_iota(jnp.int32, shape, dim)


def two_round_kernel(
    plan,
    state_hbm,
    neighbor_hbm,
    neighbor_face_hbm,
    seam_hbm,
    tables_hbm,
    change,
    state,
    neighbor,
    neighbor_face,
    seam,
    tables,
    padded,
    sent,
    arrived,
    own_faces,
    early_grads,
    early_change,
    load_sem,
    send_sem,
    recv_sem,
):
    elems, levels, curve_count, strip_count, links, rows_of, offsets = plan
    columns = elems * levels
    inner = LANES // elems
    outer_levels = levels // inner
    groups = 4 * outer_levels
    span = 4 * LANES
    total_rows = offsets[-1] + rows_of[-1]
    link_count = len(links)
    link_rows = -(-link_count // 8) * 8

    curve_pos = lax.axis_index("curve")
    strip_pos = lax.axis_index("sub")
    device_pos = curve_pos * strip_count + strip_pos
    places = []
    for axis, step in links:
        if axis == "curve":
            places.append((lax.rem(curve_pos + step + curve_count, curve_count), strip_pos))
        else:
            places.append((curve_pos, lax.rem(strip_pos + step + strip_count, strip_count)))

    barrier = pltpu.get_barrier_semaphore()
    for place in places:
        pl.semaphore_signal(
            barrier, inc=1, device_id=place, device_id_type=pl.DeviceIdType.MESH
        )
    loads = [
        pltpu.make_async_copy(source_ref, target_ref, load_sem.at[index])
        for index, (source_ref, target_ref) in enumerate(
            [
                (neighbor_hbm, neighbor),
                (neighbor_face_hbm, neighbor_face),
                (seam_hbm, seam),
                (state_hbm, state),
                (tables_hbm, tables),
            ]
        )
    ]
    for load in loads:
        load.start()
    for load in loads[:3]:
        load.wait()

    def widen(ref):
        block = ref[...]
        return jnp.concatenate([block] * inner, axis=1)

    across = widen(neighbor)
    face_back = widen(neighbor_face)
    codes = widen(seam)
    owner = across // elems
    place_in = across % elems
    turn = codes % 4
    flipped = codes // 4
    sub_level = iota((4, LANES), 1) // elems
    position = face_back * LANES + sub_level * elems + place_in
    source = jnp.where(owner == device_pos, position, -1)
    heading = (face_back + turn) % 4
    cosine = jnp.where(turn == 0, 1.0, 0.0) - jnp.where(turn == 2, 1.0, 0.0)
    sine = jnp.where(turn == 3, 1.0, 0.0) - jnp.where(turn == 1, 1.0, 0.0)
    head_x = jnp.where(heading == 0, 1.0, 0.0) - jnp.where(heading == 2, 1.0, 0.0)
    head_y = jnp.where(heading == 1, 1.0, 0.0) - jnp.where(heading == 3, 1.0, 0.0)

    link_iota = iota((link_rows, LANES), 0)
    target = jnp.full((link_rows, LANES), -1, jnp.int32)
    base = jnp.zeros((link_rows, LANES), f32)
    for index, place in enumerate(places):
        target = jnp.where(link_iota == index, place[0] * strip_count + place[1], target)
        base = jnp.where(link_iota == index, float(offsets[index] + 1), base)
    base = base + (iota((link_rows, LANES), 1) // elems).astype(f32)
    member = [
        jnp.where(owner[face : face + 1] == target, 1.0, 0.0) for face in range(4)
    ]
    from_lane = iota((LANES, 2 * LANES), 0)
    to_lane = iota((LANES, 2 * LANES), 1)
    same = from_lane // elems == (to_lane % LANES) // elems
    earlier = same & ((from_lane < to_lane) | (to_lane >= LANES))
    counts = dot(jnp.concatenate(member, axis=0).astype(bf16), onehot(earlier))
    before = jnp.zeros((link_rows, LANES), f32)
    slot_rows = []
    for face in range(4):
        part = counts[face * link_rows : (face + 1) * link_rows]
        rank = part[:, :LANES] + before
        before = before + part[:, LANES:]
        slot_rows.append(
            jnp.sum(member[face] * (base + inner * rank), axis=0, keepdims=True)
        )
    slot_row = jnp.concatenate(slot_rows, axis=1)
    pack = onehot(
        (iota((total_rows, span), 0) + 1).astype(f32)
        == jnp.broadcast_to(slot_row, (total_rows, span))
    )
    pack2 = jnp.concatenate([pack, pack], axis=1)

    def local_table():
        span_iota = iota((span, LANES), 0)
        return jnp.concatenate(
            [onehot(span_iota == source[face : face + 1]) for face in range(4)], axis=1
        )

    meta_iota = iota((8, LANES), 0)
    meta_blocks = []
    for face in range(4):
        block = jnp.zeros((8, LANES), f32)
        for row, values in enumerate(
            [flipped.astype(f32), cosine, sine, (position + 1).astype(f32)]
        ):
            block = jnp.where(meta_iota == row, values[face : face + 1], block)
        meta_blocks.append(block)
    meta = jnp.concatenate(meta_blocks, axis=1)
    heads_x = jnp.concatenate(
        [jnp.broadcast_to(head_x[face : face + 1], (8, LANES)) for face in range(4)], axis=0
    )
    heads_y = jnp.concatenate(
        [jnp.broadcast_to(head_y[face : face + 1], (8, LANES)) for face in range(4)], axis=0
    )

    def to_exchange(faces):
        return jnp.concatenate(
            [
                jnp.concatenate(
                    [
                        faces[face * 8 : face * 8 + 8, group * LANES : (group + 1) * LANES]
                        for face in range(4)
                    ],
                    axis=1,
                )
                for group in range(groups)
            ],
            axis=0,
        )

    def from_exchange(block):
        return jnp.concatenate(
            [
                jnp.concatenate(
                    [
                        block[group * 8 : group * 8 + 8, face * LANES : (face + 1) * LANES]
                        for group in range(groups)
                    ],
                    axis=1,
                )
                for face in range(4)
            ],
            axis=0,
        )

    data_lanes = groups * 8
    field_lanes = outer_levels * 8
    lane = iota((total_rows, LANES), 1)
    node_lane = lane % 8
    in_data = lane < data_lanes

    def copy_of(turn_index, index):
        rows = pl.ds(offsets[index], rows_of[index])
        return pltpu.make_async_remote_copy(
            src_ref=sent.at[turn_index, rows],
            dst_ref=arrived.at[turn_index, rows],
            send_sem=send_sem.at[turn_index, index],
            recv_sem=recv_sem.at[turn_index, index],
            device_id=places[index],
            device_id_type=pl.DeviceIdType.MESH,
        )

    def post(turn_index, block, flags):
        if flags is None:
            pieces = [block, meta]
            if data_lanes + 8 < LANES:
                pieces.append(jnp.zeros((LANES - data_lanes - 8, span), f32))
            block = jnp.concatenate(pieces, axis=0)
        high, low = halves(block)
        message = dot_t(pack2, jnp.concatenate([high, low], axis=1))
        if flags is None:
            flags = [
                jnp.broadcast_to(
                    message[:, data_lanes + index : data_lanes + index + 1], message.shape
                )
                for index in range(3)
            ]
        else:
            rest = jnp.zeros((total_rows, LANES - data_lanes), f32)
            message = jnp.concatenate([message, rest], axis=1)
        flip, cos, sin = flags
        mirrored = message
        for node, shift in ((0, LANES - 4), (1, LANES - 2), (3, 2), (4, 4)):
            mirrored = jnp.where(
                node_lane == node, pltpu.roll(message, shift, axis=1), mirrored
            )
        aligned = jnp.where(in_data & (flip > 0.5), mirrored, message)
        field = lane // field_lanes
        turned_u = cos * aligned - sin * pltpu.roll(aligned, LANES - field_lanes, axis=1)
        turned_v = cos * aligned + sin * pltpu.roll(aligned, field_lanes, axis=1)
        aligned = jnp.where(field == 1, turned_u, jnp.where(field == 2, turned_v, aligned))
        sent[turn_index] = aligned
        if turn_index == 0:
            pl.semaphore_wait(barrier, link_count)
        for index in range(link_count):
            copy_of(turn_index, index).start()
        return flags

    def gather_local(block):
        rows = block.shape[0]
        high, low = halves(block)
        both = dot(jnp.concatenate([high, low], axis=0), local_table())
        return both[:rows] + both[rows:]

    def await_all(turn_index):
        for index in range(link_count):
            copy_of(turn_index, index).wait_recv()

    def spread_table():
        message = arrived[0]
        spot = jnp.broadcast_to(
            message[:, data_lanes + 3 : data_lanes + 4], (total_rows, span)
        )
        return onehot((iota((total_rows, span), 1) + 1).astype(f32) == spot)

    def collect(turn_index, spread):
        message = arrived[turn_index]
        high, low = halves(jnp.transpose(message)[:data_lanes])
        both = dot(jnp.concatenate([high, low], axis=0), spread)
        return both[:data_lanes] + both[data_lanes:]

    row = iota((columns, columns), 0)
    col = iota((columns, columns), 1)
    to_level = onehot(row == (col % elems) * levels + col // elems)
    to_elem = onehot(row == (col % levels) * elems + col // levels)

    padded[...] = jnp.zeros_like(padded)
    for load in loads[3:]:
        load.wait()
    for field in range(4):
        padded[field, :25] = state[:, field, :]
    nodal = permute(padded[...].reshape(128, columns), to_level)
    values = jnp.concatenate(
        [nodal[field * 32 : field * 32 + 32] for field in range(4)], axis=1
    )
    high, low = halves(values)
    faces_in = dot(tables[192:224, :64], jnp.concatenate([high, low], axis=0))

    def fields_of(wide):
        return [wide[:, field * columns : (field + 1) * columns] for field in range(4)]

    def elementwise_lanes(wide):
        return permute(jnp.concatenate(fields_of(wide), axis=0), to_elem)

    def early_part(values, faces_in, faces_out, grad_x, grad_y, face_gx, face_gy, own_slope):
        face_of_row = iota((32, columns), 0) // 8
        normal_x = jnp.where(face_of_row == 0, 1.0, 0.0) - jnp.where(face_of_row == 2, 1.0, 0.0)
        normal_y = jnp.where(face_of_row == 1, 1.0, 0.0) - jnp.where(face_of_row == 3, 1.0, 0.0)

        def flux_of(faces):
            speed = faces[1] * normal_x + faces[2] * normal_y
            return [speed, faces[0] * normal_x, faces[0] * normal_y, faces[3] * speed], speed

        inside, outside = fields_of(faces_in), fields_of(faces_out)
        gx_in, gy_in = fields_of(face_gx), fields_of(face_gy)
        slope_own = fields_of(own_slope)
        flux_in, speed_in = flux_of(inside)
        flux_out, speed_out = flux_of(outside)
        wave = 1.0 + jnp.maximum(jnp.abs(speed_in), jnp.abs(speed_out))
        terms = []
        for field in range(4):
            slope_in = gx_in[field] * normal_x + gy_in[field] * normal_y
            jump = outside[field] - inside[field]
            terms.append(
                0.5 * (flux_in[field] - flux_out[field])
                - 0.5 * viscosity * (slope_in - slope_own[field])
                + (0.5 * wave + viscosity * penalty) * jump
            )
        face_term = jnp.concatenate(terms, axis=1)
        pressure, vel_u, vel_v, theta = fields_of(values)
        nothing = jnp.zeros_like(pressure)
        flux_x = jnp.concatenate([vel_u, pressure, nothing, theta * vel_u], axis=1)
        flux_y = jnp.concatenate([vel_v, nothing, pressure, theta * vel_v], axis=1)
        tendency = dot3(
            tables[128:160, :288],
            jnp.concatenate(
                [flux_x - viscosity * grad_x, flux_y - viscosity * grad_y, face_term], axis=0
            ),
        )

        return elementwise_lanes(tendency)

    block_in = to_exchange(faces_in)
    flags = post(0, block_in, None)
    always = device_pos >= 0

    @pl.when(always)
    def _():
        own = from_exchange(gather_local(block_in))
        own_faces[...] = own
        early_grads[...] = dot3(
            tables[:128, :192], jnp.concatenate([values, own - faces_in], axis=0)
        )

    await_all(0)
    spread = spread_table()
    far_faces = from_exchange(collect(0, spread))
    face_grads = early_grads[64:128] + dot3(tables[64:128, 192:288], far_faces)
    face_gx, face_gy = face_grads[:32], face_grads[32:]
    wide_x = jnp.concatenate([heads_x] * groups, axis=1)
    wide_y = jnp.concatenate([heads_y] * groups, axis=1)
    block_grad = to_exchange(face_gx * wide_x + face_gy * wide_y)
    post(1, block_grad, flags)

    @pl.when(always)
    def _():
        own_slope = from_exchange(gather_local(block_grad))
        grads = early_grads[:64] + dot3(tables[:64, 192:288], far_faces)
        faces_out = own_faces[...] + far_faces
        grad_x, grad_y = grads[:32], grads[32:]
        early_change[...] = early_part(
            values, faces_in, faces_out, grad_x, grad_y, face_gx, face_gy, own_slope
        )

    await_all(1)
    far_slope = from_exchange(collect(1, spread))
    late = elementwise_lanes(dot3(tables[160:192, :96], far_slope))
    total = early_change[...] + late
    for field in range(4):
        change[:, field, :] = total[field * 32 : field * 32 + 25]

    for turn_index in range(2):
        for index in range(link_count):
            copy_of(turn_index, index).wait_send()


def direct_kernel(
    plan,
    state_hbm,
    neighbor_hbm,
    neighbor_face_hbm,
    seam_hbm,
    face_tables_hbm,
    tables_hbm,
    register_hbm,
    own_register,
    own_state,
    late_part,
    sideways,
    state,
    indices,
    face_tables,
    tables,
    padded,
    sent,
    arrived,
    notice,
    notices,
    verdict,
    spread,
    known,
    register,
    ready,
    index_sem,
    load_sem,
    send_sem,
    recv_sem,
    notice_send_sem,
    notice_recv_sem,
    verdict_send_sem,
    verdict_recv_sem,
):
    elems, levels, curve_count, strip_count, links, rows_of, offsets = plan
    columns = elems * levels
    span = 4 * columns
    inner = LANES // elems
    outer_levels = levels // inner
    total_rows = offsets[-1] + rows_of[-1]
    link_count = len(links)
    link_rows = -(-link_count // 8) * 8
    half = LANES // outer_levels

    curve_pos = lax.axis_index("curve")
    strip_pos = lax.axis_index("sub")
    device_pos = curve_pos * strip_count + strip_pos

    def place_at(curve_step, strip_step):
        return (
            lax.rem(curve_pos + curve_step + curve_count, curve_count),
            lax.rem(strip_pos + strip_step + strip_count, strip_count),
        )

    places = [place_at(step, 0) if axis == "curve" else place_at(0, step) for axis, step in links]
    device_count = curve_count * strip_count
    herald = device_count // 2 - 1
    collectors = (0, 1, herald)
    collects = (device_pos < 2) | (device_pos == herald)

    def place_of(position):
        return (position // strip_count, position % strip_count)

    def beyond(index):
        axis, step = links[index]
        if axis == "curve" and step > 0:
            return curve_pos + step >= curve_count
        return None

    def before_start(index):
        axis, step = links[index]
        if axis == "curve" and step < 0:
            return curve_pos + step < 0
        return None

    def tell(place):
        pl.semaphore_signal(
            barrier, inc=1, device_id=place, device_id_type=pl.DeviceIdType.MESH
        )

    def notice_to(position):
        return pltpu.make_async_remote_copy(
            src_ref=notice.at[pl.ds(0, 1)],
            dst_ref=notices.at[pl.ds(device_pos, 1)],
            send_sem=notice_send_sem,
            recv_sem=notice_recv_sem,
            device_id=place_of(position),
            device_id_type=pl.DeviceIdType.MESH,
        )

    def verdict_to(position):
        return pltpu.make_async_remote_copy(
            src_ref=notice.at[pl.ds(8, 1)],
            dst_ref=verdict.at[pl.ds(0, 1)],
            send_sem=verdict_send_sem,
            recv_sem=verdict_recv_sem,
            device_id=place_of(position),
            device_id_type=pl.DeviceIdType.MESH,
        )

    def rows_done(ref, count, semaphore):
        rows = ref.at[pl.ds(0, count)]
        return pltpu.make_async_copy(rows, rows, semaphore)

    def copy_of(index):
        rows = pl.ds(offsets[index], rows_of[index])
        return pltpu.make_async_remote_copy(
            src_ref=sent.at[rows],
            dst_ref=arrived.at[rows],
            send_sem=send_sem,
            recv_sem=recv_sem,
            device_id=places[index],
            device_id_type=pl.DeviceIdType.MESH,
        )

    index_loads = [
        pltpu.make_async_copy(source_ref, indices.at[index], index_sem)
        for index, source_ref in enumerate((neighbor_face_hbm, seam_hbm, neighbor_hbm))
    ]
    loads = [
        pltpu.make_async_copy(source_ref, target_ref, load_sem.at[index])
        for index, (source_ref, target_ref) in enumerate(
            [
                (face_tables_hbm, face_tables),
                (tables_hbm, tables),
                (register_hbm, register),
            ]
        )
    ]
    nodes = state.shape[0]
    piece = -(-nodes // 5)
    state_loads = [
        pltpu.make_async_copy(
            state_hbm.at[pl.ds(start, min(piece, nodes - start))],
            state.at[pl.ds(start, min(piece, nodes - start))],
            load_sem.at[3],
        )
        for start in range(0, nodes, piece)
    ]
    for load in index_loads + state_loads + loads:
        load.start()
    notices[...] = jnp.zeros_like(notices)
    verdict[...] = jnp.zeros_like(verdict)
    barrier = pltpu.get_barrier_semaphore()
    for index, place in enumerate(places):
        if beyond(index) is None:
            tell(place)
        else:
            pl.when(jnp.logical_not(beyond(index)))(functools.partial(tell, place))
    for collector in collectors:

        @pl.when(device_pos == collector)
        def _():
            for position in range(device_count - 1, -1, -1):
                if position != collector:
                    tell(place_of(position))

    padded[...] = jnp.zeros_like(padded)
    level = iota((8, columns), 1) % levels
    link_iota = iota((link_rows, LANES), 0)
    wide_iota = iota((link_rows, columns), 0)
    target = jnp.full((link_rows, LANES), -1, jnp.int32)
    base_wide = jnp.zeros((link_rows, columns), f32)
    base_back = jnp.zeros((link_rows, LANES), f32)
    for index, place in enumerate(places):
        target = jnp.where(link_iota == index, place[0] * strip_count + place[1], target)
        base_wide = jnp.where(wide_iota == index, float(offsets[index] + 1), base_wide)
        base_back = jnp.where(link_iota == index, float(offsets[index ^ 1] + 1), base_back)
    from_elem = iota((LANES, columns), 0)
    to_elem = iota((LANES, columns), 1) // levels
    reach = jnp.concatenate(
        [
            jnp.concatenate(
                [onehot((from_elem < elems) & (from_elem < to_elem)), onehot(from_elem < elems)],
                axis=0,
            ),
            jnp.concatenate(
                [onehot(from_elem == to_elem), onehot(from_elem < 0)], axis=0
            ),
        ],
        axis=1,
    )
    pltpu.make_async_copy(indices, indices, index_sem).wait()

    face_back, codes, across = [
        jnp.concatenate([indices[index]] * inner, axis=1) for index in range(3)
    ]
    owner = across // elems
    place_in = across % elems
    turn = codes % 4
    flipped = codes // 4
    own_face = iota((4, LANES), 0)
    quarter = (face_back + turn - own_face + 4) % 4
    odd = jnp.where(quarter % 2 == 1, 1.0, 0.0)
    notice[:8] = jnp.broadcast_to(jnp.sum(odd, axis=0, keepdims=True), (8, LANES))
    early = device_pos >= device_count - strip_count // 2

    def meet():
        count = link_count + len(collectors) - jnp.where(collects, 1, 0)
        for index in range(link_count):
            if before_start(index) is not None:
                count = count - jnp.where(before_start(index), 1, 0)
        pl.semaphore_wait(barrier, count)
        for index in range(link_count):
            if beyond(index) is not None:

                @pl.when(beyond(index))
                def _():
                    pl.semaphore_signal(
                        ready.at[links[index][1] - 1],
                        inc=1,
                        device_id=places[index],
                        device_id_type=pl.DeviceIdType.MESH,
                    )

    def notify():
        for collector in collectors:

            @pl.when(device_pos != collector)
            def _():
                notice_to(collector).start()

    @pl.when(early)
    def _():
        meet()
        notify()

    side = jnp.where(quarter == 0, 1.0, -1.0)
    cosine = jnp.where(turn == 0, 1.0, 0.0) - jnp.where(turn == 2, 1.0, 0.0)
    sine = jnp.where(turn == 3, 1.0, 0.0) - jnp.where(turn == 1, 1.0, 0.0)

    loads[0].wait()
    pltpu.make_async_copy(state, state, load_sem.at[3]).wait()
    member = [
        jnp.where(owner[face : face + 1] == target, 1.0, 0.0) for face in range(4)
    ]
    extras = [
        jnp.concatenate([part, jnp.zeros_like(part)], axis=0)
        for part in (flipped.astype(f32), cosine, sine, side)
    ]
    nothing = jnp.zeros_like(member[0])
    before = [nothing, member[0], member[0] + member[1], member[0] + member[1] + member[2]]
    left = jnp.concatenate(member + extras, axis=0).astype(bf16)
    right = jnp.concatenate(before + [jnp.zeros_like(part) for part in extras], axis=0)
    wide = dot(jnp.concatenate([left, right.astype(bf16)], axis=1), reach)
    spots = []
    for face in range(4):
        part = wide[face * link_rows : (face + 1) * link_rows]
        chosen = part[:, columns:] * (base_wide + inner * part[:, :columns])
        spots.append(jnp.sum(chosen, axis=0, keepdims=True))
    extra_row = 4 * link_rows
    flip_wide, cos_wide, sin_wide, side_wide = [
        wide[extra_row + 8 * index : extra_row + 8 * index + 8, columns:]
        for index in range(4)
    ]

    def stretched(per_face):
        rows = []
        for values in per_face:
            rows.append(values)
            rows.append(jnp.zeros_like(values))
        wide = dot(jnp.concatenate(rows, axis=0).astype(bf16), reach[:LANES, columns:])
        return [wide[8 * index : 8 * index + 8] for index in range(len(per_face))]

    def rows_for(slot, stride):
        spot = slot + (level[:1] % inner + level[:1] // inner * stride).astype(f32)
        return jnp.where(slot > 0.5, spot, 0.0)

    def hot_rows(count, spots):
        count_iota = (iota((count, columns), 0) + 1).astype(f32)
        return jnp.concatenate(
            [
                onehot(
                    count_iota == jnp.broadcast_to(spots[face], (count, columns))
                )
                for face in range(4)
            ],
            axis=1,
        )

    pack = hot_rows(total_rows, [rows_for(spot, 0) for spot in spots])

    def over_faces(wide, rows):
        return jnp.concatenate(
            [jnp.broadcast_to(wide[face : face + 1], (rows, columns)) for face in range(4)],
            axis=1,
        )

    def to_fields(block):
        return jnp.concatenate(
            [
                jnp.concatenate(
                    [
                        block[face * 8 : face * 8 + 8, field * columns : (field + 1) * columns]
                        for face in range(4)
                    ],
                    axis=1,
                )
                for field in range(4)
            ],
            axis=0,
        )

    def to_faces(block):
        return jnp.concatenate(
            [
                jnp.concatenate(
                    [
                        block[field * 8 : field * 8 + 8, face * columns : (face + 1) * columns]
                        for field in range(4)
                    ],
                    axis=1,
                )
                for face in range(4)
            ],
            axis=0,
        )

    flip_all, cos_all, sin_all, side_all = [
        over_faces(wide, 8) for wide in (flip_wide, cos_wide, sin_wide, side_wide)
    ]
    level_all = iota((half, span), 1) % levels // inner

    for field in range(4):
        padded[field, :25] = state[:, field, :]
    values = jnp.concatenate([padded[field] for field in range(4)], axis=1)
    on_faces = dot3(face_tables[:, :96], values)
    traces, slopes, flipped_traces, flipped_slopes = [
        to_fields(on_faces[32 * part : 32 * part + 32]) for part in range(4)
    ]

    def aligned(plain, mirrored):
        parts = [
            jnp.where(
                flip_all > 0.5,
                mirrored[field * 8 : field * 8 + 8],
                plain[field * 8 : field * 8 + 8],
            )
            for field in range(4)
        ]
        parts[1], parts[2] = (
            cos_all * parts[1] - sin_all * parts[2],
            cos_all * parts[2] + sin_all * parts[1],
        )
        return parts

    message = aligned(traces, flipped_traces) + [
        side_all * part for part in aligned(slopes, flipped_slopes)
    ]
    high, low = halves(jnp.concatenate(message, axis=0))
    pieces = []
    for part in (high, low):
        for index in range(outer_levels):
            pieces.append(jnp.where(level_all == index, part, jnp.zeros_like(part)))
    stacked = dot_t(pack, jnp.concatenate(pieces, axis=0))
    sent[...] = stacked[:, :LANES] + stacked[:, LANES:]
    pl.when(jnp.logical_not(early))(meet)
    order = sorted(
        range(link_count), key=lambda index: (links[index][1] < 0, abs(links[index][1]))
    )
    for index in order:
        if before_start(index) is None:
            copy_of(index).start()
        else:
            pl.when(jnp.logical_not(before_start(index)))(copy_of(index).start)
    pl.when(jnp.logical_not(early))(notify)
    always = device_pos >= 0

    @pl.when(always)
    def _():
        first_of = owner * (4 * elems)
        key = (first_of + face_back * elems + place_in).astype(f32)
        first_of = first_of.astype(f32)
        key_down = jnp.transpose(jnp.concatenate([key, key], axis=0))
        back_rows = []
        for face in range(4):
            smaller = jnp.zeros((elems, LANES), f32)
            for other in range(4):
                rival = jnp.broadcast_to(key_down[:elems, other : other + 1], (elems, LANES))
                mine = (rival < key[face : face + 1]) & (rival >= first_of[face : face + 1])
                smaller = smaller + jnp.where(mine, 1.0, 0.0)
            rank = jnp.sum(smaller, axis=0, keepdims=True)
            back_rows.append(
                jnp.sum(member[face] * (base_back + inner * rank), axis=0, keepdims=True)
            )
        at_home = owner == device_pos
        homes = [
            jnp.where(at_home & (face_back == face), place_in + 1, 0).astype(f32)
            for face in range(4)
        ]
        back, *homes = stretched([jnp.concatenate(back_rows, axis=0)] + homes)
        spread[...] = hot_rows(
            outer_levels * LANES,
            [rows_for(back[face : face + 1], LANES) for face in range(4)],
        )

        slopes_out = slopes * over_faces(side_wide, 32)
        both_high, both_low = halves(jnp.concatenate([traces, slopes_out], axis=0))
        both = jnp.concatenate([both_high, both_low], axis=0)
        found = jnp.zeros((128, span), f32)
        for face in range(4):
            home_spot = jnp.where(
                homes[face] > 0.5, homes[face] * levels + (level - levels + 1).astype(f32), 0.0
            )
            found = found + dot(
                both[:, face * columns : (face + 1) * columns],
                hot_rows(columns, [home_spot[into : into + 1] for into in range(4)]),
            )
        found = found[:64] + found[64:]
        known[:32] = traces
        known[32:64] = found[:32]
        known[64:96] = found[32:] - slopes
        known[96:128] = over_faces(
            0.5 + viscosity * penalty - 0.25 * lift_gain * viscosity * (1.0 + side_wide), 32
        )
        pressure, vel_u, vel_v, theta = [
            values[:, field * columns : (field + 1) * columns] for field in range(4)
        ]
        nothing = jnp.zeros_like(pressure)
        flux_x = jnp.concatenate([vel_u, pressure, nothing, theta * vel_u], axis=1)
        flux_y = jnp.concatenate([vel_v, nothing, pressure, theta * vel_v], axis=1)
        loads[1].wait()
        loads[2].wait()
        for field in range(4):
            padded[field, :25] = register[:, field, :]
        held = jnp.concatenate([padded[field] for field in range(4)], axis=1)
        own = dot3(tables[:32, :288], jnp.concatenate([flux_x, flux_y, values], axis=0))
        own = section_a * held + step_size * own
        moved = values + section_b * own
        for field in range(4):
            sides = slice(field * columns, (field + 1) * columns)
            own_register[:, field, :] = own[:25, sides]
            own_state[:, field, :] = moved[:25, sides]

    for index in order:
        if before_start(index) is not None:

            @pl.when(before_start(index))
            def _():
                pl.semaphore_wait(ready.at[-links[index][1] - 1], 1)
                copy_of(index).start()

    rows_done(arrived, total_rows, recv_sem).wait()
    filler = jnp.zeros((LANES - total_rows, LANES), f32)
    turned = jnp.transpose(jnp.concatenate([arrived[...], filler], axis=0))
    turned = jnp.concatenate(
        [turned[half * index : half * (index + 1)] for index in range(outer_levels)], axis=1
    )
    high, low = halves(turned)
    far = dot(jnp.concatenate([high, low], axis=0), spread[...])
    far = far[:half] + far[half:]
    inside = known[:32]
    outside = known[32:64] + far[:32]
    jump = outside - inside
    slope_term = (0.5 * viscosity) * (known[64:96] + far[32:])
    weight = known[96:128]
    terms = []
    for face in range(4):
        sides = slice(face * columns, (face + 1) * columns)
        ins = [inside[field * 8 : field * 8 + 8, sides] for field in range(4)]
        outs = [outside[field * 8 : field * 8 + 8, sides] for field in range(4)]
        step = [jump[field * 8 : field * 8 + 8, sides] for field in range(4)]
        normal = 1 + face % 2
        sign = 1.0 if face < 2 else -1.0
        raw_in, raw_out = ins[normal], outs[normal]
        wave = weight[:8, sides] + 0.5 * jnp.maximum(jnp.abs(raw_in), jnp.abs(raw_out))
        drops = [
            (-0.5 * sign) * step[normal],
            None,
            None,
            (0.5 * sign) * (ins[3] * raw_in - outs[3] * raw_out),
        ]
        drops[normal] = (-0.5 * sign) * step[0]
        rows = []
        for field in range(4):
            term = wave * step[field] + slope_term[field * 8 : field * 8 + 8, sides]
            rows.append(term if drops[field] is None else term + drops[field])
        terms.append(jnp.concatenate(rows, axis=0))
    face_term = jnp.concatenate(terms, axis=1)

    @pl.when(collects)
    def _():
        rows_done(notices, device_count - 1, notice_recv_sem).wait()

        @pl.when(device_pos == herald)
        def _():
            heard = jnp.max(notices[...], axis=0, keepdims=True) + notice[:1]
            notice[8:] = jnp.broadcast_to(heard, (8, LANES))
            for position in range(device_count):
                if position not in collectors:
                    verdict_to(position).start()

    @pl.when(jnp.logical_not(collects))
    def _():
        rows_done(verdict, 1, verdict_recv_sem).wait()

    heard = jnp.maximum(notice[:8], verdict[...])
    for start in range(0, notices.shape[0], 8):
        heard = jnp.maximum(heard, notices[start : start + 8])
    sideways[0] = jnp.where(jnp.max(heard) > 0.5, 1, 0)
    late = dot3(
        tables[32:, :192], jnp.concatenate([to_faces(face_term), to_faces(jump)], axis=0)
    )
    for field in range(4):
        late_part[:, field, :] = late[:25, field * columns : (field + 1) * columns]

    @pl.when(device_pos == herald)
    def _():
        rows_done(notices, device_count - len(collectors), verdict_send_sem).wait()

    @pl.when(collects)
    def _():
        rows_done(notice, len(collectors) - 1, notice_send_sem).wait()

    @pl.when(jnp.logical_not(collects))
    def _():
        rows_done(notice, len(collectors), notice_send_sem).wait()

    rows_done(sent, total_rows, send_sem).wait()


def closing_kernel(
    own_register, own_state, late, next_state, next_register, new_state, new_register, sems
):
    nodes = late.shape[0]
    piece = -(-nodes // 3)
    for start in range(0, nodes, piece):
        rows = pl.ds(start, min(piece, nodes - start))
        part = step_size * late[rows]
        new_register[rows] = own_register[rows] + part
        pltpu.make_async_copy(new_register.at[rows], next_register.at[rows], sems.at[0]).start()
        new_state[rows] = own_state[rows] + section_b * part
        pltpu.make_async_copy(new_state.at[rows], next_state.at[rows], sems.at[1]).start()
    pltpu.make_async_copy(new_register, next_register, sems.at[0]).wait()
    pltpu.make_async_copy(new_state, next_state, sems.at[1]).wait()


def start_kernel(state, register, own_register, own_state):
    own_register[...] = section_a * register[...]
    own_state[...] = state[...] + section_b * own_register[...]


def body(curve_count, strip_count, state, register, neighbor, neighbor_face, seam):
    elems = neighbor.shape[1]
    columns = state.shape[2]
    levels = columns // elems
    inner = LANES // elems
    outer_levels = levels // inner
    reach = min(7, (curve_count - 1) // 2)
    slots = (TW + reach - 1) // reach
    links, rows_of = [], []
    for distance in range(reach, 0, -1):
        for direction in (1, -1):
            links.append(("curve", direction * distance))
            rows_of.append(-(-slots * inner // 8) * 8)
    for direction in (1, -1):
        links.append(("sub", direction))
        rows_of.append(-(-TW * inner // 8) * 8)
    offsets = [sum(rows_of[:index]) for index in range(len(links))]
    total_rows = sum(rows_of)
    plan = (elems, levels, curve_count, strip_count, links, rows_of, offsets)
    vmem = pl.BlockSpec(memory_space=pltpu.VMEM)
    nodes_first = jnp.transpose(state, (1, 0, 2))
    register_first = jnp.transpose(register, (1, 0, 2))
    shape = nodes_first.shape

    def call(kernel, tables, more, outputs, out_specs, scratch, collective_id):
        tables = [jnp.asarray(table) for table in tables]
        operands = (nodes_first, neighbor, neighbor_face, seam, *tables, *more)
        return pl.pallas_call(
            functools.partial(kernel, plan),
            out_shape=outputs,
            in_specs=[pl.BlockSpec(memory_space=pl.ANY)] * len(operands),
            out_specs=out_specs,
            scratch_shapes=scratch,
            compiler_params=pltpu.CompilerParams(
                collective_id=collective_id, has_side_effects=True
            ),
        )(*[pltpu.with_memory_space_constraint(operand, pltpu.HBM) for operand in operands])

    def two_rounds():
        change = call(
            two_round_kernel,
            (build_tables(),),
            (),
            pltpu.VMEM(nodes_first.shape, f32),
            vmem,
            [
                pltpu.VMEM(shape, f32),
                pltpu.VMEM(neighbor.shape, jnp.int32),
                pltpu.VMEM(neighbor.shape, jnp.int32),
                pltpu.VMEM(neighbor.shape, jnp.int32),
                pltpu.VMEM((224, 384), bf16),
                pltpu.VMEM((4, 32, columns), f32),
                pltpu.VMEM((2, total_rows, LANES), f32),
                pltpu.VMEM((2, total_rows, LANES), f32),
                pltpu.VMEM((32, 4 * columns), f32),
                pltpu.VMEM((128, 4 * columns), f32),
                pltpu.VMEM((128, columns), f32),
                pltpu.SemaphoreType.DMA((5,)),
                pltpu.SemaphoreType.DMA((2, len(links))),
                pltpu.SemaphoreType.DMA((2, len(links))),
            ],
            0,
        )
        started = pl.pallas_call(
            start_kernel,
            out_shape=(pltpu.VMEM(shape, f32), pltpu.VMEM(shape, f32)),
            in_specs=[vmem, vmem],
            out_specs=(vmem, vmem),
        )(*[pltpu.with_memory_space_constraint(x, pltpu.HBM) for x in (nodes_first, register_first)])
        return *started, change

    device_count = curve_count * strip_count
    if device_count <= DIRECT_LIMIT and total_rows <= LANES and outer_levels * 64 == LANES:
        *parts, sideways = call(
            direct_kernel,
            build_direct_tables(),
            (register_first,),
            (pltpu.VMEM(shape, f32),) * 3 + (pltpu.SMEM((1,), jnp.int32),),
            (vmem,) * 3 + (pl.BlockSpec(memory_space=pltpu.SMEM),),
            [
                pltpu.VMEM(shape, f32),
                pltpu.VMEM((3, *neighbor.shape), jnp.int32),
                pltpu.VMEM((128, LANES), bf16),
                pltpu.VMEM((64, 384), bf16),
                pltpu.VMEM((4, 32, columns), f32),
                pltpu.VMEM((total_rows, LANES), f32),
                pltpu.VMEM((total_rows, LANES), f32),
                pltpu.VMEM((16, LANES), f32),
                pltpu.VMEM((-(-device_count // 8) * 8, LANES), f32),
                pltpu.VMEM((8, LANES), f32),
                pltpu.VMEM((outer_levels * LANES, 4 * columns), bf16),
                pltpu.VMEM((128, 4 * columns), f32),
                pltpu.VMEM(shape, f32),
                pltpu.SemaphoreType.REGULAR((reach,)),
                pltpu.SemaphoreType.DMA,
                pltpu.SemaphoreType.DMA((4,)),
                pltpu.SemaphoreType.DMA,
                pltpu.SemaphoreType.DMA,
                pltpu.SemaphoreType.DMA,
                pltpu.SemaphoreType.DMA,
                pltpu.SemaphoreType.DMA,
                pltpu.SemaphoreType.DMA,
            ],
            1,
        )
        parts = lax.cond(
            sideways[0] == 0, lambda kept: tuple(kept), lambda _: two_rounds(), parts
        )
    else:
        parts = two_rounds()
    new = pl.pallas_call(
        closing_kernel,
        out_shape=(jax.ShapeDtypeStruct(shape, f32), jax.ShapeDtypeStruct(shape, f32)),
        in_specs=[vmem] * 3,
        out_specs=(pl.BlockSpec(memory_space=pl.ANY),) * 2,
        scratch_shapes=[
            pltpu.VMEM(shape, f32),
            pltpu.VMEM(shape, f32),
            pltpu.SemaphoreType.DMA((2,)),
        ],
    )(*parts)
    return tuple(jnp.transpose(part, (1, 0, 2)) for part in new)


def solution(mesh):
    wide = P(None, None, ("curve", "sub"))
    flat = P(None, ("curve", "sub"))
    return jax.shard_map(
        functools.partial(body, mesh.shape["curve"], mesh.shape["sub"]),
        mesh=mesh,
        in_specs=(wide, wide, flat, flat, flat),
        out_specs=(wide, wide),
        check_vma=False,
    )
```

```python
import functools
import math

import jax
import jax.numpy as jnp
import ml_dtypes
import numpy as np
from jax import lax
from jax.experimental import pallas as pl
from jax.experimental.pallas import tpu as pltpu
from jax.sharding import PartitionSpec as P

TW = 8
LANES = 128
DIRECT_LIMIT = 64

lift_gain = 10.0
step_size = 0.02
viscosity = 0.05
penalty = 2.0
section_a = -567301805773.0 / 1357537059087.0
section_b = 2404267990393.0 / 2016746695238.0

f32 = jnp.float32
bf16 = jnp.bfloat16


def build_derivative():
    points = np.array([-1.0, -math.sqrt(3.0 / 7.0), 0.0, math.sqrt(3.0 / 7.0), 1.0])
    weights = np.array(
        [
            1.0 / np.prod([points[row] - points[col] for col in range(5) if col != row])
            for row in range(5)
        ]
    )
    table = np.zeros((5, 5))
    for row in range(5):
        for col in range(5):
            if row != col:
                table[row, col] = weights[col] / weights[row] / (points[row] - points[col])
        table[row, row] = -np.sum(table[row])
    return table


def face_node(face, node):
    return [(4, node), (node, 4), (0, node), (node, 0)][face]


def split_const(table):
    high = table.astype(ml_dtypes.bfloat16)
    low = (table - high.astype(np.float64)).astype(ml_dtypes.bfloat16)
    return np.concatenate([high, low, high], axis=1)


def element_tables():
    d = build_derivative()
    eye = np.eye(5)
    dx = np.zeros((32, 32))
    dy = np.zeros((32, 32))
    dx[:25, :25] = np.kron(d, eye)
    dy[:25, :25] = np.kron(eye, d)
    pick = np.zeros((32, 32))
    for face in range(4):
        for node in range(5):
            a, b = face_node(face, node)
            pick[face * 8 + node, a * 5 + b] = 1.0
    normal_x = np.repeat([1.0, 0.0, -1.0, 0.0], 8)
    normal_y = np.repeat([0.0, 1.0, 0.0, -1.0], 8)
    lift_x = pick.T * normal_x[None] * (0.5 * lift_gain)
    lift_y = pick.T * normal_y[None] * (0.5 * lift_gain)
    return dx, dy, pick, normal_x, normal_y, lift_x, lift_y


def build_tables():
    dx, dy, pick, _, _, lift_x, lift_y = element_tables()
    grad_x = np.concatenate([dx, lift_x], axis=1)
    grad_y = np.concatenate([dy, lift_y], axis=1)
    grad = np.concatenate([grad_x, grad_y, pick @ grad_x, pick @ grad_y], axis=0)
    volume = np.concatenate([-dx, -dy, lift_gain * pick.T], axis=1)
    late = lift_gain * 0.5 * viscosity * pick.T
    out = np.zeros((224, 384), ml_dtypes.bfloat16)
    out[:128, :192] = split_const(grad)
    out[:128, 192:288] = split_const(grad[:, 32:])
    out[128:160, :288] = split_const(volume)
    out[160:192, :96] = split_const(late)
    out[192:224, :32] = pick.astype(ml_dtypes.bfloat16)
    out[192:224, 32:64] = pick.astype(ml_dtypes.bfloat16)
    return out


def build_direct_tables():
    dx, dy, pick, normal_x, normal_y, lift_x, lift_y = element_tables()
    slope = normal_x[:, None] * (pick @ dx) + normal_y[:, None] * (pick @ dy)
    base = np.concatenate([-dx, -dy, viscosity * (dx @ dx + dy @ dy)], axis=1)
    jump = viscosity * (dx @ lift_x + dy @ lift_y)
    late = np.concatenate([lift_gain * pick.T, jump], axis=1)
    mirror = np.arange(32).reshape(4, 8)
    mirror[:, :5] = mirror[:, 4::-1]
    mirror = mirror.reshape(-1)
    first = np.zeros((128, LANES), ml_dtypes.bfloat16)
    first[:, :96] = split_const(
        np.concatenate([pick, slope, pick[mirror], slope[mirror]], axis=0)
    )
    out = np.zeros((64, 384), ml_dtypes.bfloat16)
    out[:32, :288] = split_const(base)
    out[32:, :192] = split_const(late)
    return first, out


def halves(x):
    high = x.astype(bf16)
    low = (x - high.astype(f32)).astype(bf16)
    return high, low


def dot(a, b):
    return lax.dot_general(a, b, (((1,), (0,)), ((), ())), preferred_element_type=f32)


def dot_t(a, b):
    return lax.dot_general(a, b, (((1,), (1,)), ((), ())), preferred_element_type=f32)


def dot3(table, x):
    high, low = halves(x)
    return dot(table, jnp.concatenate([high, high, low], axis=0))


def onehot(mask):
    return jnp.where(mask, 1.0, 0.0).astype(bf16)


def permute(x, perm):
    rows = x.shape[0]
    high, low = halves(x)
    both = dot(jnp.concatenate([high, low], axis=0), perm)
    return both[:rows] + both[rows:]


def iota(shape, dim):
    return lax.broadcasted_iota(jnp.int32, shape, dim)


def two_round_kernel(
    plan,
    state_hbm,
    neighbor_hbm,
    neighbor_face_hbm,
    seam_hbm,
    tables_hbm,
    change,
    state,
    neighbor,
    neighbor_face,
    seam,
    tables,
    padded,
    sent,
    arrived,
    own_faces,
    early_grads,
    early_change,
    load_sem,
    send_sem,
    recv_sem,
):
    elems, levels, curve_count, strip_count, links, rows_of, offsets = plan
    columns = elems * levels
    inner = LANES // elems
    outer_levels = levels // inner
    groups = 4 * outer_levels
    span = 4 * LANES
    total_rows = offsets[-1] + rows_of[-1]
    link_count = len(links)
    link_rows = -(-link_count // 8) * 8

    curve_pos = lax.axis_index("curve")
    strip_pos = lax.axis_index("sub")
    device_pos = curve_pos * strip_count + strip_pos
    places = []
    for axis, step in links:
        if axis == "curve":
            places.append((lax.rem(curve_pos + step + curve_count, curve_count), strip_pos))
        else:
            places.append((curve_pos, lax.rem(strip_pos + step + strip_count, strip_count)))

    barrier = pltpu.get_barrier_semaphore()
    for place in places:
        pl.semaphore_signal(
            barrier, inc=1, device_id=place, device_id_type=pl.DeviceIdType.MESH
        )
    loads = [
        pltpu.make_async_copy(source_ref, target_ref, load_sem.at[index])
        for index, (source_ref, target_ref) in enumerate(
            [
                (neighbor_hbm, neighbor),
                (neighbor_face_hbm, neighbor_face),
                (seam_hbm, seam),
                (state_hbm, state),
                (tables_hbm, tables),
            ]
        )
    ]
    for load in loads:
        load.start()
    for load in loads[:3]:
        load.wait()

    def widen(ref):
        block = ref[...]
        return jnp.concatenate([block] * inner, axis=1)

    across = widen(neighbor)
    face_back = widen(neighbor_face)
    codes = widen(seam)
    owner = across // elems
    place_in = across % elems
    turn = codes % 4
    flipped = codes // 4
    sub_level = iota((4, LANES), 1) // elems
    position = face_back * LANES + sub_level * elems + place_in
    source = jnp.where(owner == device_pos, position, -1)
    heading = (face_back + turn) % 4
    cosine = jnp.where(turn == 0, 1.0, 0.0) - jnp.where(turn == 2, 1.0, 0.0)
    sine = jnp.where(turn == 3, 1.0, 0.0) - jnp.where(turn == 1, 1.0, 0.0)
    head_x = jnp.where(heading == 0, 1.0, 0.0) - jnp.where(heading == 2, 1.0, 0.0)
    head_y = jnp.where(heading == 1, 1.0, 0.0) - jnp.where(heading == 3, 1.0, 0.0)

    link_iota = iota((link_rows, LANES), 0)
    target = jnp.full((link_rows, LANES), -1, jnp.int32)
    base = jnp.zeros((link_rows, LANES), f32)
    for index, place in enumerate(places):
        target = jnp.where(link_iota == index, place[0] * strip_count + place[1], target)
        base = jnp.where(link_iota == index, float(offsets[index] + 1), base)
    base = base + (iota((link_rows, LANES), 1) // elems).astype(f32)
    member = [
        jnp.where(owner[face : face + 1] == target, 1.0, 0.0) for face in range(4)
    ]
    from_lane = iota((LANES, 2 * LANES), 0)
    to_lane = iota((LANES, 2 * LANES), 1)
    same = from_lane // elems == (to_lane % LANES) // elems
    earlier = same & ((from_lane < to_lane) | (to_lane >= LANES))
    counts = dot(jnp.concatenate(member, axis=0).astype(bf16), onehot(earlier))
    before = jnp.zeros((link_rows, LANES), f32)
    slot_rows = []
    for face in range(4):
        part = counts[face * link_rows : (face + 1) * link_rows]
        rank = part[:, :LANES] + before
        before = before + part[:, LANES:]
        slot_rows.append(
            jnp.sum(member[face] * (base + inner * rank), axis=0, keepdims=True)
        )
    slot_row = jnp.concatenate(slot_rows, axis=1)
    pack = onehot(
        (iota((total_rows, span), 0) + 1).astype(f32)
        == jnp.broadcast_to(slot_row, (total_rows, span))
    )
    pack2 = jnp.concatenate([pack, pack], axis=1)

    def local_table():
        span_iota = iota((span, LANES), 0)
        return jnp.concatenate(
            [onehot(span_iota == source[face : face + 1]) for face in range(4)], axis=1
        )

    meta_iota = iota((8, LANES), 0)
    meta_blocks = []
    for face in range(4):
        block = jnp.zeros((8, LANES), f32)
        for row, values in enumerate(
            [flipped.astype(f32), cosine, sine, (position + 1).astype(f32)]
        ):
            block = jnp.where(meta_iota == row, values[face : face + 1], block)
        meta_blocks.append(block)
    meta = jnp.concatenate(meta_blocks, axis=1)
    heads_x = jnp.concatenate(
        [jnp.broadcast_to(head_x[face : face + 1], (8, LANES)) for face in range(4)], axis=0
    )
    heads_y = jnp.concatenate(
        [jnp.broadcast_to(head_y[face : face + 1], (8, LANES)) for face in range(4)], axis=0
    )

    def to_exchange(faces):
        return jnp.concatenate(
            [
                jnp.concatenate(
                    [
                        faces[face * 8 : face * 8 + 8, group * LANES : (group + 1) * LANES]
                        for face in range(4)
                    ],
                    axis=1,
                )
                for group in range(groups)
            ],
            axis=0,
        )

    def from_exchange(block):
        return jnp.concatenate(
            [
                jnp.concatenate(
                    [
                        block[group * 8 : group * 8 + 8, face * LANES : (face + 1) * LANES]
                        for group in range(groups)
                    ],
                    axis=1,
                )
                for face in range(4)
            ],
            axis=0,
        )

    data_lanes = groups * 8
    field_lanes = outer_levels * 8
    lane = iota((total_rows, LANES), 1)
    node_lane = lane % 8
    in_data = lane < data_lanes

    def copy_of(turn_index, index):
        rows = pl.ds(offsets[index], rows_of[index])
        return pltpu.make_async_remote_copy(
            src_ref=sent.at[turn_index, rows],
            dst_ref=arrived.at[turn_index, rows],
            send_sem=send_sem.at[turn_index, index],
            recv_sem=recv_sem.at[turn_index, index],
            device_id=places[index],
            device_id_type=pl.DeviceIdType.MESH,
        )

    def post(turn_index, block, flags):
        if flags is None:
            pieces = [block, meta]
            if data_lanes + 8 < LANES:
                pieces.append(jnp.zeros((LANES - data_lanes - 8, span), f32))
            block = jnp.concatenate(pieces, axis=0)
        high, low = halves(block)
        message = dot_t(pack2, jnp.concatenate([high, low], axis=1))
        if flags is None:
            flags = [
                jnp.broadcast_to(
                    message[:, data_lanes + index : data_lanes + index + 1], message.shape
                )
                for index in range(3)
            ]
        else:
            rest = jnp.zeros((total_rows, LANES - data_lanes), f32)
            message = jnp.concatenate([message, rest], axis=1)
        flip, cos, sin = flags
        mirrored = message
        for node, shift in ((0, LANES - 4), (1, LANES - 2), (3, 2), (4, 4)):
            mirrored = jnp.where(
                node_lane == node, pltpu.roll(message, shift, axis=1), mirrored
            )
        aligned = jnp.where(in_data & (flip > 0.5), mirrored, message)
        field = lane // field_lanes
        turned_u = cos * aligned - sin * pltpu.roll(aligned, LANES - field_lanes, axis=1)
        turned_v = cos * aligned + sin * pltpu.roll(aligned, field_lanes, axis=1)
        aligned = jnp.where(field == 1, turned_u, jnp.where(field == 2, turned_v, aligned))
        sent[turn_index] = aligned
        if turn_index == 0:
            pl.semaphore_wait(barrier, link_count)
        for index in range(link_count):
            copy_of(turn_index, index).start()
        return flags

    def gather_local(block):
        rows = block.shape[0]
        high, low = halves(block)
        both = dot(jnp.concatenate([high, low], axis=0), local_table())
        return both[:rows] + both[rows:]

    def await_all(turn_index):
        for index in range(link_count):
            copy_of(turn_index, index).wait_recv()

    def spread_table():
        message = arrived[0]
        spot = jnp.broadcast_to(
            message[:, data_lanes + 3 : data_lanes + 4], (total_rows, span)
        )
        return onehot((iota((total_rows, span), 1) + 1).astype(f32) == spot)

    def collect(turn_index, spread):
        message = arrived[turn_index]
        high, low = halves(jnp.transpose(message)[:data_lanes])
        both = dot(jnp.concatenate([high, low], axis=0), spread)
        return both[:data_lanes] + both[data_lanes:]

    row = iota((columns, columns), 0)
    col = iota((columns, columns), 1)
    to_level = onehot(row == (col % elems) * levels + col // elems)
    to_elem = onehot(row == (col % levels) * elems + col // levels)

    padded[...] = jnp.zeros_like(padded)
    for load in loads[3:]:
        load.wait()
    for field in range(4):
        padded[field, :25] = state[:, field, :]
    nodal = permute(padded[...].reshape(128, columns), to_level)
    values = jnp.concatenate(
        [nodal[field * 32 : field * 32 + 32] for field in range(4)], axis=1
    )
    high, low = halves(values)
    faces_in = dot(tables[192:224, :64], jnp.concatenate([high, low], axis=0))

    def fields_of(wide):
        return [wide[:, field * columns : (field + 1) * columns] for field in range(4)]

    def elementwise_lanes(wide):
        return permute(jnp.concatenate(fields_of(wide), axis=0), to_elem)

    def early_part(values, faces_in, faces_out, grad_x, grad_y, face_gx, face_gy, own_slope):
        face_of_row = iota((32, columns), 0) // 8
        normal_x = jnp.where(face_of_row == 0, 1.0, 0.0) - jnp.where(face_of_row == 2, 1.0, 0.0)
        normal_y = jnp.where(face_of_row == 1, 1.0, 0.0) - jnp.where(face_of_row == 3, 1.0, 0.0)

        def flux_of(faces):
            speed = faces[1] * normal_x + faces[2] * normal_y
            return [speed, faces[0] * normal_x, faces[0] * normal_y, faces[3] * speed], speed

        inside, outside = fields_of(faces_in), fields_of(faces_out)
        gx_in, gy_in = fields_of(face_gx), fields_of(face_gy)
        slope_own = fields_of(own_slope)
        flux_in, speed_in = flux_of(inside)
        flux_out, speed_out = flux_of(outside)
        wave = 1.0 + jnp.maximum(jnp.abs(speed_in), jnp.abs(speed_out))
        terms = []
        for field in range(4):
            slope_in = gx_in[field] * normal_x + gy_in[field] * normal_y
            jump = outside[field] - inside[field]
            terms.append(
                0.5 * (flux_in[field] - flux_out[field])
                - 0.5 * viscosity * (slope_in - slope_own[field])
                + (0.5 * wave + viscosity * penalty) * jump
            )
        face_term = jnp.concatenate(terms, axis=1)
        pressure, vel_u, vel_v, theta = fields_of(values)
        nothing = jnp.zeros_like(pressure)
        flux_x = jnp.concatenate([vel_u, pressure, nothing, theta * vel_u], axis=1)
        flux_y = jnp.concatenate([vel_v, nothing, pressure, theta * vel_v], axis=1)
        tendency = dot3(
            tables[128:160, :288],
            jnp.concatenate(
                [flux_x - viscosity * grad_x, flux_y - viscosity * grad_y, face_term], axis=0
            ),
        )

        return elementwise_lanes(tendency)

    block_in = to_exchange(faces_in)
    flags = post(0, block_in, None)
    always = device_pos >= 0

    @pl.when(always)
    def _():
        own = from_exchange(gather_local(block_in))
        own_faces[...] = own
        early_grads[...] = dot3(
            tables[:128, :192], jnp.concatenate([values, own - faces_in], axis=0)
        )

    await_all(0)
    spread = spread_table()
    far_faces = from_exchange(collect(0, spread))
    face_grads = early_grads[64:128] + dot3(tables[64:128, 192:288], far_faces)
    face_gx, face_gy = face_grads[:32], face_grads[32:]
    wide_x = jnp.concatenate([heads_x] * groups, axis=1)
    wide_y = jnp.concatenate([heads_y] * groups, axis=1)
    block_grad = to_exchange(face_gx * wide_x + face_gy * wide_y)
    post(1, block_grad, flags)

    @pl.when(always)
    def _():
        own_slope = from_exchange(gather_local(block_grad))
        grads = early_grads[:64] + dot3(tables[:64, 192:288], far_faces)
        faces_out = own_faces[...] + far_faces
        grad_x, grad_y = grads[:32], grads[32:]
        early_change[...] = early_part(
            values, faces_in, faces_out, grad_x, grad_y, face_gx, face_gy, own_slope
        )

    await_all(1)
    far_slope = from_exchange(collect(1, spread))
    late = elementwise_lanes(dot3(tables[160:192, :96], far_slope))
    total = early_change[...] + late
    for field in range(4):
        change[:, field, :] = total[field * 32 : field * 32 + 25]

    for turn_index in range(2):
        for index in range(link_count):
            copy_of(turn_index, index).wait_send()


def direct_kernel(
    plan,
    state_hbm,
    neighbor_hbm,
    neighbor_face_hbm,
    seam_hbm,
    face_tables_hbm,
    tables_hbm,
    register_hbm,
    own_register,
    own_state,
    late_part,
    sideways,
    state,
    indices,
    face_tables,
    tables,
    padded,
    sent,
    arrived,
    notice,
    notices,
    verdict,
    spread,
    known,
    register,
    ready,
    index_sem,
    load_sem,
    send_sem,
    recv_sem,
    notice_send_sem,
    notice_recv_sem,
    verdict_send_sem,
    verdict_recv_sem,
):
    elems, levels, curve_count, strip_count, links, rows_of, offsets = plan
    columns = elems * levels
    span = 4 * columns
    inner = LANES // elems
    outer_levels = levels // inner
    total_rows = offsets[-1] + rows_of[-1]
    link_count = len(links)
    link_rows = -(-link_count // 8) * 8
    half = LANES // outer_levels

    curve_pos = lax.axis_index("curve")
    strip_pos = lax.axis_index("sub")
    device_pos = curve_pos * strip_count + strip_pos

    def place_at(curve_step, strip_step):
        return (
            lax.rem(curve_pos + curve_step + curve_count, curve_count),
            lax.rem(strip_pos + strip_step + strip_count, strip_count),
        )

    places = [place_at(step, 0) if axis == "curve" else place_at(0, step) for axis, step in links]
    device_count = curve_count * strip_count
    herald = device_count // 2 - 1
    collectors = (0, 1, herald)
    collects = (device_pos < 2) | (device_pos == herald)

    def place_of(position):
        return (position // strip_count, position % strip_count)

    def beyond(index):
        axis, step = links[index]
        if axis == "curve" and step > 0:
            return curve_pos + step >= curve_count
        return None

    def before_start(index):
        axis, step = links[index]
        if axis == "curve" and step < 0:
            return curve_pos + step < 0
        return None

    def tell(place):
        pl.semaphore_signal(
            barrier, inc=1, device_id=place, device_id_type=pl.DeviceIdType.MESH
        )

    def notice_to(position):
        return pltpu.make_async_remote_copy(
            src_ref=notice.at[pl.ds(0, 1)],
            dst_ref=notices.at[pl.ds(device_pos, 1)],
            send_sem=notice_send_sem,
            recv_sem=notice_recv_sem,
            device_id=place_of(position),
            device_id_type=pl.DeviceIdType.MESH,
        )

    def verdict_to(position):
        return pltpu.make_async_remote_copy(
            src_ref=notice.at[pl.ds(8, 1)],
            dst_ref=verdict.at[pl.ds(0, 1)],
            send_sem=verdict_send_sem,
            recv_sem=verdict_recv_sem,
            device_id=place_of(position),
            device_id_type=pl.DeviceIdType.MESH,
        )

    def rows_done(ref, count, semaphore):
        rows = ref.at[pl.ds(0, count)]
        return pltpu.make_async_copy(rows, rows, semaphore)

    def copy_of(index):
        rows = pl.ds(offsets[index], rows_of[index])
        return pltpu.make_async_remote_copy(
            src_ref=sent.at[rows],
            dst_ref=arrived.at[rows],
            send_sem=send_sem,
            recv_sem=recv_sem,
            device_id=places[index],
            device_id_type=pl.DeviceIdType.MESH,
        )

    index_loads = [
        pltpu.make_async_copy(source_ref, indices.at[index], index_sem.at[index // 2])
        for index, source_ref in enumerate((neighbor_face_hbm, seam_hbm, neighbor_hbm))
    ]
    loads = [
        pltpu.make_async_copy(source_ref, target_ref, load_sem.at[index])
        for index, (source_ref, target_ref) in enumerate(
            [
                (face_tables_hbm, face_tables),
                (tables_hbm, tables),
                (register_hbm, register),
            ]
        )
    ]
    nodes = state.shape[0]
    piece = -(-nodes // 5)
    state_loads = [
        pltpu.make_async_copy(
            state_hbm.at[pl.ds(start, min(piece, nodes - start))],
            state.at[pl.ds(start, min(piece, nodes - start))],
            load_sem.at[3],
        )
        for start in range(0, nodes, piece)
    ]
    for load in index_loads + state_loads + loads:
        load.start()
    notices[...] = jnp.zeros_like(notices)
    barrier = pltpu.get_barrier_semaphore()
    for index, place in enumerate(places):
        if beyond(index) is None:
            tell(place)
        else:
            pl.when(jnp.logical_not(beyond(index)))(functools.partial(tell, place))
    for collector in collectors:

        @pl.when(device_pos == collector)
        def _():
            for position in range(device_count - 1, -1, -1):
                if position != collector:
                    tell(place_of(position))

    padded[...] = jnp.zeros_like(padded)
    level = iota((8, columns), 1) % levels
    link_iota = iota((link_rows, LANES), 0)
    wide_iota = iota((link_rows, columns), 0)
    target = jnp.full((link_rows, LANES), -1, jnp.int32)
    base_wide = jnp.zeros((link_rows, columns), f32)
    base_back = jnp.zeros((link_rows, LANES), f32)
    for index, place in enumerate(places):
        target = jnp.where(link_iota == index, place[0] * strip_count + place[1], target)
        base_wide = jnp.where(wide_iota == index, float(offsets[index] + 1), base_wide)
        base_back = jnp.where(link_iota == index, float(offsets[index ^ 1] + 1), base_back)
    from_elem = iota((LANES, columns), 0)
    to_elem = iota((LANES, columns), 1) // levels
    reach = jnp.concatenate(
        [
            jnp.concatenate(
                [onehot((from_elem < elems) & (from_elem < to_elem)), onehot(from_elem < elems)],
                axis=0,
            ),
            jnp.concatenate(
                [onehot(from_elem == to_elem), onehot(from_elem < 0)], axis=0
            ),
        ],
        axis=1,
    )
    pair = indices.at[pl.ds(0, 2)]
    pltpu.make_async_copy(pair, pair, index_sem.at[0]).wait()

    face_back, codes = [
        jnp.concatenate([indices[index]] * inner, axis=1) for index in range(2)
    ]
    turn = codes % 4
    flipped = codes // 4
    own_face = iota((4, LANES), 0)
    quarter = (face_back + turn - own_face + 4) % 4
    odd = jnp.where(quarter % 2 == 1, 1.0, 0.0)
    notice[:8] = jnp.broadcast_to(jnp.sum(odd, axis=0, keepdims=True), (8, LANES))
    early = device_pos >= device_count - strip_count // 2

    def meet():
        count = link_count + len(collectors) - jnp.where(collects, 1, 0)
        for index in range(link_count):
            if before_start(index) is not None:
                count = count - jnp.where(before_start(index), 1, 0)
        pl.semaphore_wait(barrier, count)
        for index in range(link_count):
            if beyond(index) is not None:

                @pl.when(beyond(index))
                def _():
                    pl.semaphore_signal(
                        ready.at[links[index][1] - 1],
                        inc=1,
                        device_id=places[index],
                        device_id_type=pl.DeviceIdType.MESH,
                    )

    def notify():
        for collector in collectors:

            @pl.when(device_pos != collector)
            def _():
                notice_to(collector).start()

    @pl.when(early)
    def _():
        meet()
        notify()

    side = jnp.where(quarter == 0, 1.0, -1.0)
    cosine = jnp.where(turn == 0, 1.0, 0.0) - jnp.where(turn == 2, 1.0, 0.0)
    sine = jnp.where(turn == 3, 1.0, 0.0) - jnp.where(turn == 1, 1.0, 0.0)

    index_loads[2].wait()
    loads[0].wait()
    pltpu.make_async_copy(state, state, load_sem.at[3]).wait()
    across = jnp.concatenate([indices[2]] * inner, axis=1)
    owner = across // elems
    place_in = across % elems
    member = [
        jnp.where(owner[face : face + 1] == target, 1.0, 0.0) for face in range(4)
    ]
    extras = [
        jnp.concatenate([part, jnp.zeros_like(part)], axis=0)
        for part in (flipped.astype(f32), cosine, sine, side)
    ]
    nothing = jnp.zeros_like(member[0])
    before = [nothing, member[0], member[0] + member[1], member[0] + member[1] + member[2]]
    left = jnp.concatenate(member + extras, axis=0).astype(bf16)
    right = jnp.concatenate(before + [jnp.zeros_like(part) for part in extras], axis=0)
    wide = dot(jnp.concatenate([left, right.astype(bf16)], axis=1), reach)
    spots = []
    for face in range(4):
        part = wide[face * link_rows : (face + 1) * link_rows]
        chosen = part[:, columns:] * (base_wide + inner * part[:, :columns])
        spots.append(jnp.sum(chosen, axis=0, keepdims=True))
    extra_row = 4 * link_rows
    flip_wide, cos_wide, sin_wide, side_wide = [
        wide[extra_row + 8 * index : extra_row + 8 * index + 8, columns:]
        for index in range(4)
    ]

    def stretched(per_face):
        rows = []
        for values in per_face:
            rows.append(values)
            rows.append(jnp.zeros_like(values))
        wide = dot(jnp.concatenate(rows, axis=0).astype(bf16), reach[:LANES, columns:])
        return [wide[8 * index : 8 * index + 8] for index in range(len(per_face))]

    def rows_for(slot, stride):
        spot = slot + (level[:1] % inner + level[:1] // inner * stride).astype(f32)
        return jnp.where(slot > 0.5, spot, 0.0)

    def hot_rows(count, spots):
        count_iota = (iota((count, columns), 0) + 1).astype(f32)
        return jnp.concatenate(
            [
                onehot(
                    count_iota == jnp.broadcast_to(spots[face], (count, columns))
                )
                for face in range(4)
            ],
            axis=1,
        )

    pack = hot_rows(total_rows, [rows_for(spot, 0) for spot in spots])

    def over_faces(wide, rows):
        return jnp.concatenate(
            [jnp.broadcast_to(wide[face : face + 1], (rows, columns)) for face in range(4)],
            axis=1,
        )

    def to_fields(block):
        return jnp.concatenate(
            [
                jnp.concatenate(
                    [
                        block[face * 8 : face * 8 + 8, field * columns : (field + 1) * columns]
                        for face in range(4)
                    ],
                    axis=1,
                )
                for field in range(4)
            ],
            axis=0,
        )

    def to_faces(block):
        return jnp.concatenate(
            [
                jnp.concatenate(
                    [
                        block[field * 8 : field * 8 + 8, face * columns : (face + 1) * columns]
                        for field in range(4)
                    ],
                    axis=1,
                )
                for face in range(4)
            ],
            axis=0,
        )

    flip_all, cos_all, sin_all, side_all = [
        over_faces(wide, 8) for wide in (flip_wide, cos_wide, sin_wide, side_wide)
    ]
    level_all = iota((half, span), 1) % levels // inner

    for field in range(4):
        padded[field, :25] = state[:, field, :]
    values = jnp.concatenate([padded[field] for field in range(4)], axis=1)
    on_faces = dot3(face_tables[:, :96], values)
    traces, slopes, flipped_traces, flipped_slopes = [
        to_fields(on_faces[32 * part : 32 * part + 32]) for part in range(4)
    ]

    def aligned(plain, mirrored):
        parts = [
            jnp.where(
                flip_all > 0.5,
                mirrored[field * 8 : field * 8 + 8],
                plain[field * 8 : field * 8 + 8],
            )
            for field in range(4)
        ]
        parts[1], parts[2] = (
            cos_all * parts[1] - sin_all * parts[2],
            cos_all * parts[2] + sin_all * parts[1],
        )
        return parts

    message = aligned(traces, flipped_traces) + [
        side_all * part for part in aligned(slopes, flipped_slopes)
    ]
    high, low = halves(jnp.concatenate(message, axis=0))
    pieces = []
    for part in (high, low):
        for index in range(outer_levels):
            pieces.append(jnp.where(level_all == index, part, jnp.zeros_like(part)))
    stacked = dot_t(pack, jnp.concatenate(pieces, axis=0))
    sent[...] = stacked[:, :LANES] + stacked[:, LANES:]
    pl.when(jnp.logical_not(early))(meet)
    order = sorted(
        range(link_count), key=lambda index: (links[index][1] < 0, abs(links[index][1]))
    )
    for index in order:
        if before_start(index) is None:
            copy_of(index).start()
        else:
            pl.when(jnp.logical_not(before_start(index)))(copy_of(index).start)
    pl.when(jnp.logical_not(early))(notify)
    always = device_pos >= 0

    @pl.when(always)
    def _():
        first_of = owner * (4 * elems)
        key = (first_of + face_back * elems + place_in).astype(f32)
        first_of = first_of.astype(f32)
        key_down = jnp.transpose(jnp.concatenate([key, key], axis=0))
        back_rows = []
        for face in range(4):
            smaller = jnp.zeros((elems, LANES), f32)
            for other in range(4):
                rival = jnp.broadcast_to(key_down[:elems, other : other + 1], (elems, LANES))
                mine = (rival < key[face : face + 1]) & (rival >= first_of[face : face + 1])
                smaller = smaller + jnp.where(mine, 1.0, 0.0)
            rank = jnp.sum(smaller, axis=0, keepdims=True)
            back_rows.append(
                jnp.sum(member[face] * (base_back + inner * rank), axis=0, keepdims=True)
            )
        at_home = owner == device_pos
        homes = [
            jnp.where(at_home & (face_back == face), place_in + 1, 0).astype(f32)
            for face in range(4)
        ]
        back, *homes = stretched([jnp.concatenate(back_rows, axis=0)] + homes)
        spread[...] = hot_rows(
            outer_levels * LANES,
            [rows_for(back[face : face + 1], LANES) for face in range(4)],
        )

        slopes_out = slopes * over_faces(side_wide, 32)
        both_high, both_low = halves(jnp.concatenate([traces, slopes_out], axis=0))
        both = jnp.concatenate([both_high, both_low], axis=0)
        found = jnp.zeros((128, span), f32)
        for face in range(4):
            home_spot = jnp.where(
                homes[face] > 0.5, homes[face] * levels + (level - levels + 1).astype(f32), 0.0
            )
            found = found + dot(
                both[:, face * columns : (face + 1) * columns],
                hot_rows(columns, [home_spot[into : into + 1] for into in range(4)]),
            )
        found = found[:64] + found[64:]
        known[:32] = traces
        known[32:64] = found[:32]
        known[64:96] = found[32:] - slopes
        known[96:128] = over_faces(
            0.5 + viscosity * penalty - 0.25 * lift_gain * viscosity * (1.0 + side_wide), 32
        )
        pressure, vel_u, vel_v, theta = [
            values[:, field * columns : (field + 1) * columns] for field in range(4)
        ]
        nothing = jnp.zeros_like(pressure)
        flux_x = jnp.concatenate([vel_u, pressure, nothing, theta * vel_u], axis=1)
        flux_y = jnp.concatenate([vel_v, nothing, pressure, theta * vel_v], axis=1)
        loads[1].wait()
        loads[2].wait()
        for field in range(4):
            padded[field, :25] = register[:, field, :]
        held = jnp.concatenate([padded[field] for field in range(4)], axis=1)
        own = dot3(tables[:32, :288], jnp.concatenate([flux_x, flux_y, values], axis=0))
        own = section_a * held + step_size * own
        moved = values + section_b * own
        for field in range(4):
            sides = slice(field * columns, (field + 1) * columns)
            own_register[:, field, :] = own[:25, sides]
            own_state[:, field, :] = moved[:25, sides]

    for index in order:
        if before_start(index) is not None:

            @pl.when(before_start(index))
            def _():
                pl.semaphore_wait(ready.at[-links[index][1] - 1], 1)
                copy_of(index).start()

    rows_done(arrived, total_rows, recv_sem).wait()
    filler = jnp.zeros((LANES - total_rows, LANES), f32)
    turned = jnp.transpose(jnp.concatenate([arrived[...], filler], axis=0))
    turned = jnp.concatenate(
        [turned[half * index : half * (index + 1)] for index in range(outer_levels)], axis=1
    )
    high, low = halves(turned)
    far = dot(jnp.concatenate([high, low], axis=0), spread[...])
    far = far[:half] + far[half:]
    inside = known[:32]
    outside = known[32:64] + far[:32]
    jump = outside - inside
    slope_term = (0.5 * viscosity) * (known[64:96] + far[32:])
    weight = known[96:128]
    terms = []
    for face in range(4):
        sides = slice(face * columns, (face + 1) * columns)
        ins = [inside[field * 8 : field * 8 + 8, sides] for field in range(4)]
        outs = [outside[field * 8 : field * 8 + 8, sides] for field in range(4)]
        step = [jump[field * 8 : field * 8 + 8, sides] for field in range(4)]
        normal = 1 + face % 2
        sign = 1.0 if face < 2 else -1.0
        raw_in, raw_out = ins[normal], outs[normal]
        wave = weight[:8, sides] + 0.5 * jnp.maximum(jnp.abs(raw_in), jnp.abs(raw_out))
        drops = [
            (-0.5 * sign) * step[normal],
            None,
            None,
            (0.5 * sign) * (ins[3] * raw_in - outs[3] * raw_out),
        ]
        drops[normal] = (-0.5 * sign) * step[0]
        rows = []
        for field in range(4):
            term = wave * step[field] + slope_term[field * 8 : field * 8 + 8, sides]
            rows.append(term if drops[field] is None else term + drops[field])
        terms.append(jnp.concatenate(rows, axis=0))
    face_term = jnp.concatenate(terms, axis=1)

    @pl.when(collects)
    def _():
        rows_done(notices, device_count - 1, notice_recv_sem).wait()

        @pl.when(device_pos == herald)
        def _():
            heard = jnp.max(notices[...], axis=0, keepdims=True) + notice[:1]
            notice[8:] = jnp.broadcast_to(heard, (8, LANES))
            for position in range(device_count):
                if position not in collectors:
                    verdict_to(position).start()

    heard = notice[:8]
    for start in range(0, notices.shape[0], 8):
        heard = jnp.maximum(heard, notices[start : start + 8])
    sideways[0] = jnp.where(jnp.max(heard) > 0.5, 1, 0)
    late = dot3(
        tables[32:, :192], jnp.concatenate([to_faces(face_term), to_faces(jump)], axis=0)
    )
    for field in range(4):
        late_part[:, field, :] = late[:25, field * columns : (field + 1) * columns]

    @pl.when(device_pos == herald)
    def _():
        rows_done(notices, device_count - len(collectors), verdict_send_sem).wait()

    @pl.when(collects)
    def _():
        rows_done(notice, len(collectors) - 1, notice_send_sem).wait()

    @pl.when(jnp.logical_not(collects))
    def _():
        rows_done(notice, len(collectors), notice_send_sem).wait()
        rows_done(verdict, 1, verdict_recv_sem).wait()
        sideways[0] = jnp.where(jnp.max(verdict[:1]) > 0.5, 1, 0)

    rows_done(sent, total_rows, send_sem).wait()


def closing_kernel(
    own_register, own_state, late, next_state, next_register, new_state, new_register, sems
):
    nodes = late.shape[0]
    piece = -(-nodes // 3)
    for start in range(0, nodes, piece):
        rows = pl.ds(start, min(piece, nodes - start))
        part = step_size * late[rows]
        new_register[rows] = own_register[rows] + part
        pltpu.make_async_copy(new_register.at[rows], next_register.at[rows], sems.at[0]).start()
        new_state[rows] = own_state[rows] + section_b * part
        pltpu.make_async_copy(new_state.at[rows], next_state.at[rows], sems.at[1]).start()
    pltpu.make_async_copy(new_register, next_register, sems.at[0]).wait()
    pltpu.make_async_copy(new_state, next_state, sems.at[1]).wait()


def start_kernel(state, register, own_register, own_state):
    own_register[...] = section_a * register[...]
    own_state[...] = state[...] + section_b * own_register[...]


def body(curve_count, strip_count, state, register, neighbor, neighbor_face, seam):
    elems = neighbor.shape[1]
    columns = state.shape[2]
    levels = columns // elems
    inner = LANES // elems
    outer_levels = levels // inner
    reach = min(7, (curve_count - 1) // 2)
    slots = (TW + reach - 1) // reach
    links, rows_of = [], []
    for distance in range(reach, 0, -1):
        for direction in (1, -1):
            links.append(("curve", direction * distance))
            rows_of.append(-(-slots * inner // 8) * 8)
    for direction in (1, -1):
        links.append(("sub", direction))
        rows_of.append(-(-TW * inner // 8) * 8)
    offsets = [sum(rows_of[:index]) for index in range(len(links))]
    total_rows = sum(rows_of)
    plan = (elems, levels, curve_count, strip_count, links, rows_of, offsets)
    vmem = pl.BlockSpec(memory_space=pltpu.VMEM)
    nodes_first = jnp.transpose(state, (1, 0, 2))
    register_first = jnp.transpose(register, (1, 0, 2))
    shape = nodes_first.shape

    def call(kernel, tables, more, outputs, out_specs, scratch, collective_id):
        tables = [jnp.asarray(table) for table in tables]
        operands = (nodes_first, neighbor, neighbor_face, seam, *tables, *more)
        return pl.pallas_call(
            functools.partial(kernel, plan),
            out_shape=outputs,
            in_specs=[pl.BlockSpec(memory_space=pl.ANY)] * len(operands),
            out_specs=out_specs,
            scratch_shapes=scratch,
            compiler_params=pltpu.CompilerParams(
                collective_id=collective_id, has_side_effects=True
            ),
        )(*[pltpu.with_memory_space_constraint(operand, pltpu.HBM) for operand in operands])

    def two_rounds():
        change = call(
            two_round_kernel,
            (build_tables(),),
            (),
            pltpu.VMEM(nodes_first.shape, f32),
            vmem,
            [
                pltpu.VMEM(shape, f32),
                pltpu.VMEM(neighbor.shape, jnp.int32),
                pltpu.VMEM(neighbor.shape, jnp.int32),
                pltpu.VMEM(neighbor.shape, jnp.int32),
                pltpu.VMEM((224, 384), bf16),
                pltpu.VMEM((4, 32, columns), f32),
                pltpu.VMEM((2, total_rows, LANES), f32),
                pltpu.VMEM((2, total_rows, LANES), f32),
                pltpu.VMEM((32, 4 * columns), f32),
                pltpu.VMEM((128, 4 * columns), f32),
                pltpu.VMEM((128, columns), f32),
                pltpu.SemaphoreType.DMA((5,)),
                pltpu.SemaphoreType.DMA((2, len(links))),
                pltpu.SemaphoreType.DMA((2, len(links))),
            ],
            0,
        )
        started = pl.pallas_call(
            start_kernel,
            out_shape=(pltpu.VMEM(shape, f32), pltpu.VMEM(shape, f32)),
            in_specs=[vmem, vmem],
            out_specs=(vmem, vmem),
        )(*[pltpu.with_memory_space_constraint(x, pltpu.HBM) for x in (nodes_first, register_first)])
        return *started, change

    device_count = curve_count * strip_count
    if device_count <= DIRECT_LIMIT and total_rows <= LANES and outer_levels * 64 == LANES:
        *parts, sideways = call(
            direct_kernel,
            build_direct_tables(),
            (register_first,),
            (pltpu.VMEM(shape, f32),) * 3 + (pltpu.SMEM((1,), jnp.int32),),
            (vmem,) * 3 + (pl.BlockSpec(memory_space=pltpu.SMEM),),
            [
                pltpu.VMEM(shape, f32),
                pltpu.VMEM((3, *neighbor.shape), jnp.int32),
                pltpu.VMEM((128, LANES), bf16),
                pltpu.VMEM((64, 384), bf16),
                pltpu.VMEM((4, 32, columns), f32),
                pltpu.VMEM((total_rows, LANES), f32),
                pltpu.VMEM((total_rows, LANES), f32),
                pltpu.VMEM((16, LANES), f32),
                pltpu.VMEM((-(-device_count // 8) * 8, LANES), f32),
                pltpu.VMEM((8, LANES), f32),
                pltpu.VMEM((outer_levels * LANES, 4 * columns), bf16),
                pltpu.VMEM((128, 4 * columns), f32),
                pltpu.VMEM(shape, f32),
                pltpu.SemaphoreType.REGULAR((reach,)),
                pltpu.SemaphoreType.DMA((2,)),
                pltpu.SemaphoreType.DMA((4,)),
                pltpu.SemaphoreType.DMA,
                pltpu.SemaphoreType.DMA,
                pltpu.SemaphoreType.DMA,
                pltpu.SemaphoreType.DMA,
                pltpu.SemaphoreType.DMA,
                pltpu.SemaphoreType.DMA,
            ],
            1,
        )
        parts = lax.cond(
            sideways[0] == 0, lambda kept: tuple(kept), lambda _: two_rounds(), parts
        )
    else:
        parts = two_rounds()
    new = pl.pallas_call(
        closing_kernel,
        out_shape=(jax.ShapeDtypeStruct(shape, f32), jax.ShapeDtypeStruct(shape, f32)),
        in_specs=[vmem] * 3,
        out_specs=(pl.BlockSpec(memory_space=pl.ANY),) * 2,
        scratch_shapes=[
            pltpu.VMEM(shape, f32),
            pltpu.VMEM(shape, f32),
            pltpu.SemaphoreType.DMA((2,)),
        ],
    )(*parts)
    return tuple(jnp.transpose(part, (1, 0, 2)) for part in new)


def solution(mesh):
    wide = P(None, None, ("curve", "sub"))
    flat = P(None, ("curve", "sub"))
    return jax.shard_map(
        functools.partial(body, mesh.shape["curve"], mesh.shape["sub"]),
        mesh=mesh,
        in_specs=(wide, wide, flat, flat, flat),
        out_specs=(wide, wide),
        check_vma=False,
    )
```

```python
import functools
import math

import jax
import jax.numpy as jnp
import ml_dtypes
import numpy as np
from jax import lax
from jax.experimental import pallas as pl
from jax.experimental.pallas import tpu as pltpu
from jax.sharding import PartitionSpec as P

TW = 8
LANES = 128
DIRECT_LIMIT = 64

lift_gain = 10.0
step_size = 0.02
viscosity = 0.05
penalty = 2.0
section_a = -567301805773.0 / 1357537059087.0
section_b = 2404267990393.0 / 2016746695238.0

f32 = jnp.float32
bf16 = jnp.bfloat16


def build_derivative():
    points = np.array([-1.0, -math.sqrt(3.0 / 7.0), 0.0, math.sqrt(3.0 / 7.0), 1.0])
    weights = np.array(
        [
            1.0 / np.prod([points[row] - points[col] for col in range(5) if col != row])
            for row in range(5)
        ]
    )
    table = np.zeros((5, 5))
    for row in range(5):
        for col in range(5):
            if row != col:
                table[row, col] = weights[col] / weights[row] / (points[row] - points[col])
        table[row, row] = -np.sum(table[row])
    return table


def face_node(face, node):
    return [(4, node), (node, 4), (0, node), (node, 0)][face]


def split_const(table):
    high = table.astype(ml_dtypes.bfloat16)
    low = (table - high.astype(np.float64)).astype(ml_dtypes.bfloat16)
    return np.concatenate([high, low, high], axis=1)


def element_tables():
    d = build_derivative()
    eye = np.eye(5)
    dx = np.zeros((32, 32))
    dy = np.zeros((32, 32))
    dx[:25, :25] = np.kron(d, eye)
    dy[:25, :25] = np.kron(eye, d)
    pick = np.zeros((32, 32))
    for face in range(4):
        for node in range(5):
            a, b = face_node(face, node)
            pick[face * 8 + node, a * 5 + b] = 1.0
    normal_x = np.repeat([1.0, 0.0, -1.0, 0.0], 8)
    normal_y = np.repeat([0.0, 1.0, 0.0, -1.0], 8)
    lift_x = pick.T * normal_x[None] * (0.5 * lift_gain)
    lift_y = pick.T * normal_y[None] * (0.5 * lift_gain)
    return dx, dy, pick, normal_x, normal_y, lift_x, lift_y


def build_tables():
    dx, dy, pick, _, _, lift_x, lift_y = element_tables()
    grad_x = np.concatenate([dx, lift_x], axis=1)
    grad_y = np.concatenate([dy, lift_y], axis=1)
    grad = np.concatenate([grad_x, grad_y, pick @ grad_x, pick @ grad_y], axis=0)
    volume = np.concatenate([-dx, -dy, lift_gain * pick.T], axis=1)
    late = lift_gain * 0.5 * viscosity * pick.T
    out = np.zeros((224, 384), ml_dtypes.bfloat16)
    out[:128, :192] = split_const(grad)
    out[:128, 192:288] = split_const(grad[:, 32:])
    out[128:160, :288] = split_const(volume)
    out[160:192, :96] = split_const(late)
    out[192:224, :32] = pick.astype(ml_dtypes.bfloat16)
    out[192:224, 32:64] = pick.astype(ml_dtypes.bfloat16)
    return out


def build_direct_tables():
    dx, dy, pick, normal_x, normal_y, lift_x, lift_y = element_tables()
    slope = normal_x[:, None] * (pick @ dx) + normal_y[:, None] * (pick @ dy)
    base = np.concatenate([-dx, -dy, viscosity * (dx @ dx + dy @ dy)], axis=1)
    jump = viscosity * (dx @ lift_x + dy @ lift_y)
    late = np.concatenate([lift_gain * pick.T, jump], axis=1)
    mirror = np.arange(32).reshape(4, 8)
    mirror[:, :5] = mirror[:, 4::-1]
    mirror = mirror.reshape(-1)
    first = np.zeros((128, LANES), ml_dtypes.bfloat16)
    first[:, :96] = split_const(
        np.concatenate([pick, slope, pick[mirror], slope[mirror]], axis=0)
    )
    out = np.zeros((64, 384), ml_dtypes.bfloat16)
    out[:32, :288] = split_const(base)
    out[32:, :192] = split_const(late)
    return first, out


def halves(x):
    high = x.astype(bf16)
    low = (x - high.astype(f32)).astype(bf16)
    return high, low


def dot(a, b):
    return lax.dot_general(a, b, (((1,), (0,)), ((), ())), preferred_element_type=f32)


def dot_t(a, b):
    return lax.dot_general(a, b, (((1,), (1,)), ((), ())), preferred_element_type=f32)


def dot3(table, x):
    high, low = halves(x)
    return dot(table, jnp.concatenate([high, high, low], axis=0))


def onehot(mask):
    return jnp.where(mask, 1.0, 0.0).astype(bf16)


def permute(x, perm):
    rows = x.shape[0]
    high, low = halves(x)
    both = dot(jnp.concatenate([high, low], axis=0), perm)
    return both[:rows] + both[rows:]


def iota(shape, dim):
    return lax.broadcasted_iota(jnp.int32, shape, dim)


def two_round_kernel(
    plan,
    state_hbm,
    neighbor_hbm,
    neighbor_face_hbm,
    seam_hbm,
    tables_hbm,
    change,
    state,
    neighbor,
    neighbor_face,
    seam,
    tables,
    padded,
    sent,
    arrived,
    own_faces,
    early_grads,
    early_change,
    load_sem,
    send_sem,
    recv_sem,
):
    elems, levels, curve_count, strip_count, links, rows_of, offsets = plan
    columns = elems * levels
    inner = LANES // elems
    outer_levels = levels // inner
    groups = 4 * outer_levels
    span = 4 * LANES
    total_rows = offsets[-1] + rows_of[-1]
    link_count = len(links)
    link_rows = -(-link_count // 8) * 8

    curve_pos = lax.axis_index("curve")
    strip_pos = lax.axis_index("sub")
    device_pos = curve_pos * strip_count + strip_pos
    places = []
    for axis, step in links:
        if axis == "curve":
            places.append((lax.rem(curve_pos + step + curve_count, curve_count), strip_pos))
        else:
            places.append((curve_pos, lax.rem(strip_pos + step + strip_count, strip_count)))

    barrier = pltpu.get_barrier_semaphore()
    for place in places:
        pl.semaphore_signal(
            barrier, inc=1, device_id=place, device_id_type=pl.DeviceIdType.MESH
        )
    loads = [
        pltpu.make_async_copy(source_ref, target_ref, load_sem.at[index])
        for index, (source_ref, target_ref) in enumerate(
            [
                (neighbor_hbm, neighbor),
                (neighbor_face_hbm, neighbor_face),
                (seam_hbm, seam),
                (state_hbm, state),
                (tables_hbm, tables),
            ]
        )
    ]
    for load in loads:
        load.start()
    for load in loads[:3]:
        load.wait()

    def widen(ref):
        block = ref[...]
        return jnp.concatenate([block] * inner, axis=1)

    across = widen(neighbor)
    face_back = widen(neighbor_face)
    codes = widen(seam)
    owner = across // elems
    place_in = across % elems
    turn = codes % 4
    flipped = codes // 4
    sub_level = iota((4, LANES), 1) // elems
    position = face_back * LANES + sub_level * elems + place_in
    source = jnp.where(owner == device_pos, position, -1)
    heading = (face_back + turn) % 4
    cosine = jnp.where(turn == 0, 1.0, 0.0) - jnp.where(turn == 2, 1.0, 0.0)
    sine = jnp.where(turn == 3, 1.0, 0.0) - jnp.where(turn == 1, 1.0, 0.0)
    head_x = jnp.where(heading == 0, 1.0, 0.0) - jnp.where(heading == 2, 1.0, 0.0)
    head_y = jnp.where(heading == 1, 1.0, 0.0) - jnp.where(heading == 3, 1.0, 0.0)

    link_iota = iota((link_rows, LANES), 0)
    target = jnp.full((link_rows, LANES), -1, jnp.int32)
    base = jnp.zeros((link_rows, LANES), f32)
    for index, place in enumerate(places):
        target = jnp.where(link_iota == index, place[0] * strip_count + place[1], target)
        base = jnp.where(link_iota == index, float(offsets[index] + 1), base)
    base = base + (iota((link_rows, LANES), 1) // elems).astype(f32)
    member = [
        jnp.where(owner[face : face + 1] == target, 1.0, 0.0) for face in range(4)
    ]
    from_lane = iota((LANES, 2 * LANES), 0)
    to_lane = iota((LANES, 2 * LANES), 1)
    same = from_lane // elems == (to_lane % LANES) // elems
    earlier = same & ((from_lane < to_lane) | (to_lane >= LANES))
    counts = dot(jnp.concatenate(member, axis=0).astype(bf16), onehot(earlier))
    before = jnp.zeros((link_rows, LANES), f32)
    slot_rows = []
    for face in range(4):
        part = counts[face * link_rows : (face + 1) * link_rows]
        rank = part[:, :LANES] + before
        before = before + part[:, LANES:]
        slot_rows.append(
            jnp.sum(member[face] * (base + inner * rank), axis=0, keepdims=True)
        )
    slot_row = jnp.concatenate(slot_rows, axis=1)
    pack = onehot(
        (iota((total_rows, span), 0) + 1).astype(f32)
        == jnp.broadcast_to(slot_row, (total_rows, span))
    )
    pack2 = jnp.concatenate([pack, pack], axis=1)

    def local_table():
        span_iota = iota((span, LANES), 0)
        return jnp.concatenate(
            [onehot(span_iota == source[face : face + 1]) for face in range(4)], axis=1
        )

    meta_iota = iota((8, LANES), 0)
    meta_blocks = []
    for face in range(4):
        block = jnp.zeros((8, LANES), f32)
        for row, values in enumerate(
            [flipped.astype(f32), cosine, sine, (position + 1).astype(f32)]
        ):
            block = jnp.where(meta_iota == row, values[face : face + 1], block)
        meta_blocks.append(block)
    meta = jnp.concatenate(meta_blocks, axis=1)
    heads_x = jnp.concatenate(
        [jnp.broadcast_to(head_x[face : face + 1], (8, LANES)) for face in range(4)], axis=0
    )
    heads_y = jnp.concatenate(
        [jnp.broadcast_to(head_y[face : face + 1], (8, LANES)) for face in range(4)], axis=0
    )

    def to_exchange(faces):
        return jnp.concatenate(
            [
                jnp.concatenate(
                    [
                        faces[face * 8 : face * 8 + 8, group * LANES : (group + 1) * LANES]
                        for face in range(4)
                    ],
                    axis=1,
                )
                for group in range(groups)
            ],
            axis=0,
        )

    def from_exchange(block):
        return jnp.concatenate(
            [
                jnp.concatenate(
                    [
                        block[group * 8 : group * 8 + 8, face * LANES : (face + 1) * LANES]
                        for group in range(groups)
                    ],
                    axis=1,
                )
                for face in range(4)
            ],
            axis=0,
        )

    data_lanes = groups * 8
    field_lanes = outer_levels * 8
    lane = iota((total_rows, LANES), 1)
    node_lane = lane % 8
    in_data = lane < data_lanes

    def copy_of(turn_index, index):
        rows = pl.ds(offsets[index], rows_of[index])
        return pltpu.make_async_remote_copy(
            src_ref=sent.at[turn_index, rows],
            dst_ref=arrived.at[turn_index, rows],
            send_sem=send_sem.at[turn_index, index],
            recv_sem=recv_sem.at[turn_index, index],
            device_id=places[index],
            device_id_type=pl.DeviceIdType.MESH,
        )

    def post(turn_index, block, flags):
        if flags is None:
            pieces = [block, meta]
            if data_lanes + 8 < LANES:
                pieces.append(jnp.zeros((LANES - data_lanes - 8, span), f32))
            block = jnp.concatenate(pieces, axis=0)
        high, low = halves(block)
        message = dot_t(pack2, jnp.concatenate([high, low], axis=1))
        if flags is None:
            flags = [
                jnp.broadcast_to(
                    message[:, data_lanes + index : data_lanes + index + 1], message.shape
                )
                for index in range(3)
            ]
        else:
            rest = jnp.zeros((total_rows, LANES - data_lanes), f32)
            message = jnp.concatenate([message, rest], axis=1)
        flip, cos, sin = flags
        mirrored = message
        for node, shift in ((0, LANES - 4), (1, LANES - 2), (3, 2), (4, 4)):
            mirrored = jnp.where(
                node_lane == node, pltpu.roll(message, shift, axis=1), mirrored
            )
        aligned = jnp.where(in_data & (flip > 0.5), mirrored, message)
        field = lane // field_lanes
        turned_u = cos * aligned - sin * pltpu.roll(aligned, LANES - field_lanes, axis=1)
        turned_v = cos * aligned + sin * pltpu.roll(aligned, field_lanes, axis=1)
        aligned = jnp.where(field == 1, turned_u, jnp.where(field == 2, turned_v, aligned))
        sent[turn_index] = aligned
        if turn_index == 0:
            pl.semaphore_wait(barrier, link_count)
        for index in range(link_count):
            copy_of(turn_index, index).start()
        return flags

    def gather_local(block):
        rows = block.shape[0]
        high, low = halves(block)
        both = dot(jnp.concatenate([high, low], axis=0), local_table())
        return both[:rows] + both[rows:]

    def await_all(turn_index):
        for index in range(link_count):
            copy_of(turn_index, index).wait_recv()

    def spread_table():
        message = arrived[0]
        spot = jnp.broadcast_to(
            message[:, data_lanes + 3 : data_lanes + 4], (total_rows, span)
        )
        return onehot((iota((total_rows, span), 1) + 1).astype(f32) == spot)

    def collect(turn_index, spread):
        message = arrived[turn_index]
        high, low = halves(jnp.transpose(message)[:data_lanes])
        both = dot(jnp.concatenate([high, low], axis=0), spread)
        return both[:data_lanes] + both[data_lanes:]

    row = iota((columns, columns), 0)
    col = iota((columns, columns), 1)
    to_level = onehot(row == (col % elems) * levels + col // elems)
    to_elem = onehot(row == (col % levels) * elems + col // levels)

    padded[...] = jnp.zeros_like(padded)
    for load in loads[3:]:
        load.wait()
    for field in range(4):
        padded[field, :25] = state[:, field, :]
    nodal = permute(padded[...].reshape(128, columns), to_level)
    values = jnp.concatenate(
        [nodal[field * 32 : field * 32 + 32] for field in range(4)], axis=1
    )
    high, low = halves(values)
    faces_in = dot(tables[192:224, :64], jnp.concatenate([high, low], axis=0))

    def fields_of(wide):
        return [wide[:, field * columns : (field + 1) * columns] for field in range(4)]

    def elementwise_lanes(wide):
        return permute(jnp.concatenate(fields_of(wide), axis=0), to_elem)

    def early_part(values, faces_in, faces_out, grad_x, grad_y, face_gx, face_gy, own_slope):
        face_of_row = iota((32, columns), 0) // 8
        normal_x = jnp.where(face_of_row == 0, 1.0, 0.0) - jnp.where(face_of_row == 2, 1.0, 0.0)
        normal_y = jnp.where(face_of_row == 1, 1.0, 0.0) - jnp.where(face_of_row == 3, 1.0, 0.0)

        def flux_of(faces):
            speed = faces[1] * normal_x + faces[2] * normal_y
            return [speed, faces[0] * normal_x, faces[0] * normal_y, faces[3] * speed], speed

        inside, outside = fields_of(faces_in), fields_of(faces_out)
        gx_in, gy_in = fields_of(face_gx), fields_of(face_gy)
        slope_own = fields_of(own_slope)
        flux_in, speed_in = flux_of(inside)
        flux_out, speed_out = flux_of(outside)
        wave = 1.0 + jnp.maximum(jnp.abs(speed_in), jnp.abs(speed_out))
        terms = []
        for field in range(4):
            slope_in = gx_in[field] * normal_x + gy_in[field] * normal_y
            jump = outside[field] - inside[field]
            terms.append(
                0.5 * (flux_in[field] - flux_out[field])
                - 0.5 * viscosity * (slope_in - slope_own[field])
                + (0.5 * wave + viscosity * penalty) * jump
            )
        face_term = jnp.concatenate(terms, axis=1)
        pressure, vel_u, vel_v, theta = fields_of(values)
        nothing = jnp.zeros_like(pressure)
        flux_x = jnp.concatenate([vel_u, pressure, nothing, theta * vel_u], axis=1)
        flux_y = jnp.concatenate([vel_v, nothing, pressure, theta * vel_v], axis=1)
        tendency = dot3(
            tables[128:160, :288],
            jnp.concatenate(
                [flux_x - viscosity * grad_x, flux_y - viscosity * grad_y, face_term], axis=0
            ),
        )

        return elementwise_lanes(tendency)

    block_in = to_exchange(faces_in)
    flags = post(0, block_in, None)
    always = device_pos >= 0

    @pl.when(always)
    def _():
        own = from_exchange(gather_local(block_in))
        own_faces[...] = own
        early_grads[...] = dot3(
            tables[:128, :192], jnp.concatenate([values, own - faces_in], axis=0)
        )

    await_all(0)
    spread = spread_table()
    far_faces = from_exchange(collect(0, spread))
    face_grads = early_grads[64:128] + dot3(tables[64:128, 192:288], far_faces)
    face_gx, face_gy = face_grads[:32], face_grads[32:]
    wide_x = jnp.concatenate([heads_x] * groups, axis=1)
    wide_y = jnp.concatenate([heads_y] * groups, axis=1)
    block_grad = to_exchange(face_gx * wide_x + face_gy * wide_y)
    post(1, block_grad, flags)

    @pl.when(always)
    def _():
        own_slope = from_exchange(gather_local(block_grad))
        grads = early_grads[:64] + dot3(tables[:64, 192:288], far_faces)
        faces_out = own_faces[...] + far_faces
        grad_x, grad_y = grads[:32], grads[32:]
        early_change[...] = early_part(
            values, faces_in, faces_out, grad_x, grad_y, face_gx, face_gy, own_slope
        )

    await_all(1)
    far_slope = from_exchange(collect(1, spread))
    late = elementwise_lanes(dot3(tables[160:192, :96], far_slope))
    total = early_change[...] + late
    for field in range(4):
        change[:, field, :] = total[field * 32 : field * 32 + 25]

    for turn_index in range(2):
        for index in range(link_count):
            copy_of(turn_index, index).wait_send()


def direct_kernel(
    plan,
    state_hbm,
    neighbor_hbm,
    neighbor_face_hbm,
    seam_hbm,
    face_tables_hbm,
    tables_hbm,
    register_hbm,
    own_register,
    own_state,
    late_part,
    sideways,
    state,
    indices,
    face_tables,
    tables,
    padded,
    sent,
    arrived,
    notice,
    notices,
    verdict,
    spread,
    known,
    register,
    ready,
    index_sem,
    load_sem,
    send_sem,
    recv_sem,
    notice_send_sem,
    word_recv_sem,
    verdict_send_sem,
):
    elems, levels, curve_count, strip_count, links, rows_of, offsets = plan
    columns = elems * levels
    span = 4 * columns
    inner = LANES // elems
    outer_levels = levels // inner
    total_rows = offsets[-1] + rows_of[-1]
    link_count = len(links)
    link_rows = -(-link_count // 8) * 8
    half = LANES // outer_levels

    curve_pos = lax.axis_index("curve")
    strip_pos = lax.axis_index("sub")
    device_pos = curve_pos * strip_count + strip_pos

    def place_at(curve_step, strip_step):
        return (
            lax.rem(curve_pos + curve_step + curve_count, curve_count),
            lax.rem(strip_pos + strip_step + strip_count, strip_count),
        )

    places = [place_at(step, 0) if axis == "curve" else place_at(0, step) for axis, step in links]
    device_count = curve_count * strip_count
    herald = device_count // 2 - 1
    collectors = (0, 1, herald)
    collects = (device_pos < 2) | (device_pos == herald)

    def place_of(position):
        return (position // strip_count, position % strip_count)

    def beyond(index):
        axis, step = links[index]
        if axis == "curve" and step > 0:
            return curve_pos + step >= curve_count
        return None

    def before_start(index):
        axis, step = links[index]
        if axis == "curve" and step < 0:
            return curve_pos + step < 0
        return None

    def tell(place):
        pl.semaphore_signal(
            barrier, inc=1, device_id=place, device_id_type=pl.DeviceIdType.MESH
        )

    def notice_to(position):
        return pltpu.make_async_remote_copy(
            src_ref=notice.at[pl.ds(0, 1)],
            dst_ref=notices.at[pl.ds(device_pos, 1)],
            send_sem=notice_send_sem,
            recv_sem=word_recv_sem,
            device_id=place_of(position),
            device_id_type=pl.DeviceIdType.MESH,
        )

    def verdict_to(position):
        return pltpu.make_async_remote_copy(
            src_ref=notice.at[pl.ds(8, 1)],
            dst_ref=verdict.at[pl.ds(0, 1)],
            send_sem=verdict_send_sem,
            recv_sem=word_recv_sem,
            device_id=place_of(position),
            device_id_type=pl.DeviceIdType.MESH,
        )

    def rows_done(ref, count, semaphore):
        rows = ref.at[pl.ds(0, count)]
        return pltpu.make_async_copy(rows, rows, semaphore)

    def copy_of(index):
        rows = pl.ds(offsets[index], rows_of[index])
        return pltpu.make_async_remote_copy(
            src_ref=sent.at[rows],
            dst_ref=arrived.at[rows],
            send_sem=send_sem,
            recv_sem=recv_sem,
            device_id=places[index],
            device_id_type=pl.DeviceIdType.MESH,
        )

    index_loads = [
        pltpu.make_async_copy(source_ref, indices.at[index], index_sem.at[index // 2])
        for index, source_ref in enumerate((neighbor_face_hbm, seam_hbm, neighbor_hbm))
    ]
    loads = [
        pltpu.make_async_copy(source_ref, target_ref, load_sem.at[index])
        for index, (source_ref, target_ref) in enumerate(
            [
                (face_tables_hbm, face_tables),
                (tables_hbm, tables),
                (register_hbm, register),
            ]
        )
    ]
    nodes = state.shape[0]
    piece = -(-nodes // 5)
    state_loads = [
        pltpu.make_async_copy(
            state_hbm.at[pl.ds(start, min(piece, nodes - start))],
            state.at[pl.ds(start, min(piece, nodes - start))],
            load_sem.at[3],
        )
        for start in range(0, nodes, piece)
    ]
    for load in index_loads + state_loads + loads:
        load.start()
    notices[...] = jnp.zeros_like(notices)
    barrier = pltpu.get_barrier_semaphore()
    for index, place in enumerate(places):
        if beyond(index) is None:
            tell(place)
        else:
            pl.when(jnp.logical_not(beyond(index)))(functools.partial(tell, place))
    for collector in collectors:

        @pl.when(device_pos == collector)
        def _():
            for position in range(device_count - 1, -1, -1):
                if position != collector:
                    tell(place_of(position))

    padded[...] = jnp.zeros_like(padded)
    level = iota((8, columns), 1) % levels
    link_iota = iota((link_rows, LANES), 0)
    wide_iota = iota((link_rows, columns), 0)
    target = jnp.full((link_rows, LANES), -1, jnp.int32)
    base_wide = jnp.zeros((link_rows, columns), f32)
    base_back = jnp.zeros((link_rows, LANES), f32)
    for index, place in enumerate(places):
        target = jnp.where(link_iota == index, place[0] * strip_count + place[1], target)
        base_wide = jnp.where(wide_iota == index, float(offsets[index] + 1), base_wide)
        base_back = jnp.where(link_iota == index, float(offsets[index ^ 1] + 1), base_back)
    from_elem = iota((LANES, columns), 0)
    to_elem = iota((LANES, columns), 1) // levels
    reach = jnp.concatenate(
        [
            jnp.concatenate(
                [onehot((from_elem < elems) & (from_elem < to_elem)), onehot(from_elem < elems)],
                axis=0,
            ),
            jnp.concatenate(
                [onehot(from_elem == to_elem), onehot(from_elem < 0)], axis=0
            ),
        ],
        axis=1,
    )
    pair = indices.at[pl.ds(0, 2)]
    pltpu.make_async_copy(pair, pair, index_sem.at[0]).wait()

    face_back, codes = [
        jnp.concatenate([indices[index]] * inner, axis=1) for index in range(2)
    ]
    turn = codes % 4
    flipped = codes // 4
    own_face = iota((4, LANES), 0)
    quarter = (face_back + turn - own_face + 4) % 4
    odd = jnp.where(quarter % 2 == 1, 1.0, 0.0)
    notice[:8] = jnp.broadcast_to(jnp.sum(odd, axis=0, keepdims=True), (8, LANES))
    early = device_pos >= device_count - strip_count // 2

    def meet():
        count = link_count + len(collectors) - jnp.where(collects, 1, 0)
        for index in range(link_count):
            if before_start(index) is not None:
                count = count - jnp.where(before_start(index), 1, 0)
        pl.semaphore_wait(barrier, count)
        for index in range(link_count):
            if beyond(index) is not None:

                @pl.when(beyond(index))
                def _():
                    pl.semaphore_signal(
                        ready,
                        inc=1,
                        device_id=places[index],
                        device_id_type=pl.DeviceIdType.MESH,
                    )

    def notify():
        for collector in collectors:

            @pl.when(device_pos != collector)
            def _():
                notice_to(collector).start()

    @pl.when(early)
    def _():
        meet()
        notify()

    side = jnp.where(quarter == 0, 1.0, -1.0)
    cosine = jnp.where(turn == 0, 1.0, 0.0) - jnp.where(turn == 2, 1.0, 0.0)
    sine = jnp.where(turn == 3, 1.0, 0.0) - jnp.where(turn == 1, 1.0, 0.0)

    index_loads[2].wait()
    loads[0].wait()
    pltpu.make_async_copy(state, state, load_sem.at[3]).wait()
    across = jnp.concatenate([indices[2]] * inner, axis=1)
    owner = across // elems
    place_in = across % elems
    member = [
        jnp.where(owner[face : face + 1] == target, 1.0, 0.0) for face in range(4)
    ]
    extras = [
        jnp.concatenate([part, jnp.zeros_like(part)], axis=0)
        for part in (flipped.astype(f32), cosine, sine, side)
    ]
    nothing = jnp.zeros_like(member[0])
    before = [nothing, member[0], member[0] + member[1], member[0] + member[1] + member[2]]
    left = jnp.concatenate(member + extras, axis=0).astype(bf16)
    right = jnp.concatenate(before + [jnp.zeros_like(part) for part in extras], axis=0)
    wide = dot(jnp.concatenate([left, right.astype(bf16)], axis=1), reach)
    spots = []
    for face in range(4):
        part = wide[face * link_rows : (face + 1) * link_rows]
        chosen = part[:, columns:] * (base_wide + inner * part[:, :columns])
        spots.append(jnp.sum(chosen, axis=0, keepdims=True))
    extra_row = 4 * link_rows
    flip_wide, cos_wide, sin_wide, side_wide = [
        wide[extra_row + 8 * index : extra_row + 8 * index + 8, columns:]
        for index in range(4)
    ]

    def stretched(per_face):
        rows = []
        for values in per_face:
            rows.append(values)
            rows.append(jnp.zeros_like(values))
        wide = dot(jnp.concatenate(rows, axis=0).astype(bf16), reach[:LANES, columns:])
        return [wide[8 * index : 8 * index + 8] for index in range(len(per_face))]

    def rows_for(slot, stride):
        spot = slot + (level[:1] % inner + level[:1] // inner * stride).astype(f32)
        return jnp.where(slot > 0.5, spot, 0.0)

    def hot_rows(count, spots):
        count_iota = (iota((count, columns), 0) + 1).astype(f32)
        return jnp.concatenate(
            [
                onehot(
                    count_iota == jnp.broadcast_to(spots[face], (count, columns))
                )
                for face in range(4)
            ],
            axis=1,
        )

    pack = hot_rows(total_rows, [rows_for(spot, 0) for spot in spots])

    def over_faces(wide, rows):
        return jnp.concatenate(
            [jnp.broadcast_to(wide[face : face + 1], (rows, columns)) for face in range(4)],
            axis=1,
        )

    def to_fields(block):
        return jnp.concatenate(
            [
                jnp.concatenate(
                    [
                        block[face * 8 : face * 8 + 8, field * columns : (field + 1) * columns]
                        for face in range(4)
                    ],
                    axis=1,
                )
                for field in range(4)
            ],
            axis=0,
        )

    def to_faces(block):
        return jnp.concatenate(
            [
                jnp.concatenate(
                    [
                        block[field * 8 : field * 8 + 8, face * columns : (face + 1) * columns]
                        for field in range(4)
                    ],
                    axis=1,
                )
                for face in range(4)
            ],
            axis=0,
        )

    flip_all, cos_all, sin_all, side_all = [
        over_faces(wide, 8) for wide in (flip_wide, cos_wide, sin_wide, side_wide)
    ]
    level_all = iota((half, span), 1) % levels // inner

    for field in range(4):
        padded[field, :25] = state[:, field, :]
    values = jnp.concatenate([padded[field] for field in range(4)], axis=1)
    on_faces = dot3(face_tables[:, :96], values)
    traces, slopes, flipped_traces, flipped_slopes = [
        to_fields(on_faces[32 * part : 32 * part + 32]) for part in range(4)
    ]

    def aligned(plain, mirrored):
        parts = [
            jnp.where(
                flip_all > 0.5,
                mirrored[field * 8 : field * 8 + 8],
                plain[field * 8 : field * 8 + 8],
            )
            for field in range(4)
        ]
        parts[1], parts[2] = (
            cos_all * parts[1] - sin_all * parts[2],
            cos_all * parts[2] + sin_all * parts[1],
        )
        return parts

    message = aligned(traces, flipped_traces) + [
        side_all * part for part in aligned(slopes, flipped_slopes)
    ]
    high, low = halves(jnp.concatenate(message, axis=0))
    pieces = []
    for part in (high, low):
        for index in range(outer_levels):
            pieces.append(jnp.where(level_all == index, part, jnp.zeros_like(part)))
    stacked = dot_t(pack, jnp.concatenate(pieces, axis=0))
    sent[...] = stacked[:, :LANES] + stacked[:, LANES:]
    pl.when(jnp.logical_not(early))(meet)
    order = sorted(
        range(link_count), key=lambda index: (links[index][1] < 0, abs(links[index][1]))
    )
    for index in order:
        if before_start(index) is None:
            copy_of(index).start()
        else:
            pl.when(jnp.logical_not(before_start(index)))(copy_of(index).start)
    pl.when(jnp.logical_not(early))(notify)
    always = device_pos >= 0

    @pl.when(always)
    def _():
        first_of = owner * (4 * elems)
        key = (first_of + face_back * elems + place_in).astype(f32)
        first_of = first_of.astype(f32)
        key_down = jnp.transpose(jnp.concatenate([key, key], axis=0))
        back_rows = []
        for face in range(4):
            smaller = jnp.zeros((elems, LANES), f32)
            for other in range(4):
                rival = jnp.broadcast_to(key_down[:elems, other : other + 1], (elems, LANES))
                mine = (rival < key[face : face + 1]) & (rival >= first_of[face : face + 1])
                smaller = smaller + jnp.where(mine, 1.0, 0.0)
            rank = jnp.sum(smaller, axis=0, keepdims=True)
            back_rows.append(
                jnp.sum(member[face] * (base_back + inner * rank), axis=0, keepdims=True)
            )
        at_home = owner == device_pos
        homes = [
            jnp.where(at_home & (face_back == face), place_in + 1, 0).astype(f32)
            for face in range(4)
        ]
        back, *homes = stretched([jnp.concatenate(back_rows, axis=0)] + homes)
        spread[...] = hot_rows(
            outer_levels * LANES,
            [rows_for(back[face : face + 1], LANES) for face in range(4)],
        )

        slopes_out = slopes * over_faces(side_wide, 32)
        both_high, both_low = halves(jnp.concatenate([traces, slopes_out], axis=0))
        both = jnp.concatenate([both_high, both_low], axis=0)
        found = jnp.zeros((128, span), f32)
        for face in range(4):
            home_spot = jnp.where(
                homes[face] > 0.5, homes[face] * levels + (level - levels + 1).astype(f32), 0.0
            )
            found = found + dot(
                both[:, face * columns : (face + 1) * columns],
                hot_rows(columns, [home_spot[into : into + 1] for into in range(4)]),
            )
        found = found[:64] + found[64:]
        known[:32] = traces
        known[32:64] = found[:32]
        known[64:96] = found[32:] - slopes
        known[96:128] = over_faces(
            0.5 + viscosity * penalty - 0.25 * lift_gain * viscosity * (1.0 + side_wide), 32
        )
        pressure, vel_u, vel_v, theta = [
            values[:, field * columns : (field + 1) * columns] for field in range(4)
        ]
        nothing = jnp.zeros_like(pressure)
        flux_x = jnp.concatenate([vel_u, pressure, nothing, theta * vel_u], axis=1)
        flux_y = jnp.concatenate([vel_v, nothing, pressure, theta * vel_v], axis=1)
        loads[1].wait()
        loads[2].wait()
        for field in range(4):
            padded[field, :25] = register[:, field, :]
        held = jnp.concatenate([padded[field] for field in range(4)], axis=1)
        own = dot3(tables[:32, :288], jnp.concatenate([flux_x, flux_y, values], axis=0))
        own = section_a * held + step_size * own
        moved = values + section_b * own
        for field in range(4):
            sides = slice(field * columns, (field + 1) * columns)
            own_register[:, field, :] = own[:25, sides]
            own_state[:, field, :] = moved[:25, sides]

    waiting = [index for index in order if before_start(index) is not None]
    late_partners = sum(jnp.where(before_start(index), 1, 0) for index in waiting)

    @pl.when(late_partners > 0)
    def _():
        pl.semaphore_wait(ready, late_partners)

    for index in waiting:
        pl.when(before_start(index))(copy_of(index).start)

    rows_done(arrived, total_rows, recv_sem).wait()
    filler = jnp.zeros((LANES - total_rows, LANES), f32)
    turned = jnp.transpose(jnp.concatenate([arrived[...], filler], axis=0))
    turned = jnp.concatenate(
        [turned[half * index : half * (index + 1)] for index in range(outer_levels)], axis=1
    )
    high, low = halves(turned)
    far = dot(jnp.concatenate([high, low], axis=0), spread[...])
    far = far[:half] + far[half:]
    inside = known[:32]
    outside = known[32:64] + far[:32]
    jump = outside - inside
    slope_term = (0.5 * viscosity) * (known[64:96] + far[32:])
    weight = known[96:128]
    terms = []
    for face in range(4):
        sides = slice(face * columns, (face + 1) * columns)
        ins = [inside[field * 8 : field * 8 + 8, sides] for field in range(4)]
        outs = [outside[field * 8 : field * 8 + 8, sides] for field in range(4)]
        step = [jump[field * 8 : field * 8 + 8, sides] for field in range(4)]
        normal = 1 + face % 2
        sign = 1.0 if face < 2 else -1.0
        raw_in, raw_out = ins[normal], outs[normal]
        wave = weight[:8, sides] + 0.5 * jnp.maximum(jnp.abs(raw_in), jnp.abs(raw_out))
        drops = [
            (-0.5 * sign) * step[normal],
            None,
            None,
            (0.5 * sign) * (ins[3] * raw_in - outs[3] * raw_out),
        ]
        drops[normal] = (-0.5 * sign) * step[0]
        rows = []
        for field in range(4):
            term = wave * step[field] + slope_term[field * 8 : field * 8 + 8, sides]
            rows.append(term if drops[field] is None else term + drops[field])
        terms.append(jnp.concatenate(rows, axis=0))
    face_term = jnp.concatenate(terms, axis=1)

    @pl.when(collects)
    def _():
        rows_done(notices, device_count - 1, word_recv_sem).wait()

        @pl.when(device_pos == herald)
        def _():
            heard = jnp.max(notices[...], axis=0, keepdims=True) + notice[:1]
            notice[8:] = jnp.broadcast_to(heard, (8, LANES))
            for position in range(device_count):
                if position not in collectors:
                    verdict_to(position).start()

    heard = notice[:8]
    for start in range(0, notices.shape[0], 8):
        heard = jnp.maximum(heard, notices[start : start + 8])
    sideways[0] = jnp.where(jnp.max(heard) > 0.5, 1, 0)
    late = dot3(
        tables[32:, :192], jnp.concatenate([to_faces(face_term), to_faces(jump)], axis=0)
    )
    for field in range(4):
        late_part[:, field, :] = late[:25, field * columns : (field + 1) * columns]

    @pl.when(device_pos == herald)
    def _():
        rows_done(notices, device_count - len(collectors), verdict_send_sem).wait()

    @pl.when(collects)
    def _():
        rows_done(notice, len(collectors) - 1, notice_send_sem).wait()

    @pl.when(jnp.logical_not(collects))
    def _():
        rows_done(notice, len(collectors), notice_send_sem).wait()
        rows_done(verdict, 1, word_recv_sem).wait()
        sideways[0] = jnp.where(jnp.max(verdict[:1]) > 0.5, 1, 0)

    rows_done(sent, total_rows, send_sem).wait()


def closing_kernel(
    own_register, own_state, late, next_state, next_register, new_state, new_register, sems
):
    nodes = late.shape[0]
    piece = -(-nodes // 3)
    for start in range(0, nodes, piece):
        rows = pl.ds(start, min(piece, nodes - start))
        part = step_size * late[rows]
        new_register[rows] = own_register[rows] + part
        pltpu.make_async_copy(new_register.at[rows], next_register.at[rows], sems.at[0]).start()
        new_state[rows] = own_state[rows] + section_b * part
        pltpu.make_async_copy(new_state.at[rows], next_state.at[rows], sems.at[1]).start()
    pltpu.make_async_copy(new_register, next_register, sems.at[0]).wait()
    pltpu.make_async_copy(new_state, next_state, sems.at[1]).wait()


def start_kernel(state, register, own_register, own_state):
    own_register[...] = section_a * register[...]
    own_state[...] = state[...] + section_b * own_register[...]


def body(curve_count, strip_count, state, register, neighbor, neighbor_face, seam):
    elems = neighbor.shape[1]
    columns = state.shape[2]
    levels = columns // elems
    inner = LANES // elems
    outer_levels = levels // inner
    reach = min(7, (curve_count - 1) // 2)
    slots = (TW + reach - 1) // reach
    links, rows_of = [], []
    for distance in range(reach, 0, -1):
        for direction in (1, -1):
            links.append(("curve", direction * distance))
            rows_of.append(-(-slots * inner // 8) * 8)
    for direction in (1, -1):
        links.append(("sub", direction))
        rows_of.append(-(-TW * inner // 8) * 8)
    offsets = [sum(rows_of[:index]) for index in range(len(links))]
    total_rows = sum(rows_of)
    plan = (elems, levels, curve_count, strip_count, links, rows_of, offsets)
    vmem = pl.BlockSpec(memory_space=pltpu.VMEM)
    nodes_first = jnp.transpose(state, (1, 0, 2))
    register_first = jnp.transpose(register, (1, 0, 2))
    shape = nodes_first.shape

    def call(kernel, tables, more, outputs, out_specs, scratch, collective_id):
        tables = [jnp.asarray(table) for table in tables]
        operands = (nodes_first, neighbor, neighbor_face, seam, *tables, *more)
        return pl.pallas_call(
            functools.partial(kernel, plan),
            out_shape=outputs,
            in_specs=[pl.BlockSpec(memory_space=pl.ANY)] * len(operands),
            out_specs=out_specs,
            scratch_shapes=scratch,
            compiler_params=pltpu.CompilerParams(
                collective_id=collective_id, has_side_effects=True
            ),
        )(*[pltpu.with_memory_space_constraint(operand, pltpu.HBM) for operand in operands])

    def two_rounds():
        change = call(
            two_round_kernel,
            (build_tables(),),
            (),
            pltpu.VMEM(nodes_first.shape, f32),
            vmem,
            [
                pltpu.VMEM(shape, f32),
                pltpu.VMEM(neighbor.shape, jnp.int32),
                pltpu.VMEM(neighbor.shape, jnp.int32),
                pltpu.VMEM(neighbor.shape, jnp.int32),
                pltpu.VMEM((224, 384), bf16),
                pltpu.VMEM((4, 32, columns), f32),
                pltpu.VMEM((2, total_rows, LANES), f32),
                pltpu.VMEM((2, total_rows, LANES), f32),
                pltpu.VMEM((32, 4 * columns), f32),
                pltpu.VMEM((128, 4 * columns), f32),
                pltpu.VMEM((128, columns), f32),
                pltpu.SemaphoreType.DMA((5,)),
                pltpu.SemaphoreType.DMA((2, len(links))),
                pltpu.SemaphoreType.DMA((2, len(links))),
            ],
            0,
        )
        started = pl.pallas_call(
            start_kernel,
            out_shape=(pltpu.VMEM(shape, f32), pltpu.VMEM(shape, f32)),
            in_specs=[vmem, vmem],
            out_specs=(vmem, vmem),
        )(*[pltpu.with_memory_space_constraint(x, pltpu.HBM) for x in (nodes_first, register_first)])
        return *started, change

    device_count = curve_count * strip_count
    if device_count <= DIRECT_LIMIT and total_rows <= LANES and outer_levels * 64 == LANES:
        *parts, sideways = call(
            direct_kernel,
            build_direct_tables(),
            (register_first,),
            (pltpu.VMEM(shape, f32),) * 3 + (pltpu.SMEM((1,), jnp.int32),),
            (vmem,) * 3 + (pl.BlockSpec(memory_space=pltpu.SMEM),),
            [
                pltpu.VMEM(shape, f32),
                pltpu.VMEM((3, *neighbor.shape), jnp.int32),
                pltpu.VMEM((128, LANES), bf16),
                pltpu.VMEM((64, 384), bf16),
                pltpu.VMEM((4, 32, columns), f32),
                pltpu.VMEM((total_rows, LANES), f32),
                pltpu.VMEM((total_rows, LANES), f32),
                pltpu.VMEM((16, LANES), f32),
                pltpu.VMEM((-(-device_count // 8) * 8, LANES), f32),
                pltpu.VMEM((8, LANES), f32),
                pltpu.VMEM((outer_levels * LANES, 4 * columns), bf16),
                pltpu.VMEM((128, 4 * columns), f32),
                pltpu.VMEM(shape, f32),
                pltpu.SemaphoreType.REGULAR,
                pltpu.SemaphoreType.DMA((2,)),
                pltpu.SemaphoreType.DMA((4,)),
                pltpu.SemaphoreType.DMA,
                pltpu.SemaphoreType.DMA,
                pltpu.SemaphoreType.DMA,
                pltpu.SemaphoreType.DMA,
                pltpu.SemaphoreType.DMA,
            ],
            1,
        )
        parts = lax.cond(
            sideways[0] == 0, lambda kept: tuple(kept), lambda _: two_rounds(), parts
        )
    else:
        parts = two_rounds()
    new = pl.pallas_call(
        closing_kernel,
        out_shape=(jax.ShapeDtypeStruct(shape, f32), jax.ShapeDtypeStruct(shape, f32)),
        in_specs=[vmem] * 3,
        out_specs=(pl.BlockSpec(memory_space=pl.ANY),) * 2,
        scratch_shapes=[
            pltpu.VMEM(shape, f32),
            pltpu.VMEM(shape, f32),
            pltpu.SemaphoreType.DMA((2,)),
        ],
    )(*parts)
    return tuple(jnp.transpose(part, (1, 0, 2)) for part in new)


def solution(mesh):
    wide = P(None, None, ("curve", "sub"))
    flat = P(None, ("curve", "sub"))
    return jax.shard_map(
        functools.partial(body, mesh.shape["curve"], mesh.shape["sub"]),
        mesh=mesh,
        in_specs=(wide, wide, flat, flat, flat),
        out_specs=(wide, wide),
        check_vma=False,
    )
```

```python
import functools
import math

import jax
import jax.numpy as jnp
import ml_dtypes
import numpy as np
from jax import lax
from jax.experimental import pallas as pl
from jax.experimental.pallas import tpu as pltpu
from jax.sharding import PartitionSpec as P

TW = 8
LANES = 128
DIRECT_LIMIT = 64

lift_gain = 10.0
step_size = 0.02
viscosity = 0.05
penalty = 2.0
section_a = -567301805773.0 / 1357537059087.0
section_b = 2404267990393.0 / 2016746695238.0

f32 = jnp.float32
bf16 = jnp.bfloat16


def build_derivative():
    points = np.array([-1.0, -math.sqrt(3.0 / 7.0), 0.0, math.sqrt(3.0 / 7.0), 1.0])
    weights = np.array(
        [
            1.0 / np.prod([points[row] - points[col] for col in range(5) if col != row])
            for row in range(5)
        ]
    )
    table = np.zeros((5, 5))
    for row in range(5):
        for col in range(5):
            if row != col:
                table[row, col] = weights[col] / weights[row] / (points[row] - points[col])
        table[row, row] = -np.sum(table[row])
    return table


def face_node(face, node):
    return [(4, node), (node, 4), (0, node), (node, 0)][face]


def split_const(table):
    high = table.astype(ml_dtypes.bfloat16)
    low = (table - high.astype(np.float64)).astype(ml_dtypes.bfloat16)
    return np.concatenate([high, low, high], axis=1)


def element_tables():
    d = build_derivative()
    eye = np.eye(5)
    dx = np.zeros((32, 32))
    dy = np.zeros((32, 32))
    dx[:25, :25] = np.kron(d, eye)
    dy[:25, :25] = np.kron(eye, d)
    pick = np.zeros((32, 32))
    for face in range(4):
        for node in range(5):
            a, b = face_node(face, node)
            pick[face * 8 + node, a * 5 + b] = 1.0
    normal_x = np.repeat([1.0, 0.0, -1.0, 0.0], 8)
    normal_y = np.repeat([0.0, 1.0, 0.0, -1.0], 8)
    lift_x = pick.T * normal_x[None] * (0.5 * lift_gain)
    lift_y = pick.T * normal_y[None] * (0.5 * lift_gain)
    return dx, dy, pick, normal_x, normal_y, lift_x, lift_y


def build_tables():
    dx, dy, pick, _, _, lift_x, lift_y = element_tables()
    grad_x = np.concatenate([dx, lift_x], axis=1)
    grad_y = np.concatenate([dy, lift_y], axis=1)
    grad = np.concatenate([grad_x, grad_y, pick @ grad_x, pick @ grad_y], axis=0)
    volume = np.concatenate([-dx, -dy, lift_gain * pick.T], axis=1)
    late = lift_gain * 0.5 * viscosity * pick.T
    out = np.zeros((224, 384), ml_dtypes.bfloat16)
    out[:128, :192] = split_const(grad)
    out[:128, 192:288] = split_const(grad[:, 32:])
    out[128:160, :288] = split_const(volume)
    out[160:192, :96] = split_const(late)
    out[192:224, :32] = pick.astype(ml_dtypes.bfloat16)
    out[192:224, 32:64] = pick.astype(ml_dtypes.bfloat16)
    return out


def build_direct_tables():
    dx, dy, pick, normal_x, normal_y, lift_x, lift_y = element_tables()
    slope = normal_x[:, None] * (pick @ dx) + normal_y[:, None] * (pick @ dy)
    base = np.concatenate([-dx, -dy, viscosity * (dx @ dx + dy @ dy)], axis=1)
    jump = viscosity * (dx @ lift_x + dy @ lift_y)
    late = np.concatenate([lift_gain * pick.T, jump], axis=1)
    mirror = np.arange(32).reshape(4, 8)
    mirror[:, :5] = mirror[:, 4::-1]
    mirror = mirror.reshape(-1)
    first = np.zeros((128, LANES), ml_dtypes.bfloat16)
    first[:, :96] = split_const(
        np.concatenate([pick, slope, pick[mirror], slope[mirror]], axis=0)
    )
    out = np.zeros((64, 384), ml_dtypes.bfloat16)
    out[:32, :288] = split_const(base)
    out[32:, :192] = split_const(late)
    return first, out


def halves(x):
    high = x.astype(bf16)
    low = (x - high.astype(f32)).astype(bf16)
    return high, low


def dot(a, b):
    return lax.dot_general(a, b, (((1,), (0,)), ((), ())), preferred_element_type=f32)


def dot_t(a, b):
    return lax.dot_general(a, b, (((1,), (1,)), ((), ())), preferred_element_type=f32)


def dot3(table, x):
    high, low = halves(x)
    return dot(table, jnp.concatenate([high, high, low], axis=0))


def onehot(mask):
    return jnp.where(mask, 1.0, 0.0).astype(bf16)


def permute(x, perm):
    rows = x.shape[0]
    high, low = halves(x)
    both = dot(jnp.concatenate([high, low], axis=0), perm)
    return both[:rows] + both[rows:]


def iota(shape, dim):
    return lax.broadcasted_iota(jnp.int32, shape, dim)


def two_round_kernel(
    plan,
    state_hbm,
    neighbor_hbm,
    neighbor_face_hbm,
    seam_hbm,
    tables_hbm,
    change,
    state,
    neighbor,
    neighbor_face,
    seam,
    tables,
    padded,
    sent,
    arrived,
    own_faces,
    early_grads,
    early_change,
    load_sem,
    send_sem,
    recv_sem,
):
    elems, levels, curve_count, strip_count, links, rows_of, offsets = plan
    columns = elems * levels
    inner = LANES // elems
    outer_levels = levels // inner
    groups = 4 * outer_levels
    span = 4 * LANES
    total_rows = offsets[-1] + rows_of[-1]
    link_count = len(links)
    link_rows = -(-link_count // 8) * 8

    curve_pos = lax.axis_index("curve")
    strip_pos = lax.axis_index("sub")
    device_pos = curve_pos * strip_count + strip_pos
    places = []
    for axis, step in links:
        if axis == "curve":
            places.append((lax.rem(curve_pos + step + curve_count, curve_count), strip_pos))
        else:
            places.append((curve_pos, lax.rem(strip_pos + step + strip_count, strip_count)))

    barrier = pltpu.get_barrier_semaphore()
    for place in places:
        pl.semaphore_signal(
            barrier, inc=1, device_id=place, device_id_type=pl.DeviceIdType.MESH
        )
    loads = [
        pltpu.make_async_copy(source_ref, target_ref, load_sem.at[index])
        for index, (source_ref, target_ref) in enumerate(
            [
                (neighbor_hbm, neighbor),
                (neighbor_face_hbm, neighbor_face),
                (seam_hbm, seam),
                (state_hbm, state),
                (tables_hbm, tables),
            ]
        )
    ]
    for load in loads:
        load.start()
    for load in loads[:3]:
        load.wait()

    def widen(ref):
        block = ref[...]
        return jnp.concatenate([block] * inner, axis=1)

    across = widen(neighbor)
    face_back = widen(neighbor_face)
    codes = widen(seam)
    owner = across // elems
    place_in = across % elems
    turn = codes % 4
    flipped = codes // 4
    sub_level = iota((4, LANES), 1) // elems
    position = face_back * LANES + sub_level * elems + place_in
    source = jnp.where(owner == device_pos, position, -1)
    heading = (face_back + turn) % 4
    cosine = jnp.where(turn == 0, 1.0, 0.0) - jnp.where(turn == 2, 1.0, 0.0)
    sine = jnp.where(turn == 3, 1.0, 0.0) - jnp.where(turn == 1, 1.0, 0.0)
    head_x = jnp.where(heading == 0, 1.0, 0.0) - jnp.where(heading == 2, 1.0, 0.0)
    head_y = jnp.where(heading == 1, 1.0, 0.0) - jnp.where(heading == 3, 1.0, 0.0)

    link_iota = iota((link_rows, LANES), 0)
    target = jnp.full((link_rows, LANES), -1, jnp.int32)
    base = jnp.zeros((link_rows, LANES), f32)
    for index, place in enumerate(places):
        target = jnp.where(link_iota == index, place[0] * strip_count + place[1], target)
        base = jnp.where(link_iota == index, float(offsets[index] + 1), base)
    base = base + (iota((link_rows, LANES), 1) // elems).astype(f32)
    member = [
        jnp.where(owner[face : face + 1] == target, 1.0, 0.0) for face in range(4)
    ]
    from_lane = iota((LANES, 2 * LANES), 0)
    to_lane = iota((LANES, 2 * LANES), 1)
    same = from_lane // elems == (to_lane % LANES) // elems
    earlier = same & ((from_lane < to_lane) | (to_lane >= LANES))
    counts = dot(jnp.concatenate(member, axis=0).astype(bf16), onehot(earlier))
    before = jnp.zeros((link_rows, LANES), f32)
    slot_rows = []
    for face in range(4):
        part = counts[face * link_rows : (face + 1) * link_rows]
        rank = part[:, :LANES] + before
        before = before + part[:, LANES:]
        slot_rows.append(
            jnp.sum(member[face] * (base + inner * rank), axis=0, keepdims=True)
        )
    slot_row = jnp.concatenate(slot_rows, axis=1)
    pack = onehot(
        (iota((total_rows, span), 0) + 1).astype(f32)
        == jnp.broadcast_to(slot_row, (total_rows, span))
    )
    pack2 = jnp.concatenate([pack, pack], axis=1)

    def local_table():
        span_iota = iota((span, LANES), 0)
        return jnp.concatenate(
            [onehot(span_iota == source[face : face + 1]) for face in range(4)], axis=1
        )

    meta_iota = iota((8, LANES), 0)
    meta_blocks = []
    for face in range(4):
        block = jnp.zeros((8, LANES), f32)
        for row, values in enumerate(
            [flipped.astype(f32), cosine, sine, (position + 1).astype(f32)]
        ):
            block = jnp.where(meta_iota == row, values[face : face + 1], block)
        meta_blocks.append(block)
    meta = jnp.concatenate(meta_blocks, axis=1)
    heads_x = jnp.concatenate(
        [jnp.broadcast_to(head_x[face : face + 1], (8, LANES)) for face in range(4)], axis=0
    )
    heads_y = jnp.concatenate(
        [jnp.broadcast_to(head_y[face : face + 1], (8, LANES)) for face in range(4)], axis=0
    )

    def to_exchange(faces):
        return jnp.concatenate(
            [
                jnp.concatenate(
                    [
                        faces[face * 8 : face * 8 + 8, group * LANES : (group + 1) * LANES]
                        for face in range(4)
                    ],
                    axis=1,
                )
                for group in range(groups)
            ],
            axis=0,
        )

    def from_exchange(block):
        return jnp.concatenate(
            [
                jnp.concatenate(
                    [
                        block[group * 8 : group * 8 + 8, face * LANES : (face + 1) * LANES]
                        for group in range(groups)
                    ],
                    axis=1,
                )
                for face in range(4)
            ],
            axis=0,
        )

    data_lanes = groups * 8
    field_lanes = outer_levels * 8
    lane = iota((total_rows, LANES), 1)
    node_lane = lane % 8
    in_data = lane < data_lanes

    def copy_of(turn_index, index):
        rows = pl.ds(offsets[index], rows_of[index])
        return pltpu.make_async_remote_copy(
            src_ref=sent.at[turn_index, rows],
            dst_ref=arrived.at[turn_index, rows],
            send_sem=send_sem.at[turn_index, index],
            recv_sem=recv_sem.at[turn_index, index],
            device_id=places[index],
            device_id_type=pl.DeviceIdType.MESH,
        )

    def post(turn_index, block, flags):
        if flags is None:
            pieces = [block, meta]
            if data_lanes + 8 < LANES:
                pieces.append(jnp.zeros((LANES - data_lanes - 8, span), f32))
            block = jnp.concatenate(pieces, axis=0)
        high, low = halves(block)
        message = dot_t(pack2, jnp.concatenate([high, low], axis=1))
        if flags is None:
            flags = [
                jnp.broadcast_to(
                    message[:, data_lanes + index : data_lanes + index + 1], message.shape
                )
                for index in range(3)
            ]
        else:
            rest = jnp.zeros((total_rows, LANES - data_lanes), f32)
            message = jnp.concatenate([message, rest], axis=1)
        flip, cos, sin = flags
        mirrored = message
        for node, shift in ((0, LANES - 4), (1, LANES - 2), (3, 2), (4, 4)):
            mirrored = jnp.where(
                node_lane == node, pltpu.roll(message, shift, axis=1), mirrored
            )
        aligned = jnp.where(in_data & (flip > 0.5), mirrored, message)
        field = lane // field_lanes
        turned_u = cos * aligned - sin * pltpu.roll(aligned, LANES - field_lanes, axis=1)
        turned_v = cos * aligned + sin * pltpu.roll(aligned, field_lanes, axis=1)
        aligned = jnp.where(field == 1, turned_u, jnp.where(field == 2, turned_v, aligned))
        sent[turn_index] = aligned
        if turn_index == 0:
            pl.semaphore_wait(barrier, link_count)
        for index in range(link_count):
            copy_of(turn_index, index).start()
        return flags

    def gather_local(block):
        rows = block.shape[0]
        high, low = halves(block)
        both = dot(jnp.concatenate([high, low], axis=0), local_table())
        return both[:rows] + both[rows:]

    def await_all(turn_index):
        for index in range(link_count):
            copy_of(turn_index, index).wait_recv()

    def spread_table():
        message = arrived[0]
        spot = jnp.broadcast_to(
            message[:, data_lanes + 3 : data_lanes + 4], (total_rows, span)
        )
        return onehot((iota((total_rows, span), 1) + 1).astype(f32) == spot)

    def collect(turn_index, spread):
        message = arrived[turn_index]
        high, low = halves(jnp.transpose(message)[:data_lanes])
        both = dot(jnp.concatenate([high, low], axis=0), spread)
        return both[:data_lanes] + both[data_lanes:]

    row = iota((columns, columns), 0)
    col = iota((columns, columns), 1)
    to_level = onehot(row == (col % elems) * levels + col // elems)
    to_elem = onehot(row == (col % levels) * elems + col // levels)

    padded[...] = jnp.zeros_like(padded)
    for load in loads[3:]:
        load.wait()
    for field in range(4):
        padded[field, :25] = state[:, field, :]
    nodal = permute(padded[...].reshape(128, columns), to_level)
    values = jnp.concatenate(
        [nodal[field * 32 : field * 32 + 32] for field in range(4)], axis=1
    )
    high, low = halves(values)
    faces_in = dot(tables[192:224, :64], jnp.concatenate([high, low], axis=0))

    def fields_of(wide):
        return [wide[:, field * columns : (field + 1) * columns] for field in range(4)]

    def elementwise_lanes(wide):
        return permute(jnp.concatenate(fields_of(wide), axis=0), to_elem)

    def early_part(values, faces_in, faces_out, grad_x, grad_y, face_gx, face_gy, own_slope):
        face_of_row = iota((32, columns), 0) // 8
        normal_x = jnp.where(face_of_row == 0, 1.0, 0.0) - jnp.where(face_of_row == 2, 1.0, 0.0)
        normal_y = jnp.where(face_of_row == 1, 1.0, 0.0) - jnp.where(face_of_row == 3, 1.0, 0.0)

        def flux_of(faces):
            speed = faces[1] * normal_x + faces[2] * normal_y
            return [speed, faces[0] * normal_x, faces[0] * normal_y, faces[3] * speed], speed

        inside, outside = fields_of(faces_in), fields_of(faces_out)
        gx_in, gy_in = fields_of(face_gx), fields_of(face_gy)
        slope_own = fields_of(own_slope)
        flux_in, speed_in = flux_of(inside)
        flux_out, speed_out = flux_of(outside)
        wave = 1.0 + jnp.maximum(jnp.abs(speed_in), jnp.abs(speed_out))
        terms = []
        for field in range(4):
            slope_in = gx_in[field] * normal_x + gy_in[field] * normal_y
            jump = outside[field] - inside[field]
            terms.append(
                0.5 * (flux_in[field] - flux_out[field])
                - 0.5 * viscosity * (slope_in - slope_own[field])
                + (0.5 * wave + viscosity * penalty) * jump
            )
        face_term = jnp.concatenate(terms, axis=1)
        pressure, vel_u, vel_v, theta = fields_of(values)
        nothing = jnp.zeros_like(pressure)
        flux_x = jnp.concatenate([vel_u, pressure, nothing, theta * vel_u], axis=1)
        flux_y = jnp.concatenate([vel_v, nothing, pressure, theta * vel_v], axis=1)
        tendency = dot3(
            tables[128:160, :288],
            jnp.concatenate(
                [flux_x - viscosity * grad_x, flux_y - viscosity * grad_y, face_term], axis=0
            ),
        )

        return elementwise_lanes(tendency)

    block_in = to_exchange(faces_in)
    flags = post(0, block_in, None)
    always = device_pos >= 0

    @pl.when(always)
    def _():
        own = from_exchange(gather_local(block_in))
        own_faces[...] = own
        early_grads[...] = dot3(
            tables[:128, :192], jnp.concatenate([values, own - faces_in], axis=0)
        )

    await_all(0)
    spread = spread_table()
    far_faces = from_exchange(collect(0, spread))
    face_grads = early_grads[64:128] + dot3(tables[64:128, 192:288], far_faces)
    face_gx, face_gy = face_grads[:32], face_grads[32:]
    wide_x = jnp.concatenate([heads_x] * groups, axis=1)
    wide_y = jnp.concatenate([heads_y] * groups, axis=1)
    block_grad = to_exchange(face_gx * wide_x + face_gy * wide_y)
    post(1, block_grad, flags)

    @pl.when(always)
    def _():
        own_slope = from_exchange(gather_local(block_grad))
        grads = early_grads[:64] + dot3(tables[:64, 192:288], far_faces)
        faces_out = own_faces[...] + far_faces
        grad_x, grad_y = grads[:32], grads[32:]
        early_change[...] = early_part(
            values, faces_in, faces_out, grad_x, grad_y, face_gx, face_gy, own_slope
        )

    await_all(1)
    far_slope = from_exchange(collect(1, spread))
    late = elementwise_lanes(dot3(tables[160:192, :96], far_slope))
    total = early_change[...] + late
    for field in range(4):
        change[:, field, :] = total[field * 32 : field * 32 + 25]

    for turn_index in range(2):
        for index in range(link_count):
            copy_of(turn_index, index).wait_send()


def direct_kernel(
    plan,
    state_hbm,
    neighbor_hbm,
    neighbor_face_hbm,
    seam_hbm,
    face_tables_hbm,
    tables_hbm,
    register_hbm,
    own_register,
    own_state,
    late_part,
    sideways,
    state,
    indices,
    face_tables,
    tables,
    padded,
    sent,
    arrived,
    notice,
    notices,
    verdict,
    spread,
    known,
    register,
    ready,
    index_sem,
    load_sem,
    send_sem,
    recv_sem,
    notice_send_sem,
    word_recv_sem,
    verdict_send_sem,
):
    elems, levels, curve_count, strip_count, links, rows_of, offsets = plan
    columns = elems * levels
    span = 4 * columns
    inner = LANES // elems
    outer_levels = levels // inner
    total_rows = offsets[-1] + rows_of[-1]
    link_count = len(links)
    link_rows = -(-link_count // 8) * 8
    half = LANES // outer_levels

    curve_pos = lax.axis_index("curve")
    strip_pos = lax.axis_index("sub")
    device_pos = curve_pos * strip_count + strip_pos

    def place_at(curve_step, strip_step):
        return (
            lax.rem(curve_pos + curve_step + curve_count, curve_count),
            lax.rem(strip_pos + strip_step + strip_count, strip_count),
        )

    places = [place_at(step, 0) if axis == "curve" else place_at(0, step) for axis, step in links]
    device_count = curve_count * strip_count
    herald = device_count // 2 - 1
    collectors = (0, 1, herald)
    collects = (device_pos < 2) | (device_pos == herald)

    def place_of(position):
        return (position // strip_count, position % strip_count)

    tile_rows = 4 * columns // LANES

    def sides_of(row):
        start = row % 4 * columns + row // 4 * LANES
        return slice(start, start + LANES)

    def beyond(index):
        axis, step = links[index]
        if axis == "curve" and step > 0:
            return curve_pos + step >= curve_count
        return None

    def before_start(index):
        axis, step = links[index]
        if axis == "curve" and step < 0:
            return curve_pos + step < 0
        return None

    def tell(place):
        pl.semaphore_signal(
            barrier, inc=1, device_id=place, device_id_type=pl.DeviceIdType.MESH
        )

    def notice_to(position):
        return pltpu.make_async_remote_copy(
            src_ref=notice.at[pl.ds(0, 1)],
            dst_ref=notices.at[pl.ds(device_pos, 1)],
            send_sem=notice_send_sem,
            recv_sem=word_recv_sem,
            device_id=place_of(position),
            device_id_type=pl.DeviceIdType.MESH,
        )

    def verdict_to(position):
        return pltpu.make_async_remote_copy(
            src_ref=notice.at[pl.ds(8, 1)],
            dst_ref=verdict.at[pl.ds(0, 1)],
            send_sem=verdict_send_sem,
            recv_sem=word_recv_sem,
            device_id=place_of(position),
            device_id_type=pl.DeviceIdType.MESH,
        )

    def rows_done(ref, count, semaphore):
        rows = ref.at[pl.ds(0, count)]
        return pltpu.make_async_copy(rows, rows, semaphore)

    def copy_of(index):
        rows = pl.ds(offsets[index], rows_of[index])
        return pltpu.make_async_remote_copy(
            src_ref=sent.at[rows],
            dst_ref=arrived.at[rows],
            send_sem=send_sem,
            recv_sem=recv_sem,
            device_id=places[index],
            device_id_type=pl.DeviceIdType.MESH,
        )

    index_loads = [
        pltpu.make_async_copy(source_ref, indices.at[index], index_sem)
        for index, source_ref in enumerate((neighbor_face_hbm, seam_hbm, neighbor_hbm))
    ]
    loads = [
        pltpu.make_async_copy(source_ref, target_ref, load_sem.at[index])
        for index, (source_ref, target_ref) in enumerate(
            [
                (face_tables_hbm, face_tables),
                (tables_hbm, tables),
                (register_hbm, register),
            ]
        )
    ]
    nodes = state.shape[0]
    piece = -(-nodes // 5)
    state_loads = [
        pltpu.make_async_copy(
            state_hbm.at[pl.ds(start, min(piece, nodes - start))],
            state.at[pl.ds(start, min(piece, nodes - start))],
            load_sem.at[3],
        )
        for start in range(0, nodes, piece)
    ]
    for load in index_loads + state_loads + loads:
        load.start()
    notices[...] = jnp.zeros_like(notices)
    barrier = pltpu.get_barrier_semaphore()
    for index, place in enumerate(places):
        if beyond(index) is None:
            tell(place)
        else:
            pl.when(jnp.logical_not(beyond(index)))(functools.partial(tell, place))
    for collector in collectors:

        @pl.when(device_pos == collector)
        def _():
            for position in range(device_count - 1, -1, -1):
                if position != collector:
                    tell(place_of(position))

    padded[...] = jnp.zeros_like(padded)
    level = iota((8, columns), 1) % levels
    link_iota = iota((link_rows, LANES), 0)
    wide_iota = iota((link_rows, columns), 0)
    target = jnp.full((link_rows, LANES), -1, jnp.int32)
    base_wide = jnp.zeros((link_rows, columns), f32)
    base_back = jnp.zeros((link_rows, LANES), f32)
    for index, place in enumerate(places):
        target = jnp.where(link_iota == index, place[0] * strip_count + place[1], target)
        base_wide = jnp.where(wide_iota == index, float(offsets[index] + 1), base_wide)
        base_back = jnp.where(link_iota == index, float(offsets[index ^ 1] + 1), base_back)
    from_elem = iota((LANES, columns), 0)
    to_elem = iota((LANES, columns), 1) // levels
    reach = jnp.concatenate(
        [
            jnp.concatenate(
                [onehot((from_elem < elems) & (from_elem < to_elem)), onehot(from_elem < elems)],
                axis=0,
            ),
            jnp.concatenate(
                [onehot(from_elem == to_elem), onehot(from_elem < 0)], axis=0
            ),
        ],
        axis=1,
    )
    pltpu.make_async_copy(indices, indices, index_sem).wait()

    face_back, codes = [
        jnp.concatenate([indices[index]] * inner, axis=1) for index in range(2)
    ]
    turn = codes % 4
    flipped = codes // 4
    own_face = iota((4, LANES), 0)
    quarter = (face_back + turn - own_face + 4) % 4
    odd = jnp.where(quarter % 2 == 1, 1.0, 0.0)
    notice[:8] = jnp.broadcast_to(jnp.sum(odd, axis=0, keepdims=True), (8, LANES))
    early = device_pos >= device_count - strip_count // 2

    def meet():
        count = link_count + len(collectors) - jnp.where(collects, 1, 0)
        for index in range(link_count):
            if before_start(index) is not None:
                count = count - jnp.where(before_start(index), 1, 0)
        pl.semaphore_wait(barrier, count)
        for index in range(link_count):
            if beyond(index) is not None:

                @pl.when(beyond(index))
                def _():
                    pl.semaphore_signal(
                        ready,
                        inc=1,
                        device_id=places[index],
                        device_id_type=pl.DeviceIdType.MESH,
                    )

    def notify():
        for collector in collectors:

            @pl.when(device_pos != collector)
            def _():
                notice_to(collector).start()

    @pl.when(early)
    def _():
        meet()
        notify()

    side = jnp.where(quarter == 0, 1.0, -1.0)
    cosine = jnp.where(turn == 0, 1.0, 0.0) - jnp.where(turn == 2, 1.0, 0.0)
    sine = jnp.where(turn == 3, 1.0, 0.0) - jnp.where(turn == 1, 1.0, 0.0)

    loads[0].wait()
    pltpu.make_async_copy(state, state, load_sem.at[3]).wait()
    across = jnp.concatenate([indices[2]] * inner, axis=1)
    owner = across // elems
    place_in = across % elems
    member = [
        jnp.where(owner[face : face + 1] == target, 1.0, 0.0) for face in range(4)
    ]
    extras = [
        jnp.concatenate([part, jnp.zeros_like(part)], axis=0)
        for part in (flipped.astype(f32), cosine, sine, side)
    ]
    nothing = jnp.zeros_like(member[0])
    before = [nothing, member[0], member[0] + member[1], member[0] + member[1] + member[2]]
    left = jnp.concatenate(member + extras, axis=0).astype(bf16)
    right = jnp.concatenate(before + [jnp.zeros_like(part) for part in extras], axis=0)
    wide = dot(jnp.concatenate([left, right.astype(bf16)], axis=1), reach)
    spots = []
    for face in range(4):
        part = wide[face * link_rows : (face + 1) * link_rows]
        chosen = part[:, columns:] * (base_wide + inner * part[:, :columns])
        spots.append(jnp.sum(chosen, axis=0, keepdims=True))
    extra_row = 4 * link_rows
    flip_wide, cos_wide, sin_wide, side_wide = [
        wide[extra_row + 8 * index : extra_row + 8 * index + 8, columns:]
        for index in range(4)
    ]

    def stretched(per_face):
        rows = []
        for values in per_face:
            rows.append(values)
            rows.append(jnp.zeros_like(values))
        wide = dot(jnp.concatenate(rows, axis=0).astype(bf16), reach[:LANES, columns:])
        return [wide[8 * index : 8 * index + 8] for index in range(len(per_face))]

    def rows_for(slot, stride):
        spot = slot + (level[:1] % inner + level[:1] // inner * stride).astype(f32)
        return jnp.where(slot > 0.5, spot, 0.0)

    def hot_rows(count, spots):
        count_iota = (iota((count, columns), 0) + 1).astype(f32)
        return jnp.concatenate(
            [
                onehot(
                    count_iota == jnp.broadcast_to(spots[face], (count, columns))
                )
                for face in range(4)
            ],
            axis=1,
        )

    pack = hot_rows(total_rows, [rows_for(spot, 0) for spot in spots])

    def over_faces(wide, rows):
        return jnp.concatenate(
            [jnp.broadcast_to(wide[face : face + 1], (rows, columns)) for face in range(4)],
            axis=1,
        )

    def to_fields(block):
        return jnp.concatenate(
            [
                jnp.concatenate(
                    [
                        block[face * 8 : face * 8 + 8, field * columns : (field + 1) * columns]
                        for face in range(4)
                    ],
                    axis=1,
                )
                for field in range(4)
            ],
            axis=0,
        )

    def to_faces(block):
        return jnp.concatenate(
            [
                jnp.concatenate(
                    [
                        block[field * 8 : field * 8 + 8, face * columns : (face + 1) * columns]
                        for field in range(4)
                    ],
                    axis=1,
                )
                for face in range(4)
            ],
            axis=0,
        )

    flip_all, cos_all, sin_all, side_all = [
        over_faces(wide, 8) for wide in (flip_wide, cos_wide, sin_wide, side_wide)
    ]
    level_all = iota((half, span), 1) % levels // inner

    for field in range(4):
        padded[field, :25] = state[:, field, :]
    values = jnp.concatenate([padded[field] for field in range(4)], axis=1)
    on_faces = dot3(face_tables[:, :96], values)
    traces, slopes, flipped_traces, flipped_slopes = [
        to_fields(on_faces[32 * part : 32 * part + 32]) for part in range(4)
    ]

    def aligned(plain, mirrored):
        parts = [
            jnp.where(
                flip_all > 0.5,
                mirrored[field * 8 : field * 8 + 8],
                plain[field * 8 : field * 8 + 8],
            )
            for field in range(4)
        ]
        parts[1], parts[2] = (
            cos_all * parts[1] - sin_all * parts[2],
            cos_all * parts[2] + sin_all * parts[1],
        )
        return parts

    message = aligned(traces, flipped_traces) + [
        side_all * part for part in aligned(slopes, flipped_slopes)
    ]
    high, low = halves(jnp.concatenate(message, axis=0))
    pieces = []
    for part in (high, low):
        for index in range(outer_levels):
            pieces.append(jnp.where(level_all == index, part, jnp.zeros_like(part)))
    stacked = dot_t(pack, jnp.concatenate(pieces, axis=0))
    sent[...] = stacked[:, :LANES] + stacked[:, LANES:]
    pl.when(jnp.logical_not(early))(meet)
    order = sorted(
        range(link_count), key=lambda index: (links[index][1] < 0, abs(links[index][1]))
    )
    for index in order:
        if before_start(index) is None:
            copy_of(index).start()
        else:
            pl.when(jnp.logical_not(before_start(index)))(copy_of(index).start)
    pl.when(jnp.logical_not(early))(notify)
    always = device_pos >= 0

    @pl.when(always)
    def _():
        first_of = owner * (4 * elems)
        key = (first_of + face_back * elems + place_in).astype(f32)
        first_of = first_of.astype(f32)
        key_down = jnp.transpose(jnp.concatenate([key, key], axis=0))
        back_rows = []
        for face in range(4):
            smaller = jnp.zeros((elems, LANES), f32)
            for other in range(4):
                rival = jnp.broadcast_to(key_down[:elems, other : other + 1], (elems, LANES))
                mine = (rival < key[face : face + 1]) & (rival >= first_of[face : face + 1])
                smaller = smaller + jnp.where(mine, 1.0, 0.0)
            rank = jnp.sum(smaller, axis=0, keepdims=True)
            back_rows.append(
                jnp.sum(member[face] * (base_back + inner * rank), axis=0, keepdims=True)
            )
        at_home = owner == device_pos
        homes = [
            jnp.where(at_home & (face_back == face), place_in + 1, 0).astype(f32)
            for face in range(4)
        ]
        back, *homes = stretched([jnp.concatenate(back_rows, axis=0)] + homes)
        spread[...] = hot_rows(
            outer_levels * LANES,
            [rows_for(back[face : face + 1], LANES) for face in range(4)],
        )

        slopes_out = slopes * over_faces(side_wide, 32)
        both_high, both_low = halves(jnp.concatenate([traces, slopes_out], axis=0))
        both = jnp.concatenate([both_high, both_low], axis=0)
        found = jnp.zeros((128, span), f32)
        for face in range(4):
            home_spot = jnp.where(
                homes[face] > 0.5, homes[face] * levels + (level - levels + 1).astype(f32), 0.0
            )
            found = found + dot(
                both[:, face * columns : (face + 1) * columns],
                hot_rows(columns, [home_spot[into : into + 1] for into in range(4)]),
            )
        found = found[:64] + found[64:]
        known[:32] = traces
        known[32:64] = found[:32]
        known[64:96] = found[32:] - slopes
        known[96:128] = over_faces(
            0.5 + viscosity * penalty - 0.25 * lift_gain * viscosity * (1.0 + side_wide), 32
        )
        pressure, vel_u, vel_v, theta = [
            values[:, field * columns : (field + 1) * columns] for field in range(4)
        ]
        nothing = jnp.zeros_like(pressure)
        flux_x = jnp.concatenate([vel_u, pressure, nothing, theta * vel_u], axis=1)
        flux_y = jnp.concatenate([vel_v, nothing, pressure, theta * vel_v], axis=1)
        loads[1].wait()
        loads[2].wait()
        for field in range(4):
            padded[field, :25] = register[:, field, :]
        held = jnp.concatenate([padded[field] for field in range(4)], axis=1)
        own = dot3(tables[:32, :288], jnp.concatenate([flux_x, flux_y, values], axis=0))
        own = section_a * held + step_size * own
        moved = values + section_b * own
        for row in range(tile_rows):
            own_register[:, row, :] = own[:25, sides_of(row)]
            own_state[:, row, :] = moved[:25, sides_of(row)]

    waiting = [index for index in order if before_start(index) is not None]
    late_partners = sum(jnp.where(before_start(index), 1, 0) for index in waiting)

    @pl.when(late_partners > 0)
    def _():
        pl.semaphore_wait(ready, late_partners)

    for index in waiting:
        pl.when(before_start(index))(copy_of(index).start)

    rows_done(arrived, total_rows, recv_sem).wait()
    filler = jnp.zeros((LANES - total_rows, LANES), f32)
    turned = jnp.transpose(jnp.concatenate([arrived[...], filler], axis=0))
    turned = jnp.concatenate(
        [turned[half * index : half * (index + 1)] for index in range(outer_levels)], axis=1
    )
    high, low = halves(turned)
    far = dot(jnp.concatenate([high, low], axis=0), spread[...])
    far = far[:half] + far[half:]
    inside = known[:32]
    outside = known[32:64] + far[:32]
    jump = outside - inside
    slope_term = (0.5 * viscosity) * (known[64:96] + far[32:])
    weight = known[96:128]
    terms = []
    for face in range(4):
        sides = slice(face * columns, (face + 1) * columns)
        ins = [inside[field * 8 : field * 8 + 8, sides] for field in range(4)]
        outs = [outside[field * 8 : field * 8 + 8, sides] for field in range(4)]
        step = [jump[field * 8 : field * 8 + 8, sides] for field in range(4)]
        normal = 1 + face % 2
        sign = 1.0 if face < 2 else -1.0
        raw_in, raw_out = ins[normal], outs[normal]
        wave = weight[:8, sides] + 0.5 * jnp.maximum(jnp.abs(raw_in), jnp.abs(raw_out))
        drops = [
            (-0.5 * sign) * step[normal],
            None,
            None,
            (0.5 * sign) * (ins[3] * raw_in - outs[3] * raw_out),
        ]
        drops[normal] = (-0.5 * sign) * step[0]
        rows = []
        for field in range(4):
            term = wave * step[field] + slope_term[field * 8 : field * 8 + 8, sides]
            rows.append(term if drops[field] is None else term + drops[field])
        terms.append(jnp.concatenate(rows, axis=0))
    face_term = jnp.concatenate(terms, axis=1)

    @pl.when(collects)
    def _():
        rows_done(notices, device_count - 1, word_recv_sem).wait()

        @pl.when(device_pos == herald)
        def _():
            heard = jnp.max(notices[...], axis=0, keepdims=True) + notice[:1]
            notice[8:] = jnp.broadcast_to(heard, (8, LANES))
            for position in range(device_count):
                if position not in collectors:
                    verdict_to(position).start()

    heard = notice[:8]
    for start in range(0, notices.shape[0], 8):
        heard = jnp.maximum(heard, notices[start : start + 8])
    sideways[0] = jnp.where(jnp.max(heard) > 0.5, 1, 0)
    late = dot3(
        tables[32:, :192], jnp.concatenate([to_faces(face_term), to_faces(jump)], axis=0)
    )
    for row in range(tile_rows):
        late_part[:, row, :] = late[:25, sides_of(row)]

    @pl.when(device_pos == herald)
    def _():
        rows_done(notices, device_count - len(collectors), verdict_send_sem).wait()

    @pl.when(collects)
    def _():
        rows_done(notice, len(collectors) - 1, notice_send_sem).wait()

    @pl.when(jnp.logical_not(collects))
    def _():
        rows_done(notice, len(collectors), notice_send_sem).wait()
        rows_done(verdict, 1, word_recv_sem).wait()
        sideways[0] = jnp.where(jnp.max(verdict[:1]) > 0.5, 1, 0)

    rows_done(sent, total_rows, send_sem).wait()


def closing_kernel(
    own_register, own_state, late, next_state, next_register, new_state, new_register, sems
):
    nodes = late.shape[0]
    piece = -(-nodes // 3)
    for start in range(0, nodes, piece):
        rows = pl.ds(start, min(piece, nodes - start))
        part = step_size * late[rows]
        new_register[rows] = own_register[rows] + part
        pltpu.make_async_copy(new_register.at[rows], next_register.at[rows], sems.at[0]).start()
        new_state[rows] = own_state[rows] + section_b * part
        pltpu.make_async_copy(new_state.at[rows], next_state.at[rows], sems.at[1]).start()
    pltpu.make_async_copy(new_register, next_register, sems.at[0]).wait()
    pltpu.make_async_copy(new_state, next_state, sems.at[1]).wait()


def start_kernel(state, register, own_register, own_state):
    own_register[...] = section_a * register[...]
    own_state[...] = state[...] + section_b * own_register[...]


def body(curve_count, strip_count, state, register, neighbor, neighbor_face, seam):
    elems = neighbor.shape[1]
    columns = state.shape[2]
    levels = columns // elems
    inner = LANES // elems
    outer_levels = levels // inner
    reach = min(7, (curve_count - 1) // 2)
    slots = (TW + reach - 1) // reach
    links, rows_of = [], []
    for distance in range(reach, 0, -1):
        for direction in (1, -1):
            links.append(("curve", direction * distance))
            rows_of.append(-(-slots * inner // 8) * 8)
    for direction in (1, -1):
        links.append(("sub", direction))
        rows_of.append(-(-TW * inner // 8) * 8)
    offsets = [sum(rows_of[:index]) for index in range(len(links))]
    total_rows = sum(rows_of)
    plan = (elems, levels, curve_count, strip_count, links, rows_of, offsets)
    vmem = pl.BlockSpec(memory_space=pltpu.VMEM)
    nodes_first = jnp.transpose(state, (1, 0, 2))
    register_first = jnp.transpose(register, (1, 0, 2))
    shape = nodes_first.shape
    tiled = (shape[0], 4 * columns // LANES, LANES)

    def to_tiles(x):
        split = x.reshape(shape[0], 4, columns // LANES, LANES)
        return jnp.transpose(split, (0, 2, 1, 3)).reshape(tiled)

    def from_tiles(x):
        split = x.reshape(shape[0], columns // LANES, 4, LANES)
        return jnp.transpose(split, (2, 0, 1, 3)).reshape(4, shape[0], columns)


    def call(kernel, tables, more, outputs, out_specs, scratch, collective_id):
        tables = [jnp.asarray(table) for table in tables]
        operands = (nodes_first, neighbor, neighbor_face, seam, *tables, *more)
        return pl.pallas_call(
            functools.partial(kernel, plan),
            out_shape=outputs,
            in_specs=[pl.BlockSpec(memory_space=pl.ANY)] * len(operands),
            out_specs=out_specs,
            scratch_shapes=scratch,
            compiler_params=pltpu.CompilerParams(
                collective_id=collective_id, has_side_effects=True
            ),
        )(*[pltpu.with_memory_space_constraint(operand, pltpu.HBM) for operand in operands])

    def two_rounds():
        change = call(
            two_round_kernel,
            (build_tables(),),
            (),
            pltpu.VMEM(nodes_first.shape, f32),
            vmem,
            [
                pltpu.VMEM(shape, f32),
                pltpu.VMEM(neighbor.shape, jnp.int32),
                pltpu.VMEM(neighbor.shape, jnp.int32),
                pltpu.VMEM(neighbor.shape, jnp.int32),
                pltpu.VMEM((224, 384), bf16),
                pltpu.VMEM((4, 32, columns), f32),
                pltpu.VMEM((2, total_rows, LANES), f32),
                pltpu.VMEM((2, total_rows, LANES), f32),
                pltpu.VMEM((32, 4 * columns), f32),
                pltpu.VMEM((128, 4 * columns), f32),
                pltpu.VMEM((128, columns), f32),
                pltpu.SemaphoreType.DMA((5,)),
                pltpu.SemaphoreType.DMA((2, len(links))),
                pltpu.SemaphoreType.DMA((2, len(links))),
            ],
            0,
        )
        started = pl.pallas_call(
            start_kernel,
            out_shape=(pltpu.VMEM(tiled, f32), pltpu.VMEM(tiled, f32)),
            in_specs=[vmem, vmem],
            out_specs=(vmem, vmem),
        )(*[pltpu.with_memory_space_constraint(x, pltpu.HBM) for x in (to_tiles(nodes_first), to_tiles(register_first))])
        return *started, to_tiles(change)

    device_count = curve_count * strip_count
    if device_count <= DIRECT_LIMIT and total_rows <= LANES and outer_levels * 64 == LANES:
        *parts, sideways = call(
            direct_kernel,
            build_direct_tables(),
            (register_first,),
            (pltpu.VMEM(tiled, f32),) * 3 + (pltpu.SMEM((1,), jnp.int32),),
            (vmem,) * 3 + (pl.BlockSpec(memory_space=pltpu.SMEM),),
            [
                pltpu.VMEM(shape, f32),
                pltpu.VMEM((3, *neighbor.shape), jnp.int32),
                pltpu.VMEM((128, LANES), bf16),
                pltpu.VMEM((64, 384), bf16),
                pltpu.VMEM((4, 32, columns), f32),
                pltpu.VMEM((total_rows, LANES), f32),
                pltpu.VMEM((total_rows, LANES), f32),
                pltpu.VMEM((16, LANES), f32),
                pltpu.VMEM((-(-device_count // 8) * 8, LANES), f32),
                pltpu.VMEM((8, LANES), f32),
                pltpu.VMEM((outer_levels * LANES, 4 * columns), bf16),
                pltpu.VMEM((128, 4 * columns), f32),
                pltpu.VMEM(shape, f32),
                pltpu.SemaphoreType.REGULAR,
                pltpu.SemaphoreType.DMA,
                pltpu.SemaphoreType.DMA((4,)),
                pltpu.SemaphoreType.DMA,
                pltpu.SemaphoreType.DMA,
                pltpu.SemaphoreType.DMA,
                pltpu.SemaphoreType.DMA,
                pltpu.SemaphoreType.DMA,
            ],
            1,
        )
        parts = lax.cond(
            sideways[0] == 0, lambda kept: tuple(kept), lambda _: two_rounds(), parts
        )
    else:
        parts = two_rounds()
    new = pl.pallas_call(
        closing_kernel,
        out_shape=(jax.ShapeDtypeStruct(tiled, f32), jax.ShapeDtypeStruct(tiled, f32)),
        in_specs=[vmem] * 3,
        out_specs=(pl.BlockSpec(memory_space=pl.ANY),) * 2,
        scratch_shapes=[
            pltpu.VMEM(tiled, f32),
            pltpu.VMEM(tiled, f32),
            pltpu.SemaphoreType.DMA((2,)),
        ],
    )(*parts)
    return tuple(from_tiles(part) for part in new)


def solution(mesh):
    wide = P(None, None, ("curve", "sub"))
    flat = P(None, ("curve", "sub"))
    return jax.shard_map(
        functools.partial(body, mesh.shape["curve"], mesh.shape["sub"]),
        mesh=mesh,
        in_specs=(wide, wide, flat, flat, flat),
        out_specs=(wide, wide),
        check_vma=False,
    )
```
